32 devices in a mesh: dp: 4 (over z), neg: 8 (over y, x, core).
Axes of the slice: x: 2, y: 2, z: 4, core: 2. Of those that a mesh axis runs over, the one named last changes fastest.
Arguments:
- query_emb: bfloat16 [128, 32, 128], P(('dp', 'neg')), may hold values from -6 to 6
- positive: int32 [128], P(('dp', 'neg')), may hold values from 0 to 31
- passage_emb: bfloat16 [32, 512, 128], P(('dp', 'neg')), may hold values from -6 to 6
- lengths: int32 [32], P(('dp', 'neg')), may hold values from 256 to 512
- residual: bfloat16 [16384, 1024], P(('dp', 'neg')), may hold values from -6 to 6
- context: bfloat16 [16384, 1024], P(('dp', 'neg')), may hold values from -6 to 6
- out_proj: bfloat16 [1024, 1024], replicated, may hold values from -0.1875 to 0.1875
- norm_gain: float32 [1024], replicated, may hold values from 0.5 to 1.5
- colbert_proj: bfloat16 [1024, 128], replicated, may hold values from -0.1875 to 0.1875
Outputs:
- loss: float32 [], replicated
- query_grad: float32 [128, 32, 128], P(('dp', 'neg'))
- residual_grad: bfloat16 [16384, 1024], P(('dp', 'neg'))
- context_grad: bfloat16 [16384, 1024], P(('dp', 'neg'))
- out_proj_grad: float32 [1024, 1024], replicated
- colbert_grad: float32 [1024, 128], replicated
- gain_grad: float32 [1024], replicated
The draws below stay inside these ranges and needn't reach their ends.
Inputs may be any that keep to these rules, and one draw needn't show every extreme that they name: A passage's first lengths[p] token slots are real, the rest padding.
All inputs are finite; a program needn't handle non-finite values.
Results may differ from the reference program's by a relative error of at most 0.0065.
Values may be sent and summed in bfloat16 or wider, within the bound.
A program may use at most 64 MiB of HBM per device.

```python
import jax
import jax.numpy as jnp
from jax import lax

D = 1024
DIM = 128
QLEN = 32
PLEN = 512
QUERIES = 128
PASSAGES = 32
ROWS = 16384


noise_level = 0.6


similar_gap = 9.5


def unit_rows(values):
    return values / jnp.sqrt(jnp.sum(values * values, axis=-1, keepdims=True))


def shared_parts(key):
    midpoint = DIM // 2
    first_half = (jnp.arange(DIM) < midpoint).astype(jnp.float32)
    second_half = 1.0 - first_half
    chosen = jax.random.randint(jax.random.fold_in(key, 101), (QUERIES,), 0, PASSAGES).astype(jnp.int32)
    directions = unit_rows(jax.random.normal(jax.random.fold_in(key, 102), (PASSAGES, DIM), jnp.float32) * first_half)
    query_common = unit_rows(jax.random.normal(jax.random.fold_in(key, 103), (DIM,), jnp.float32) * second_half)
    passage_common = unit_rows(jax.random.normal(jax.random.fold_in(key, 104), (DIM,), jnp.float32) * second_half)
    return (chosen, directions, query_common, passage_common, first_half, second_half)


def draw_positive(key, part):
    return shared_parts(key)[0]


def draw_query_emb(key, part):
    chosen, directions, query_common, passage_common, first_half, second_half = shared_parts(key)
    spread = noise_level * DIM ** (-0.25) * (second_half + 0.25 * first_half)
    noise_key = jax.random.fold_in(key, 201)
    noise = jax.random.normal(noise_key, (QUERIES, QLEN, DIM), jnp.float32)
    common = query_common
    aligned = similar_gap / QLEN * directions[chosen]
    values = noise * spread + common + aligned[:, None, :]
    return jnp.clip(values, -6.0, 6.0).astype(jnp.bfloat16)


def draw_passage_emb(key, part):
    chosen, directions, query_common, passage_common, first_half, second_half = shared_parts(key)
    spread = noise_level * DIM ** (-0.25)
    noise_key = jax.random.fold_in(key, 301)
    noise = jax.random.normal(noise_key, (PASSAGES, PLEN, DIM), jnp.float32)
    common = passage_common
    values = noise * spread + common + directions[:, None, :]
    return jnp.clip(values, -6.0, 6.0).astype(jnp.bfloat16)


def touch_ends(entries, key, least, high):
    index_at = [jax.random.randint(jax.random.fold_in(key, axis), (), 0, length) for axis, length in enumerate(entries.shape)]
    widest = entries.shape.index(max(entries.shape))
    beside = index_at[:widest] + [(index_at[widest] + 1) % entries.shape[widest]] + index_at[widest + 1:]
    return entries.at[tuple(index_at)].set(least).at[tuple(beside)].set(high)


def levels(key, extent, split, smallest, high):
    def one(position, parts):
        heights = jax.random.uniform(jax.random.fold_in(jax.random.fold_in(key, 6), position), (parts,), jnp.float32, smallest / len(split), high / len(split))
        return jnp.repeat(jnp.exp(heights), extent[position] // parts).reshape((-1,) + (1,) * (len(extent) - position - 1))

    loudness = one(*split[0])
    for cut in split[1:]:
        loudness = loudness * one(*cut)
    return loudness


def bell_draw(key, extent, scale, most, split=(), dtype=jnp.bfloat16):
    loudness = levels(key, extent, split, -0.22, 0.18) if split else 1.0
    entries = jax.random.normal(key, extent, jnp.float32) * scale * loudness
    return jnp.minimum(jnp.maximum(entries, -most), most).astype(dtype)


def setup_inputs(seed: int = 0) -> dict:
    key_list = jax.random.split(jax.random.key(seed), 10)
    query_emb = draw_query_emb(jax.random.fold_in(key_list[9], 71), 0)
    positive = draw_positive(jax.random.fold_in(key_list[9], 71), 0)
    passage_emb = draw_passage_emb(jax.random.fold_in(key_list[9], 71), 0)
    lengths = touch_ends(jax.random.randint(key_list[3], (PASSAGES,), PLEN // 2, PLEN + 1), jax.random.fold_in(key_list[3], 1), PLEN // 2, PLEN).astype(jnp.int32)
    residual = bell_draw(key_list[4], (ROWS, D), 1.0, 6.0, ((0, 32),))
    context = bell_draw(key_list[5], (ROWS, D), 1.0, 6.0, ((0, 32),))
    out_proj = bell_draw(key_list[6], (D, D), D ** -0.5, 0.1875)
    norm_gain = jnp.clip(1.0 + 0.1 * jax.random.normal(key_list[7], (D,), jnp.float32), 0.5, 1.5)
    colbert_proj = bell_draw(key_list[8], (D, DIM), D ** -0.5, 0.1875)
    return {"query_emb": query_emb, "positive": positive, "passage_emb": passage_emb, "lengths": lengths, "residual": residual, "context": context, "out_proj": out_proj, "norm_gain": norm_gain, "colbert_proj": colbert_proj}


def masked_scores(query_flat, passage_tokens, length):
    scores = jnp.dot(query_flat, passage_tokens.T, preferred_element_type=jnp.float32)
    usable = (jnp.arange(passage_tokens.shape[0]) < length)[None, :]
    return jnp.where(usable, scores, -1e+30)

def window_rows(running, inputs, out_proj, norm_gain, colbert_proj):
    resid_rows, context_rows, grad_rows = inputs
    hidden = resid_rows.astype(jnp.float32) + jnp.dot(context_rows, out_proj, preferred_element_type=jnp.float32)
    row_mean = lax.optimization_barrier(jnp.mean(hidden, axis=1, keepdims=True))
    centred = hidden - row_mean
    variance = lax.optimization_barrier(jnp.mean(centred * centred, axis=1, keepdims=True))
    inv_std = 1.0 / jnp.sqrt(variance + 1e-05)
    normed = centred * inv_std
    scaled = (normed * norm_gain).astype(jnp.bfloat16)
    colbert_part = jnp.dot(scaled.T, grad_rows, preferred_element_type=jnp.float32)
    scaled_grad = jnp.dot(grad_rows, colbert_proj.T, preferred_element_type=jnp.float32)
    gain_part = lax.optimization_barrier(jnp.sum(scaled_grad * normed, axis=0))
    gained = scaled_grad * norm_gain
    hidden_grad = (inv_std * (gained - lax.optimization_barrier(jnp.mean(gained, axis=1, keepdims=True)) - normed * lax.optimization_barrier(jnp.mean(gained * normed, axis=1, keepdims=True)))).astype(jnp.bfloat16)
    context_grad = jnp.dot(hidden_grad, out_proj.T, preferred_element_type=jnp.float32).astype(jnp.bfloat16)
    proj_part = jnp.dot(context_rows.T, hidden_grad, preferred_element_type=jnp.float32)
    running = (running[0] + proj_part, running[1] + colbert_part, running[2] + gain_part)
    return (running, (hidden_grad, context_grad))

def reference(query_emb, positive, passage_emb, lengths, residual, context, out_proj, norm_gain, colbert_proj):
    query_flat = query_emb.reshape(QUERIES * QLEN, DIM)

    def forward(inputs):
        passage_tokens, length = inputs
        masked = masked_scores(query_flat, passage_tokens, length)
        highest = lax.optimization_barrier(jnp.max(masked, axis=1, keepdims=True))
        inner_lse = highest[:, 0] + jnp.log(lax.optimization_barrier(jnp.sum(jnp.exp(masked - highest), axis=1)))
        shifted = inner_lse - jnp.log(length.astype(jnp.float32))
        return (inner_lse, lax.optimization_barrier(jnp.sum(shifted.reshape(QUERIES, QLEN), axis=1)))
    inner_all, similar = lax.map(forward, (passage_emb, lengths))
    similar = similar.T
    highest = lax.optimization_barrier(jnp.max(similar, axis=1, keepdims=True))
    log_total = highest[:, 0] + jnp.log(lax.optimization_barrier(jnp.sum(jnp.exp(similar - highest), axis=1)))
    is_positive = jnp.arange(PASSAGES).astype(jnp.int32)[None, :] == positive[:, None]
    positive_score = lax.optimization_barrier(jnp.sum(jnp.where(is_positive, similar, 0.0), axis=1))
    loss = jnp.mean(log_total - positive_score)
    coefficient = jnp.exp(similar - log_total[:, None]) - is_positive.astype(jnp.float32)

    def backward(running, inputs):
        passage_tokens, length, inner_lse, column = inputs
        masked = masked_scores(query_flat, passage_tokens, length)
        spread = jnp.exp(masked - inner_lse[:, None]).reshape(QUERIES, QLEN, PLEN)
        weight = (spread * column[:, None, None]).reshape(QUERIES * QLEN, PLEN).astype(jnp.bfloat16)
        running = running + jnp.dot(weight, passage_tokens, preferred_element_type=jnp.float32)
        passage_grad = jnp.dot(weight.T, query_flat, preferred_element_type=jnp.float32).astype(jnp.bfloat16)
        return (running, passage_grad)
    start = jnp.zeros((QUERIES * QLEN, DIM), jnp.float32)
    query_sum, emb_grad = lax.scan(backward, start, (passage_emb, lengths, inner_all, coefficient.T))
    query_grad = query_sum.reshape(QUERIES, QLEN, DIM)

    def window_step(running, inputs):
        return window_rows(running, inputs, out_proj, norm_gain, colbert_proj)
    begin = (jnp.zeros((D, D), jnp.float32), jnp.zeros((D, DIM), jnp.float32), jnp.zeros((D,), jnp.float32))
    sums, grads = lax.scan(window_step, begin, (residual.reshape(PASSAGES, PLEN, D), context.reshape(PASSAGES, PLEN, D), emb_grad))
    residual_grad = grads[0].reshape(ROWS, D)
    context_grad = grads[1].reshape(ROWS, D)
    return (loss, query_grad, residual_grad, context_grad, sums[0], sums[1], sums[2])
```

```python
import functools

import jax
import jax.numpy as jnp
from jax import lax
from jax.experimental import pallas as pl
from jax.experimental.pallas import tpu as pltpu
from jax.sharding import PartitionSpec as P

MESH = pl.DeviceIdType.MESH
VMEM = pl.BlockSpec(memory_space=pltpu.VMEM)
SMEM = pl.BlockSpec(memory_space=pltpu.SMEM)
ANY = pl.BlockSpec(memory_space=pl.ANY)
LOW = -1e30
F32 = jnp.float32
BF16 = jnp.bfloat16
NT = (((1,), (1,)), ((), ()))
LAG = 3


def exact(a, b, dims=(((1,), (0,)), ((), ()))):
    return lax.dot_general(a, b, dims, precision=lax.Precision.HIGHEST, preferred_element_type=F32)


def each(size, act):
    def turn(k, carry):
        act(k)
        return carry

    lax.fori_loop(1, size, turn, 0)


def loop(low, high, act):
    def turn(k, carry):
        act(k)
        return carry

    lax.fori_loop(low, high, turn, 0)


def remote(src, dst, send, recv, device):
    return pltpu.make_async_remote_copy(
        src_ref=src, dst_ref=dst, send_sem=send, recv_sem=recv, device_id=device, device_id_type=MESH
    )


class Grid:
    def __init__(self, dp, neg):
        groups = neg // 2
        self.dp, self.neg = dp, neg
        self.a = 2 if groups % 2 == 0 else 1
        self.b = groups // self.a
        self.n1, self.n2, self.nz = self.b, self.a, dp
        self.turned = self.a == self.b
        self.n = dp * neg
        self.half = self.n // 2
        self.plane = self.n2 * self.nz

    def locate(self):
        self.r, self.col = lax.axis_index("dp"), lax.axis_index("neg")
        self.core = lax.rem(self.col, 2)
        g = self.col // 2
        self.y, self.x = g // self.b, lax.rem(g, self.b)
        self.me = self.r * self.neg + self.col

    def flip(self, core):
        return core if self.turned else 0 * core

    def own(self, core):
        f = self.flip(core)
        return (self.x * (1 - f) + self.y * f, self.y * (1 - f) + self.x * f)

    def column(self, j1, j2, core):
        f = self.flip(core)
        x, y = j1 * (1 - f) + j2 * f, j2 * (1 - f) + j1 * f
        return (y * self.b + x) * 2 + core

    def nearby(self, k):
        there, bit = self.r, 1
        while bit < self.nz:
            there = there + lax.rem(k // bit, 2) * bit * (1 - 2 * lax.rem(self.r // bit, 2))
            bit *= 2
        return there

    def arrival(self, i, core):
        i1, i2 = self.own(core)
        m2, m1, k = i // (self.n1 * self.nz), lax.rem(i // self.nz, self.n1), lax.rem(i, self.nz)
        return (self.nearby(k), lax.rem(i1 + m1, self.n1), lax.rem(i2 + m2, self.n2))

    def slot(self, rr, j1, j2, core):
        return rr * self.neg + self.column(j1, j2, core)


def main_kernel(dp, neg, own, per, query, positive, passage, lengths, resid, context, out_proj, gain, colbert,
                loss, query_grad, resid_grad, context_grad, sum_main, sum_col,
                q_all, msg, e_all, u_all, sums, inner, scale, bias, flipped, emb_acc,
                res_v, ctx_v, wo_v, cp_v, ctx_t, scaled_t, normed, inv_std, hg, cg,
                q_own, q_snd, q_pl, q_b1, q_l1, q_b2, q_l2, q_b3, q_l3,
                c_own, c_snd, c_pl, c_b1, c_l1, c_b2, c_l2, c_b3, c_l3,
                m_own, m_snd, m_pl, m_b1, m_l1, m_b2, m_l2, m_b3, m_l3,
                ld, zs, a1s, a2s, pps, agr, xs, xr, rs_s, rs_r, ag_s, ag_r, st):
    at = Grid(dp, neg)
    at.locate()
    r, core, me = at.r, at.core, at.me
    other = 1 - core
    i1, i2 = at.own(core)
    n, n1, n2, nz, half, plane = at.n, at.n1, at.n2, at.nz, at.half, at.plane
    place = (i1 * n2 + i2) * nz + r
    partner = (r, at.col + 1 - 2 * core)
    tok = own * per
    wide = n * own
    rows, width = resid.shape
    block = rows // 4
    chunks = sum_main.shape[0]
    cw = sum_main.shape[-1]

    def dev1(t):
        return (r, at.column(lax.rem(i1 + t, n1), i2, core))

    def dev2(t):
        return (r, at.column(i1, lax.rem(i2 + t, n2), core))

    def devz(k):
        return (lax.rem(r + k, nz), at.col)

    def any_device(k):
        d = lax.rem(me + k, n)
        return (d // neg, lax.rem(d, neg))

    loads = [
        pltpu.make_async_copy(context, ctx_v, ld.at[0]),
        pltpu.make_async_copy(out_proj, wo_v, ld.at[1]),
        pltpu.make_async_copy(resid, res_v, ld.at[2]),
        pltpu.make_async_copy(colbert, cp_v, ld.at[3]),
        pltpu.make_async_copy(query, q_all.at[me], ld.at[4]),
    ]
    for copy in loads:
        copy.start()
    barrier = pltpu.get_barrier_semaphore()
    each(n, lambda k: pl.semaphore_signal(barrier, inc=1, device_id=any_device(k), device_id_type=MESH))

    length = lengths[0]
    pas = passage[...]
    position = lax.broadcasted_iota(jnp.int32, bias.shape, 0)
    bias[...] = jnp.where(position < length, 0.0, LOW)
    flipped[...] = pas.astype(F32).T.astype(BF16)
    for copy in loads:
        copy.wait()

    def norm_block(i):
        at_row = pl.multiple_of(i * block, block)
        cut = pl.ds(at_row, block)
        ctx = ctx_v[cut, :]
        hidden = res_v[cut, :].astype(F32) + jnp.dot(ctx, wo_v[...], preferred_element_type=F32)
        centred = hidden - jnp.mean(hidden, axis=1, keepdims=True)
        variance = jnp.mean(centred * centred, axis=1, keepdims=True)
        inv = 1.0 / jnp.sqrt(variance + 1e-05)
        norm = centred * inv
        normed[cut, :] = norm
        inv_std[cut, :] = jnp.broadcast_to(inv, (block, inv_std.shape[1]))
        scaled_t[:, cut] = (norm * gain[...]).T.astype(BF16)
        ctx_t[:, cut] = ctx.astype(F32).T.astype(BF16)

    loop(0, 4, norm_block)
    pl.semaphore_wait(barrier, n - 1)

    def z_copy(k):
        return remote(q_all.at[me], q_all.at[me], zs.at[k], agr.at[me], devz(k))

    def a1_copy(s, rr, t):
        return remote(q_all.at[s], q_all.at[s], a1s.at[rr, t], agr.at[s], dev1(t))

    def a2_copy(s, rr, j1, t):
        return remote(q_all.at[s], q_all.at[s], a2s.at[rr * n1 + j1, t], agr.at[s], dev2(t))

    def pp_copy(s, rr, j1, j2):
        return remote(q_all.at[s], q_all.at[s], pps.at[(j1 * n2 + j2) * nz + rr], agr.at[s], partner)

    def landed(s):
        remote(q_all.at[s], q_all.at[s], zs.at[0], agr.at[s], partner).wait_recv()

    def forward(i):
        rr, j1, j2 = at.arrival(i, core)
        s = at.slot(rr, j1, j2, core)

        @pl.when(i < nz)
        def _():
            each(n1, lambda t: a1_copy(s, rr, t).start())

        @pl.when(i < nz * n1)
        def _():
            each(n2, lambda t: a2_copy(s, rr, j1, t).start())

        pp_copy(s, rr, j1, j2).start()

    def attend(s):
        scores = lax.dot_general(passage[...], q_all[s], NT, preferred_element_type=F32) + bias[...]
        highest = jnp.max(scores, axis=0, keepdims=True)
        spread = jnp.exp(scores - highest)
        total = jnp.sum(spread, axis=0, keepdims=True)
        low = spread.astype(BF16)
        e_all[s] = low
        sums[pl.ds(s, 1), :] = total
        inner[pl.ds(s, 1), :] = highest + jnp.log(total)
        u_all[s] = jnp.dot(flipped[...], low, preferred_element_type=F32)

    def attend_pair(i):
        attend(at.slot(*at.arrival(i, core), core))
        s = at.slot(*at.arrival(i, other), other)
        landed(s)
        attend(s)

    each(nz, lambda k: z_copy(k).start())
    forward(0)

    def relay(i):
        landed(at.slot(*at.arrival(i, core), core))
        forward(i)

        @pl.when(i >= LAG)
        def _():
            attend_pair(i - LAG)

    loop(1, half, relay)
    loop(half - LAG, half, attend_pair)

    token = lax.broadcasted_iota(jnp.int32, (tok, wide), 0)
    lane = lax.broadcasted_iota(jnp.int32, (tok, wide), 1)
    spots = jnp.where(token // per == lax.rem(lane, own), 1.0, 0.0)
    slot_of = lax.broadcasted_iota(jnp.int32, (n, wide), 0)
    lane_of = lax.broadcasted_iota(jnp.int32, (n, wide), 1)
    mine = slot_of == lane_of // own
    grouped = exact(inner[...], spots)
    similar = jnp.sum(jnp.where(mine, grouped, 0.0), axis=0, keepdims=True)
    shift = jnp.log(jnp.full((1, wide), length, jnp.int32).astype(F32)) * per
    row_lane = lax.broadcasted_iota(jnp.int32, (1, wide), 1)
    chosen = jnp.zeros((1, wide), jnp.int32)
    for i in range(own):
        chosen = chosen + jnp.where(row_lane == me * own + i, positive[i], 0)
    msg[me, :, :wide] = similar - shift
    msg[me, :, wide:] = chosen.astype(F32)

    def msg_copy(k, slot):
        return remote(msg.at[slot], msg.at[slot], xs.at[k], xr.at[k], any_device(k))

    each(n, lambda k: msg_copy(k, me).start())
    each(n, lambda k: msg_copy(k, lax.rem(me - k + n, n)).wait_recv())

    everyone = msg[:, :, :wide]
    picked = jnp.sum(msg[:, :, wide:], axis=0)
    highest = jnp.max(everyone, axis=0)
    log_total = highest + jnp.log(jnp.sum(jnp.exp(everyone - highest[None]), axis=0))
    which = lax.broadcasted_iota(jnp.int32, everyone.shape, 0).astype(F32)
    score = jnp.sum(jnp.where(which == picked[None], everyone, 0.0), axis=0)
    average = jnp.sum(log_total - score, axis=1, keepdims=True) / wide
    loss[...] = jnp.broadcast_to(average, loss.shape)
    hit = jnp.where(picked == me.astype(F32), 1.0, 0.0)
    coefficient = jnp.exp(similar - shift - log_total) - hit
    laid = jnp.where(mine, jnp.broadcast_to(coefficient, mine.shape), 0.0)
    scale[...] = exact(laid, spots, NT) / sums[...]

    jobs = [(q_own, q_snd, q_pl, q_b1, q_l1, q_b2, q_l2, q_b3, q_l3, None)]
    jobs += [(c_own, c_snd, c_pl, c_b1, c_l1, c_b2, c_l2, c_b3, c_l3, sum_col)]
    for k in range(chunks):
        jobs.append((m_own.at[k], m_snd.at[k], m_pl.at[k], m_b1.at[k], m_l1.at[k], m_b2.at[k], m_l2.at[k],
                     m_b3.at[k], m_l3.at[k], sum_main.at[k]))

    def pair_copy(j):
        return remote(jobs[j][1], jobs[j][2], rs_s.at[j, 0, 0], rs_r.at[j, 0, 0], partner)

    def rs1_copy(j, t):
        there = pl.ds(lax.rem(i1 + t, n1) * plane, plane)
        return remote(jobs[j][3].at[there], jobs[j][4].at[t], rs_s.at[j, 1, t], rs_r.at[j, 1, t], dev1(t))

    def rs2_copy(j, t):
        there = pl.ds(lax.rem(i2 + t, n2) * nz, nz)
        return remote(jobs[j][5].at[there], jobs[j][6].at[t], rs_s.at[j, 2, t], rs_r.at[j, 2, t], dev2(t))

    def rs3_copy(j, k):
        return remote(jobs[j][7].at[lax.rem(r + k, nz)], jobs[j][8].at[k], rs_s.at[j, 3, k], rs_r.at[j, 3, k], devz(k))

    def ag3_copy(j, k, here):
        piece = jobs[j][9].at[core, here]
        return remote(piece, piece, ag_s.at[j, 0, k], ag_r.at[j, 0, k], devz(k))

    def ag2_copy(j, t, j2):
        piece = jobs[j][9].at[core, pl.ds((i1 * n2 + j2) * nz, nz)]
        return remote(piece, piece, ag_s.at[j, 1, t], ag_r.at[j, 1, t], dev2(t))

    def ag1_copy(j, t, j1):
        piece = jobs[j][9].at[core, pl.ds(j1 * plane, plane)]
        return remote(piece, piece, ag_s.at[j, 2, t], ag_r.at[j, 2, t], dev1(t))

    def ag0_copy(j, c):
        piece = jobs[j][9].at[c]
        return remote(piece, piece, ag_s.at[j, 3, 0], ag_r.at[j, 3, 0], partner)

    def step1(j):
        pair_copy(j).wait_recv()
        job = jobs[j]
        job[3][...] = (job[0][...].astype(F32) + job[2][...].astype(F32)).astype(BF16)
        for t in range(1, n1):
            rs1_copy(j, t).start()

    def step2(j):
        job = jobs[j]
        total = job[3][pl.ds(i1 * plane, plane)].astype(F32)
        for t in range(1, n1):
            rs1_copy(j, t).wait_recv()
            total = total + job[4][t].astype(F32)
        job[5][...] = total.astype(BF16)
        for t in range(1, n2):
            rs2_copy(j, t).start()

    def step3(j):
        job = jobs[j]
        total = job[5][pl.ds(i2 * nz, nz)].astype(F32)
        for t in range(1, n2):
            rs2_copy(j, t).wait_recv()
            total = total + job[6][t].astype(F32)
        job[7][...] = total.astype(BF16)
        for k in range(1, nz):
            rs3_copy(j, k).start()

    def step4(j):
        job = jobs[j]
        total = job[7][r].astype(F32)
        for k in range(1, nz):
            rs3_copy(j, k).wait_recv()
            total = total + job[8][k].astype(F32)
        if job[9] is None:
            query_grad[...] = total.T
        else:
            job[9][core, place] = total.astype(BF16)
            for k in range(1, nz):
                ag3_copy(j, k, place).start()

    def step5(j):
        if jobs[j][9] is None:
            return
        for k in range(1, nz):
            ag3_copy(j, k, (i1 * n2 + i2) * nz + lax.rem(r - k + nz, nz)).wait_recv()
        for t in range(1, n2):
            ag2_copy(j, t, i2).start()

    def step6(j):
        if jobs[j][9] is None:
            return
        for t in range(1, n2):
            ag2_copy(j, t, lax.rem(i2 - t + n2, n2)).wait_recv()
        for t in range(1, n1):
            ag1_copy(j, t, i1).start()

    def step7(j):
        if jobs[j][9] is None:
            return
        for t in range(1, n1):
            ag1_copy(j, t, lax.rem(i1 - t + n1, n1)).wait_recv()
        ag0_copy(j, core).start()

    def step8(j):
        if jobs[j][9] is None:
            return
        ag0_copy(j, other).wait_recv()

    def query_term(p, parity, into):
        j1, j2, rr = p // plane, lax.rem(p // nz, n2), lax.rem(p, nz)
        s = at.slot(rr, j1, j2, parity)
        into[p] = (u_all[s] * scale[pl.ds(s, 1), :]).astype(BF16)

    loop(0, half, lambda p: query_term(p, other, q_snd))
    pair_copy(0).start()

    emb_acc[...] = jnp.zeros_like(emb_acc)

    def emb_term(u):
        parts = []
        for v in range(4):
            s = u * 4 + v
            parts.append((e_all[s].astype(F32) * scale[pl.ds(s, 1), :]).astype(BF16))
        weight = jnp.concatenate(parts, axis=1)
        tokens = q_all[pl.ds(u * 4, 4)].reshape(4 * tok, q_all.shape[2])
        emb_acc[...] += jnp.dot(weight, tokens, preferred_element_type=F32)

    loop(0, n // 4, emb_term)
    emb = emb_acc[...].astype(BF16)
    loop(0, half, lambda p: query_term(p, core, q_own))

    def halves(j, own_half, snd_half):
        jobs[j][1][...] = snd_half.reshape(jobs[j][1].shape).astype(BF16)
        pair_copy(j).start()
        jobs[j][0][...] = own_half.reshape(jobs[j][0].shape).astype(BF16)

    mid = width // 2
    other_rows = pl.ds(pl.multiple_of(other * mid, mid), mid)
    own_rows = pl.ds(pl.multiple_of(core * mid, mid), mid)
    halves(1, jnp.dot(scaled_t[own_rows, :], emb, preferred_element_type=F32),
           jnp.dot(scaled_t[other_rows, :], emb, preferred_element_type=F32))
    step1(0)

    emb_acc[...] = emb.astype(F32)

    def grad_block(i):
        cut = pl.ds(pl.multiple_of(i * block, block), block)
        scaled_grad = lax.dot_general(emb_acc[cut, :].astype(BF16), cp_v[...], NT, preferred_element_type=F32)
        gained = scaled_grad * gain[...]
        norm = normed[cut, :]
        hidden_grad = inv_std[cut, 0:1] * (
            gained
            - jnp.mean(gained, axis=1, keepdims=True)
            - norm * jnp.mean(gained * norm, axis=1, keepdims=True)
        )
        hg[cut, :] = hidden_grad.astype(BF16)

    loop(0, 4, grad_block)
    stores = [pltpu.make_async_copy(hg, resid_grad, st.at[0]), pltpu.make_async_copy(cg, context_grad, st.at[1])]
    stores[0].start()

    steps = [step1, step2, step3, step4, step5, step6, step7, step8]
    done = {0: 1, 1: 0}

    def advance():
        for j in sorted(done):
            if done[j] < len(steps):
                steps[done[j]](j)
                done[j] += 1

    def context_block(i):
        cut = pl.ds(i * block, block)
        cg[cut, :] = lax.dot_general(hg[cut, :], wo_v[...], NT, preferred_element_type=F32).astype(BF16)

    for k in range(chunks):
        columns = slice(k * cw, (k + 1) * cw)
        halves(2 + k, jnp.dot(ctx_t[own_rows, :], hg[:, columns], preferred_element_type=F32),
               jnp.dot(ctx_t[other_rows, :], hg[:, columns], preferred_element_type=F32))
        advance()
        done[2 + k] = 0
    for i in range(4):
        context_block(i)
        advance()
    stores[1].start()
    while any(done[j] < len(steps) for j in done):
        advance()
    for copy in stores:
        copy.wait()

    each(nz, lambda k: z_copy(k).wait_send())

    def drain(i):
        rr, j1, j2 = at.arrival(i, core)
        s = at.slot(rr, j1, j2, core)

        @pl.when(i < nz)
        def _():
            each(n1, lambda t: a1_copy(s, rr, t).wait_send())

        @pl.when(i < nz * n1)
        def _():
            each(n2, lambda t: a2_copy(s, rr, j1, t).wait_send())

        pp_copy(s, rr, j1, j2).wait_send()

    loop(0, half, drain)
    each(n, lambda k: msg_copy(k, me).wait_send())
    for j in range(len(jobs)):
        pair_copy(j).wait_send()
        for t in range(1, n1):
            rs1_copy(j, t).wait_send()
        for t in range(1, n2):
            rs2_copy(j, t).wait_send()
        for k in range(1, nz):
            rs3_copy(j, k).wait_send()
        if jobs[j][9] is not None:
            for k in range(1, nz):
                ag3_copy(j, k, place).wait_send()
            for t in range(1, n2):
                ag2_copy(j, t, i2).wait_send()
            for t in range(1, n1):
                ag1_copy(j, t, i1).wait_send()
            ag0_copy(j, core).wait_send()


def finish_kernel(main, col, gain, colbert, proj_grad, colbert_grad, gain_grad):
    chunks, rows, cw = main.shape
    for k in range(chunks):
        proj_grad[:, k * cw : (k + 1) * cw] = main[k].astype(F32)
    wide = col[...].astype(F32)
    colbert_grad[...] = wide
    ones = jnp.ones((8, wide.shape[1]), F32)
    summed = exact(ones, wide * colbert[...].astype(F32), NT)
    gain_grad[...] = summed[0:1, :] / gain[...]


def job_buffers(at, piece, cols, lead=()):
    shapes = [
        (at.half, piece, cols),
        (at.half, piece, cols),
        (at.half, piece, cols),
        (at.half, piece, cols),
        (at.n1, at.plane, piece, cols),
        (at.plane, piece, cols),
        (at.n2, at.nz, piece, cols),
        (at.nz, piece, cols),
        (at.nz, piece, cols),
    ]
    return [pltpu.VMEM(lead + shape, BF16) for shape in shapes]


def body(sizes, query_emb, positive, passage_emb, lengths, residual, context, out_proj, norm_gain, colbert_proj):
    dp, neg = sizes["dp"], sizes["neg"]
    at = Grid(dp, neg)
    own, per, dim = query_emb.shape
    plen = passage_emb.shape[1]
    rows, width = residual.shape
    tok = own * per
    n = at.n
    chunks = 4
    cw = width // chunks
    piece = width // (2 * at.half)
    dma = pltpu.SemaphoreType.DMA
    vm = pltpu.VMEM
    most = max(at.n1, at.n2, at.nz)
    scratch = [
        vm((n, tok, dim), BF16),
        vm((n, 1, 2 * n * own), F32),
        vm((n, plen, tok), BF16),
        vm((n, dim, tok), F32),
        vm((n, tok), F32),
        vm((n, tok), F32),
        vm((n, tok), F32),
        vm((plen, tok), F32),
        vm((dim, plen), BF16),
        vm((plen, dim), F32),
        vm((rows, width), BF16),
        vm((rows, width), BF16),
        vm((width, width), BF16),
        vm((width, dim), BF16),
        vm((width, rows), BF16),
        vm((width, rows), BF16),
        vm((rows, width), F32),
        vm((rows, 128), F32),
        vm((rows, width), BF16),
        vm((rows, width), BF16),
    ]
    scratch += job_buffers(at, dim, tok)
    scratch += job_buffers(at, piece, dim)
    scratch += job_buffers(at, piece, cw, (chunks,))
    scratch += [
        dma((5,)),
        dma((at.nz,)),
        dma((at.nz, at.n1)),
        dma((at.nz * at.n1, at.n2)),
        dma((at.half,)),
        dma((n,)),
        dma((n,)),
        dma((n,)),
        dma((chunks + 2, 4, most)),
        dma((chunks + 2, 4, most)),
        dma((chunks + 2, 4, most)),
        dma((chunks + 2, 4, most)),
        dma((2,)),
    ]
    loss, query_grad, resid_grad, context_grad, sum_main, sum_col = pl.pallas_call(
        functools.partial(main_kernel, dp, neg, own, per),
        out_shape=[
            jax.ShapeDtypeStruct((1, 128), F32),
            jax.ShapeDtypeStruct((tok, dim), F32),
            jax.ShapeDtypeStruct((rows, width), BF16),
            jax.ShapeDtypeStruct((rows, width), BF16),
            jax.ShapeDtypeStruct((chunks, 2, at.half, piece, cw), BF16),
            jax.ShapeDtypeStruct((2, at.half, piece, dim), BF16),
        ],
        in_specs=[VMEM, SMEM, VMEM, SMEM, ANY, ANY, ANY, VMEM, ANY],
        out_specs=[VMEM, VMEM, ANY, ANY, VMEM, VMEM],
        scratch_shapes=scratch,
        compiler_params=pltpu.CompilerParams(
            collective_id=1, has_side_effects=True, vmem_limit_bytes=67043328
        ),
        name="maxsim_main",
    )(
        query_emb.reshape(tok, dim),
        positive,
        passage_emb.reshape(plen, dim),
        lengths,
        residual,
        context,
        out_proj,
        norm_gain[None, :],
        colbert_proj,
    )
    proj_grad, colbert_grad, gain_grad = pl.pallas_call(
        finish_kernel,
        out_shape=[
            jax.ShapeDtypeStruct((width, width), F32),
            jax.ShapeDtypeStruct((width, dim), F32),
            jax.ShapeDtypeStruct((1, width), F32),
        ],
        in_specs=[VMEM] * 4,
        out_specs=[VMEM] * 3,
        name="maxsim_finish",
    )(
        sum_main.reshape(chunks, width, cw),
        sum_col.reshape(width, dim),
        norm_gain[None, :],
        colbert_proj,
    )
    return (
        loss[0, 0],
        query_grad.reshape(own, per, dim),
        resid_grad,
        context_grad,
        proj_grad,
        colbert_grad,
        gain_grad.reshape(width),
    )


def solution(mesh):
    sizes = {axis: mesh.shape[axis] for axis in ("dp", "neg")}
    split = ("dp", "neg")
    in_specs = (
        P(split, None, None),
        P(split),
        P(split, None, None),
        P(split),
        P(split, None),
        P(split, None),
        P(),
        P(),
        P(),
    )
    out_specs = (
        P(),
        P(split, None, None),
        P(split, None),
        P(split, None),
        P(),
        P(),
        P(),
    )
    return jax.shard_map(
        functools.partial(body, sizes), mesh=mesh, in_specs=in_specs, out_specs=out_specs, check_vma=False
    )
```

```python
import functools
import math

import jax
import jax.numpy as jnp
from jax import lax
from jax.experimental import pallas as pl
from jax.experimental.pallas import tpu as pltpu
from jax.sharding import PartitionSpec as P

MESH = pl.DeviceIdType.MESH
VMEM = pl.BlockSpec(memory_space=pltpu.VMEM)
SMEM = pl.BlockSpec(memory_space=pltpu.SMEM)
ANY = pl.BlockSpec(memory_space=pl.ANY)
HBM = pl.BlockSpec(memory_space=pltpu.HBM)
LOW = -1e30
F32 = jnp.float32
BF16 = jnp.bfloat16
NT = (((1,), (1,)), ((), ()))
LAG = 1


def exact(a, b, dims=(((1,), (0,)), ((), ()))):
    return lax.dot_general(a, b, dims, precision=lax.Precision.HIGHEST, preferred_element_type=F32)


def each(size, act):
    def turn(k, carry):
        act(k)
        return carry

    lax.fori_loop(1, size, turn, 0)


def loop(low, high, act):
    def turn(k, carry):
        act(k)
        return carry

    lax.fori_loop(low, high, turn, 0)


def remote(src, dst, send, recv, device):
    return pltpu.make_async_remote_copy(
        src_ref=src, dst_ref=dst, send_sem=send, recv_sem=recv, device_id=device, device_id_type=MESH
    )


class Grid:
    def __init__(self, dp, neg):
        groups = neg // 2
        self.dp, self.neg = dp, neg
        self.a = 2 if groups % 2 == 0 else 1
        self.b = groups // self.a
        self.n1, self.n2, self.nz = self.b, self.a, dp
        self.turned = self.a == self.b
        self.n = dp * neg
        self.half = self.n // 2
        self.plane = self.n2 * self.nz

    def locate(self):
        self.r, self.col = lax.axis_index("dp"), lax.axis_index("neg")
        self.core = lax.rem(self.col, 2)
        g = self.col // 2
        self.y, self.x = g // self.b, lax.rem(g, self.b)
        self.me = self.r * self.neg + self.col

    def flip(self, core):
        return core if self.turned else 0 * core

    def own(self, core):
        f = self.flip(core)
        return (self.x * (1 - f) + self.y * f, self.y * (1 - f) + self.x * f)

    def column(self, j1, j2, core):
        f = self.flip(core)
        x, y = j1 * (1 - f) + j2 * f, j2 * (1 - f) + j1 * f
        return (y * self.b + x) * 2 + core

    def nearby(self, k):
        there, bit = self.r, 1
        while bit < self.nz:
            there = there + lax.rem(k // bit, 2) * bit * (1 - 2 * lax.rem(self.r // bit, 2))
            bit *= 2
        return there

    def arrival(self, i, core):
        i1, i2 = self.own(core)
        m2, m1, k = i // (self.n1 * self.nz), lax.rem(i // self.nz, self.n1), lax.rem(i, self.nz)
        return (self.nearby(k), lax.rem(i1 + m1, self.n1), lax.rem(i2 + m2, self.n2))

    def slot(self, rr, j1, j2, core):
        return rr * self.neg + self.column(j1, j2, core)


def main_kernel(dp, neg, own, per, query, positive_in, passage, lengths, resid, context, out_proj, gain_in, colbert,
                loss, query_grad, resid_grad, context_grad, sum_main, sum_col,
                q_all, msg, e_all, u_all, sums, inner, scale, bias, pas_v, flipped, emb_acc,
                positive, gain, wo_v, cp_v, ctx_t, scaled_t, normed, inv_std, *rest):
    at = Grid(dp, neg)
    at.locate()
    r, core, me = at.r, at.core, at.me
    other = 1 - core
    i1, i2 = at.own(core)
    n, n1, n2, nz, half, plane = at.n, at.n1, at.n2, at.nz, at.half, at.plane
    place = (i1 * n2 + i2) * nz + r
    partner = (r, at.col + 1 - 2 * core)
    tok = own * per
    wide = n * own
    rows, width = resid.shape
    block = rows // 4
    chunks = sum_main.shape[0]
    cw = sum_main.shape[-1]
    count = len(JOB)
    sems = rest[3 * count :]
    ld, zs, a1s, a2s, pps, agr, xs, xr, rs_s, rs_r, ag_s, ag_r = sems

    def dev1(t):
        return (r, at.column(lax.rem(i1 + t, n1), i2, core))

    def dev2(t):
        return (r, at.column(i1, lax.rem(i2 + t, n2), core))

    def devz(k):
        return (lax.rem(r + k, nz), at.col)

    def any_device(k):
        d = lax.rem(me + k, n)
        return (d // neg, lax.rem(d, neg))

    barrier = pltpu.get_barrier_semaphore()

    def greet(device):
        pl.semaphore_signal(barrier, inc=1, device_id=device, device_id_type=MESH)

    each(nz, lambda k: greet(devz(k)))
    each(n1, lambda t: greet(dev1(t)))
    each(n2, lambda t: greet(dev2(t)))
    greet(partner)
    loads = [
        pltpu.make_async_copy(query, q_all.at[me], ld.at[0]),
        pltpu.make_async_copy(passage, pas_v, ld.at[1]),
        pltpu.make_async_copy(context, context_grad, ld.at[2]),
        pltpu.make_async_copy(out_proj, wo_v, ld.at[3]),
        pltpu.make_async_copy(resid, resid_grad, ld.at[4]),
        pltpu.make_async_copy(colbert, cp_v, ld.at[5]),
        pltpu.make_async_copy(gain_in, gain, ld.at[7]),
        pltpu.make_async_copy(positive_in, positive, ld.at[8]),
    ]
    for copy in loads:
        copy.start()
    loads[0].wait()
    pl.semaphore_wait(barrier, nz + n1 + n2 - 2)

    def z_copy(k):
        return remote(q_all.at[me], q_all.at[me], zs.at[k], agr.at[me], devz(k))

    def a1_copy(s, rr, t):
        return remote(q_all.at[s], q_all.at[s], a1s.at[rr, t], agr.at[s], dev1(t))

    def a2_copy(s, rr, j1, t):
        return remote(q_all.at[s], q_all.at[s], a2s.at[rr * n1 + j1, t], agr.at[s], dev2(t))

    def pp_copy(s, rr, j1, j2):
        return remote(q_all.at[s], q_all.at[s], pps.at[(j1 * n2 + j2) * nz + rr], agr.at[s], partner)

    def landed(s):
        remote(q_all.at[s], q_all.at[s], zs.at[0], agr.at[s], partner).wait_recv()

    def route(i, act):
        rr, j1, j2 = at.arrival(i, core)
        s = at.slot(rr, j1, j2, core)

        @pl.when(i < nz)
        def _():
            each(n1, lambda t: act(a1_copy(s, rr, t)))

        @pl.when(i < nz * n1)
        def _():
            each(n2, lambda t: act(a2_copy(s, rr, j1, t)))

        act(pp_copy(s, rr, j1, j2))

    def attend(slots):
        tokens = jnp.concatenate([q_all[s] for s in slots], axis=0)
        scores = lax.dot_general(pas_v[...], tokens, NT, preferred_element_type=F32) + bias[...]
        highest = jnp.max(scores, axis=0, keepdims=True)
        spread = jnp.exp(scores - highest)
        total = jnp.sum(spread, axis=0, keepdims=True)
        low = spread.astype(BF16)
        level = highest + jnp.log(total)
        below = jnp.dot(flipped[...], low, preferred_element_type=F32)
        for v, s in enumerate(slots):
            cut = slice(v * tok, (v + 1) * tok)
            e_all[s] = low[:, cut]
            sums[pl.ds(s, 1), :] = total[:, cut]
            inner[pl.ds(s, 1), :] = level[:, cut]
            u_all[s] = below[:, cut]

    def attend_group(u):
        mine = [at.slot(*at.arrival(2 * u + v, core), core) for v in range(2)]
        theirs = [at.slot(*at.arrival(2 * u + v, other), other) for v in range(2)]
        for s in theirs:
            landed(s)
        attend(mine)
        attend(theirs)

    each(nz, lambda k: z_copy(k).start())
    route(0, lambda copy: copy.start())
    loads[1].wait()
    length = lengths[0]
    position = lax.broadcasted_iota(jnp.int32, bias.shape, 0)
    bias[...] = jnp.where(position < length, 0.0, LOW)
    flipped[...] = pas_v[...].astype(F32).T.astype(BF16)

    def relay(i):
        landed(at.slot(*at.arrival(i, core), core))
        route(i, lambda copy: copy.start())

    def relay_group(u):
        @pl.when(u > 0)
        def _():
            relay(2 * u)

        relay(2 * u + 1)

        @pl.when(u >= LAG)
        def _():
            attend_group(u - LAG)

    loop(0, half // 2, relay_group)
    loop(half // 2 - LAG, half // 2, attend_group)

    loads[7].wait()
    token = lax.broadcasted_iota(jnp.int32, (tok, wide), 0)
    lane = lax.broadcasted_iota(jnp.int32, (tok, wide), 1)
    spots = jnp.where(token // per == lax.rem(lane, own), 1.0, 0.0)
    slot_of = lax.broadcasted_iota(jnp.int32, (n, wide), 0)
    lane_of = lax.broadcasted_iota(jnp.int32, (n, wide), 1)
    mine = slot_of == lane_of // own
    grouped = exact(inner[...], spots)
    similar = jnp.sum(jnp.where(mine, grouped, 0.0), axis=0, keepdims=True)
    shift = jnp.log(jnp.full((1, wide), length, jnp.int32).astype(F32)) * per
    row_lane = lax.broadcasted_iota(jnp.int32, (1, wide), 1)
    chosen = jnp.zeros((1, wide), jnp.int32)
    for i in range(own):
        chosen = chosen + jnp.where(row_lane == me * own + i, positive[i], 0)
    msg[me, :, :wide] = similar - shift
    msg[me, :, wide:] = chosen.astype(F32)

    def msg_copy(k, slot):
        return remote(msg.at[slot], msg.at[slot], xs.at[k], xr.at[k], any_device(k))

    each(n, lambda k: msg_copy(k, me).start())

    for copy in loads[2:7]:
        copy.wait()

    def norm_block(i):
        cut = pl.ds(pl.multiple_of(i * block, block), block)
        ctx = context_grad[cut, :]
        hidden = resid_grad[cut, :].astype(F32) + jnp.dot(ctx, wo_v[...], preferred_element_type=F32)
        centred = hidden - jnp.mean(hidden, axis=1, keepdims=True)
        variance = jnp.mean(centred * centred, axis=1, keepdims=True)
        inv = 1.0 / jnp.sqrt(variance + 1e-05)
        norm = centred * inv
        normed[cut, :] = norm
        inv_std[cut, :] = jnp.broadcast_to(inv, (block, inv_std.shape[1]))
        scaled_t[:, cut] = (norm * gain[...]).T.astype(BF16)
        ctx_t[:, cut] = ctx.astype(F32).T.astype(BF16)

    loop(0, 4, norm_block)
    each(nz, lambda k: z_copy(k).wait_send())
    loop(0, half, lambda i: route(i, lambda copy: copy.wait_send()))
    each(n, lambda k: msg_copy(k, lax.rem(me - k + n, n)).wait_recv())

    everyone = msg[:, :, :wide]
    picked = jnp.sum(msg[:, :, wide:], axis=0)
    highest = jnp.max(everyone, axis=0)
    log_total = highest + jnp.log(jnp.sum(jnp.exp(everyone - highest[None]), axis=0))
    which = lax.broadcasted_iota(jnp.int32, everyone.shape, 0).astype(F32)
    score = jnp.sum(jnp.where(which == picked[None], everyone, 0.0), axis=0)
    average = jnp.sum(log_total - score, axis=1, keepdims=True) / wide
    loss[...] = jnp.broadcast_to(average, loss.shape)
    hit = jnp.where(picked == me.astype(F32), 1.0, 0.0)
    coefficient = jnp.exp(similar - shift - log_total) - hit
    laid = jnp.where(mine, jnp.broadcast_to(coefficient, mine.shape), 0.0)
    scale[...] = exact(laid, spots, NT) / sums[...]

    jobs = []
    for which_job, out in ((0, None), (1, sum_col)):
        jobs.append(dict(zip(JOB, rest[which_job * count : (which_job + 1) * count]), out=out))
    for k in range(chunks):
        jobs.append(dict(zip(JOB, [ref.at[k] for ref in rest[2 * count : 3 * count]]), out=sum_main.at[k]))

    def pair_copy(j):
        return remote(jobs[j]["snd"], jobs[j]["pl"], rs_s.at[j, 0, 0], rs_r.at[j, 0, 0], partner)

    def rs1_copy(j, t):
        there = pl.ds(lax.rem(i1 + t, n1) * plane, plane)
        return remote(jobs[j]["b1"].at[there], jobs[j]["l1"].at[t], rs_s.at[j, 1, t], rs_r.at[j, 1, t], dev1(t))

    def rs2_copy(j, t):
        there = pl.ds(lax.rem(i2 + t, n2) * nz, nz)
        return remote(jobs[j]["b2"].at[there], jobs[j]["l2"].at[t], rs_s.at[j, 2, t], rs_r.at[j, 2, t], dev2(t))

    def rs3_copy(j, k):
        return remote(jobs[j]["b3"].at[lax.rem(r + k, nz)], jobs[j]["l3"].at[k], rs_s.at[j, 3, k], rs_r.at[j, 3, k], devz(k))

    def ag3_copy(j, k, here):
        piece = jobs[j]["out"].at[core, here]
        return remote(piece, piece, ag_s.at[j, 0, k], ag_r.at[j, 0, k], devz(k))

    def ag2_copy(j, t, j2):
        piece = jobs[j]["out"].at[core, pl.ds((i1 * n2 + j2) * nz, nz)]
        return remote(piece, piece, ag_s.at[j, 1, t], ag_r.at[j, 1, t], dev2(t))

    def ag1_copy(j, t, j1):
        piece = jobs[j]["out"].at[core, pl.ds(j1 * plane, plane)]
        return remote(piece, piece, ag_s.at[j, 2, t], ag_r.at[j, 2, t], dev1(t))

    def ag0_copy(j, c):
        piece = jobs[j]["out"].at[c]
        return remote(piece, piece, ag_s.at[j, 3, 0], ag_r.at[j, 3, 0], partner)

    def step1(j):
        job = jobs[j]
        pair_copy(j).wait_recv()
        if j > 0:
            job["b1"][...] = (job["own"][...] + job["pl"][...].astype(F32)).astype(BF16)
            kept = pl.ds(i1 * plane, plane)
            job["k1"][...] = job["own"][kept] + job["pl"][kept].astype(F32)
        else:

            def send_term(p):
                j1, j2, rr = p // plane, lax.rem(p // nz, n2), lax.rem(p, nz)
                s = at.slot(rr, j1, j2, core)
                total = u_all[s] * scale[pl.ds(s, 1), :] + job["pl"][p].astype(F32)
                job["b1"][p] = total.astype(BF16)

            def keep_term(q):
                p = i1 * plane + q
                j1, j2, rr = p // plane, lax.rem(p // nz, n2), lax.rem(p, nz)
                s = at.slot(rr, j1, j2, core)
                job["k1"][q] = u_all[s] * scale[pl.ds(s, 1), :] + job["pl"][p].astype(F32)

            loop(plane, half, lambda p: send_term(lax.rem(i1 * plane + p, half)))
            loop(0, plane, keep_term)
        for t in range(1, n1):
            rs1_copy(j, t).start()

    def step2(j):
        job = jobs[j]
        total = job["k1"][...]
        for t in range(1, n1):
            rs1_copy(j, t).wait_recv()
            total = total + job["l1"][t].astype(F32)
        job["b2"][...] = total.astype(BF16)
        job["k1"][...] = total
        for t in range(1, n2):
            rs2_copy(j, t).start()

    def step3(j):
        job = jobs[j]
        total = job["k1"][pl.ds(i2 * nz, nz)]
        for t in range(1, n2):
            rs2_copy(j, t).wait_recv()
            total = total + job["l2"][t].astype(F32)
        job["b3"][...] = total.astype(BF16)
        job["k2"][...] = total
        for k in range(1, nz):
            rs3_copy(j, k).start()

    def step4(j):
        job = jobs[j]
        total = job["k2"][r]
        for k in range(1, nz):
            rs3_copy(j, k).wait_recv()
            total = total + job["l3"][k].astype(F32)
        if job["out"] is None:
            query_grad[...] = total.T
        else:
            job["out"][core, place] = total.astype(BF16)
            for k in range(1, nz):
                ag3_copy(j, k, place).start()

    def step5(j):
        for k in range(1, nz):
            ag3_copy(j, k, (i1 * n2 + i2) * nz + lax.rem(r - k + nz, nz)).wait_recv()
        for t in range(1, n2):
            ag2_copy(j, t, i2).start()

    def step6(j):
        for t in range(1, n2):
            ag2_copy(j, t, lax.rem(i2 - t + n2, n2)).wait_recv()
        for t in range(1, n1):
            ag1_copy(j, t, i1).start()

    def step7(j):
        for t in range(1, n1):
            ag1_copy(j, t, lax.rem(i1 - t + n1, n1)).wait_recv()
        ag0_copy(j, core).start()

    def step8(j):
        ag0_copy(j, other).wait_recv()

    def drain_sum(j):
        pair_copy(j).wait_send()
        for t in range(1, n1):
            rs1_copy(j, t).wait_send()
        for t in range(1, n2):
            rs2_copy(j, t).wait_send()
        for k in range(1, nz):
            rs3_copy(j, k).wait_send()

    def drain_out(j):
        for k in range(1, nz):
            ag3_copy(j, k, place).wait_send()
        for t in range(1, n2):
            ag2_copy(j, t, i2).wait_send()
        for t in range(1, n1):
            ag1_copy(j, t, i1).wait_send()
        ag0_copy(j, core).wait_send()

    def query_term(p):
        j1, j2, rr = p // plane, lax.rem(p // nz, n2), lax.rem(p, nz)
        s = at.slot(rr, j1, j2, other)
        jobs[0]["snd"][p] = (u_all[s] * scale[pl.ds(s, 1), :]).astype(BF16)

    loop(0, half, query_term)
    pair_copy(0).start()

    emb_acc[...] = jnp.zeros_like(emb_acc)

    def emb_term(u):
        parts = []
        for v in range(8):
            s = u * 8 + v
            row = jnp.broadcast_to(scale[pl.ds(s, 1), :], (16, tok)).astype(BF16)
            spread = e_all[s]
            parts.append((spread.reshape(-1, 16, tok) * row[None]).reshape(spread.shape))
        weight = jnp.concatenate(parts, axis=1)
        tokens = q_all[pl.ds(u * 8, 8)].reshape(8 * tok, q_all.shape[2])
        emb_acc[...] += jnp.dot(weight, tokens, preferred_element_type=F32)

    loop(0, n // 8, emb_term)
    emb = emb_acc[...].astype(BF16)

    def halves(j, left, right):
        job = jobs[j]
        job["snd"][...] = jnp.dot(left(other), right, preferred_element_type=F32).reshape(job["snd"].shape).astype(BF16)
        pair_copy(j).start()
        job["own"][...] = jnp.dot(left(core), right, preferred_element_type=F32).reshape(job["own"].shape)

    mid = width // 2

    def half_rows(ref):
        return lambda c: ref[pl.ds(pl.multiple_of(c * mid, mid), mid), :]

    halves(1, half_rows(scaled_t), emb)
    emb_acc[...] = emb.astype(F32)
    step1(0)

    def grad_block(i):
        cut = pl.ds(pl.multiple_of(i * block, block), block)
        scaled_grad = lax.dot_general(emb_acc[cut, :].astype(BF16), cp_v[...], NT, preferred_element_type=F32)
        gained = scaled_grad * gain[...]
        norm = normed[cut, :]
        hidden_grad = inv_std[cut, 0:1] * (
            gained
            - jnp.mean(gained, axis=1, keepdims=True)
            - norm * jnp.mean(gained * norm, axis=1, keepdims=True)
        )
        resid_grad[cut, :] = hidden_grad.astype(BF16)

    loop(0, 4, grad_block)

    def context_block(i):
        cut = pl.ds(i * block, block)
        context_grad[cut, :] = lax.dot_general(
            resid_grad[cut, :], wo_v[...], NT, preferred_element_type=F32
        ).astype(BF16)

    step1(1)
    for k in range(chunks):
        halves(2 + k, half_rows(ctx_t), resid_grad[:, k * cw : (k + 1) * cw])
        if k > 0:
            step1(1 + k)
    context_block(0)
    step1(1 + chunks)
    steps = [None, step1, step2, step3, step4, step5, step6, step7, step8]
    order = sorted((j + s, j, s) for j in range(1, chunks + 2) for s in range(2, 9))
    late = chunks + 1
    fillers = 1
    for tick, j, s in order:
        if j == 1 and fillers < 4:
            context_block(fillers)
            fillers += 1
        if j == late and s == 4:
            step2(0)
        if j == late and s == 6:
            step3(0)
        if j == late and s == 7:
            step4(0)
        if j == late and s == 8:
            each(n, lambda k: msg_copy(k, me).wait_send())
            for k in range(chunks + 2):
                drain_sum(k)
            for k in range(1, chunks + 1):
                drain_out(k)
        steps[s](j)
    drain_out(late)


JOB = ("own", "snd", "pl", "b1", "k1", "l1", "b2", "l2", "b3", "k2", "l3")


def finish_kernel(main, col, gain, colbert, loss_in, query_in, resid_in, context_in,
                  proj_grad, colbert_grad, gain_grad, loss, query_grad, resid_grad, context_grad, proj_v, sem):
    copies = [
        pltpu.make_async_copy(resid_in, resid_grad, sem.at[0]),
        pltpu.make_async_copy(context_in, context_grad, sem.at[1]),
        pltpu.make_async_copy(query_in, query_grad, sem.at[2]),
    ]
    for copy in copies:
        copy.start()
    chunks, rows, cw = main.shape
    band = rows // 4
    for b in range(4):
        cut = slice(b * band, (b + 1) * band)
        for k in range(chunks):
            proj_v[cut, k * cw : (k + 1) * cw] = main[k, cut, :].astype(F32)
        copy = pltpu.make_async_copy(proj_v.at[cut], proj_grad.at[cut], sem.at[3 + b])
        copy.start()
        copies.append(copy)
    wide = col[...].astype(F32)
    colbert_grad[...] = wide
    ones = jnp.ones((8, wide.shape[1]), F32)
    summed = exact(ones, wide * colbert[...].astype(F32), NT)
    gain_grad[...] = summed[0:1, :] / gain[...]
    loss[...] = loss_in[:, 0:1]
    for copy in copies:
        copy.wait()


def stay(array):
    return pltpu.with_memory_space_constraint(array, pltpu.HBM)


def job_buffers(at, piece, cols, lead=(), own=True):
    shapes = [
        ((at.half if own else 1, piece, cols), F32),
        ((at.half, piece, cols), BF16),
        ((at.half, piece, cols), BF16),
        ((at.half, piece, cols), BF16),
        ((at.plane, piece, cols), F32),
        ((at.n1, at.plane, piece, cols), BF16),
        ((at.plane, piece, cols), BF16),
        ((at.n2, at.nz, piece, cols), BF16),
        ((at.nz, piece, cols), BF16),
        ((at.nz, piece, cols), F32),
        ((at.nz, piece, cols), BF16),
    ]
    return [pltpu.VMEM(lead + shape, kind) for shape, kind in shapes]


def body(sizes, query_emb, positive, passage_emb, lengths, residual, context, out_proj, norm_gain, colbert_proj):
    dp, neg = sizes["dp"], sizes["neg"]
    at = Grid(dp, neg)
    own, per, dim = query_emb.shape
    plen = passage_emb.shape[1]
    rows, width = residual.shape
    tok = own * per
    n = at.n
    chunks = 4
    cw = width // chunks
    piece = width // (2 * at.half)
    dma = pltpu.SemaphoreType.DMA
    vm = pltpu.VMEM
    most = max(at.n1, at.n2, at.nz)
    scratch = [
        vm((n, tok, dim), BF16),
        vm((n, 1, 2 * n * own), F32),
        vm((n, plen, tok), BF16),
        vm((n, dim, tok), F32),
        vm((n, tok), F32),
        vm((n, tok), F32),
        vm((n, tok), F32),
        vm((plen, 2 * tok), F32),
        vm((plen, dim), BF16),
        vm((dim, plen), BF16),
        vm((plen, dim), F32),
        pltpu.SMEM((own,), jnp.int32),
        vm((1, width), F32),
        vm((width, width), BF16),
        vm((width, dim), BF16),
        vm((width, rows), BF16),
        vm((width, rows), BF16),
        vm((rows, width), F32),
        vm((rows, 128), F32),
    ]
    scratch += job_buffers(at, dim, tok, own=False)
    scratch += job_buffers(at, piece, dim)
    scratch += job_buffers(at, piece, cw, (chunks,))
    scratch += [
        dma((9,)),
        dma((at.nz,)),
        dma((at.nz, at.n1)),
        dma((at.nz * at.n1, at.n2)),
        dma((at.half,)),
        dma((n,)),
        dma((n,)),
        dma((n,)),
        dma((chunks + 2, 4, most)),
        dma((chunks + 2, 4, most)),
        dma((chunks + 2, 4, most)),
        dma((chunks + 2, 4, most)),
    ]
    held = sum(math.prod(ref.shape) * jnp.dtype(ref.dtype).itemsize for ref in scratch[:-12])
    limit = min(held + held // 8 + 8 * 1024 * 1024, 67043328)
    loss, query_grad, resid_grad, context_grad, sum_main, sum_col = pl.pallas_call(
        functools.partial(main_kernel, dp, neg, own, per),
        out_shape=[
            jax.ShapeDtypeStruct((1, 128), F32),
            jax.ShapeDtypeStruct((tok, dim), F32),
            jax.ShapeDtypeStruct((rows, width), BF16),
            jax.ShapeDtypeStruct((rows, width), BF16),
            jax.ShapeDtypeStruct((chunks, 2, at.half, piece, cw), BF16),
            jax.ShapeDtypeStruct((2, at.half, piece, dim), BF16),
        ],
        in_specs=[HBM, HBM, HBM, SMEM, HBM, HBM, HBM, HBM, HBM],
        out_specs=[VMEM] * 6,
        scratch_shapes=scratch,
        compiler_params=pltpu.CompilerParams(
            collective_id=1, has_side_effects=True, vmem_limit_bytes=limit
        ),
        name="maxsim_main",
    )(
        stay(query_emb.reshape(tok, dim)),
        stay(positive),
        stay(passage_emb.reshape(plen, dim)),
        lengths,
        stay(residual),
        stay(context),
        stay(out_proj),
        stay(norm_gain[None, :]),
        stay(colbert_proj),
    )
    proj_grad, colbert_grad, gain_grad, loss, query_grad, resid_grad, context_grad = pl.pallas_call(
        finish_kernel,
        out_shape=[
            jax.ShapeDtypeStruct((width, width), F32),
            jax.ShapeDtypeStruct((width, dim), F32),
            jax.ShapeDtypeStruct((1, width), F32),
            jax.ShapeDtypeStruct((1, 1), F32),
            jax.ShapeDtypeStruct((tok, dim), F32),
            jax.ShapeDtypeStruct((rows, width), BF16),
            jax.ShapeDtypeStruct((rows, width), BF16),
        ],
        in_specs=[VMEM] * 8,
        out_specs=[ANY, VMEM, VMEM, VMEM, ANY, ANY, ANY],
        scratch_shapes=[vm((width, width), F32), dma((7,))],
        compiler_params=pltpu.CompilerParams(vmem_limit_bytes=20000000),
        name="maxsim_finish",
    )(
        sum_main.reshape(chunks, width, cw),
        sum_col.reshape(width, dim),
        norm_gain[None, :],
        colbert_proj,
        loss,
        query_grad,
        resid_grad,
        context_grad,
    )
    return (
        loss.reshape(()),
        query_grad.reshape(own, per, dim),
        resid_grad,
        context_grad,
        proj_grad,
        colbert_grad,
        gain_grad.reshape(width),
    )


def solution(mesh):
    sizes = {axis: mesh.shape[axis] for axis in ("dp", "neg")}
    split = ("dp", "neg")
    in_specs = (
        P(split, None, None),
        P(split),
        P(split, None, None),
        P(split),
        P(split, None),
        P(split, None),
        P(),
        P(),
        P(),
    )
    out_specs = (
        P(),
        P(split, None, None),
        P(split, None),
        P(split, None),
        P(),
        P(),
        P(),
    )
    return jax.shard_map(
        functools.partial(body, sizes), mesh=mesh, in_specs=in_specs, out_specs=out_specs, check_vma=False
    )
```

```python
import functools
import math

import jax
import jax.numpy as jnp
from jax import lax
from jax.experimental import pallas as pl
from jax.experimental.pallas import tpu as pltpu
from jax.sharding import PartitionSpec as P

MESH = pl.DeviceIdType.MESH
VMEM = pl.BlockSpec(memory_space=pltpu.VMEM)
SMEM = pl.BlockSpec(memory_space=pltpu.SMEM)
ANY = pl.BlockSpec(memory_space=pl.ANY)
HBM = pl.BlockSpec(memory_space=pltpu.HBM)
LOW = -1e30
F32 = jnp.float32
BF16 = jnp.bfloat16
NT = (((1,), (1,)), ((), ()))
LAG = 2
ORDER = (
    21, -1, 41, -1, 51, -1, -1, -1, 91, -1, 22, -1, 42, 61, -1, 52, 71, -1, 92, 23, 81, 62, 31, 11, 43, 53, 72, 93, 63,
    24, 82, 44, 32, 1, 73, 54, 94, 83, 33, 12, 25, 45, 74, 55, 2, 13, 46, 64, 84, 95, 34, 56, 14, 75, 26, 3, 65, 96, 85,
    76, 35, 15, 66, 57, 97, 86, 36, 47, 16, 48, 77, 27, 67, 87, 58, 37, 17, 78, 98, 88, 28, 4, 68, 38, 18,
)


def exact(a, b, dims=(((1,), (0,)), ((), ()))):
    return lax.dot_general(a, b, dims, precision=lax.Precision.HIGHEST, preferred_element_type=F32)


def each(size, act):
    def turn(k, carry):
        act(k)
        return carry

    lax.fori_loop(1, size, turn, 0)


def loop(low, high, act):
    def turn(k, carry):
        act(k)
        return carry

    lax.fori_loop(low, high, turn, 0)


def remote(src, dst, send, recv, device):
    return pltpu.make_async_remote_copy(
        src_ref=src, dst_ref=dst, send_sem=send, recv_sem=recv, device_id=device, device_id_type=MESH
    )


class Grid:
    def __init__(self, dp, neg):
        groups = neg // 2
        self.dp, self.neg = dp, neg
        self.a = 2 if groups % 2 == 0 else 1
        self.b = groups // self.a
        self.n1, self.n2, self.nz = self.b, self.a, dp
        self.turned = self.a == self.b
        self.n = dp * neg
        self.half = self.n // 2
        self.plane = self.n2 * self.nz

    def locate(self):
        self.r, self.col = lax.axis_index("dp"), lax.axis_index("neg")
        self.core = lax.rem(self.col, 2)
        g = self.col // 2
        self.y, self.x = g // self.b, lax.rem(g, self.b)
        self.me = self.r * self.neg + self.col

    def flip(self, core):
        return core if self.turned else 0 * core

    def own(self, core):
        f = self.flip(core)
        return (self.x * (1 - f) + self.y * f, self.y * (1 - f) + self.x * f)

    def column(self, j1, j2, core):
        f = self.flip(core)
        x, y = j1 * (1 - f) + j2 * f, j2 * (1 - f) + j1 * f
        return (y * self.b + x) * 2 + core

    def nearby(self, k):
        there, bit = self.r, 1
        while bit < self.nz:
            there = there + lax.rem(k // bit, 2) * bit * (1 - 2 * lax.rem(self.r // bit, 2))
            bit *= 2
        return there

    def arrival(self, i, core):
        i1, i2 = self.own(core)
        m2, m1, k = i // (self.n1 * self.nz), lax.rem(i // self.nz, self.n1), lax.rem(i, self.nz)
        return (self.nearby(k), lax.rem(i1 + m1, self.n1), lax.rem(i2 + m2, self.n2))

    def slot(self, rr, j1, j2, core):
        return rr * self.neg + self.column(j1, j2, core)


def main_kernel(dp, neg, own, per, query, positive_in, passage, lengths, resid, context, out_proj, gain_in, colbert,
                loss, query_grad, resid_grad, context_grad, sum_main, sum_col,
                q_all, msg, e_all, u_all, sums, inner, scale, bias, pas_v, flipped, emb_acc,
                positive, gain, wo_v, cp_v, ctx_t, scaled_t, normed, inv_std, blend, *rest):
    at = Grid(dp, neg)
    at.locate()
    r, core, me = at.r, at.core, at.me
    other = 1 - core
    i1, i2 = at.own(core)
    n, n1, n2, nz, half, plane = at.n, at.n1, at.n2, at.nz, at.half, at.plane
    place = (i1 * n2 + i2) * nz + r
    partner = (r, at.col + 1 - 2 * core)
    tok = own * per
    wide = n * own
    rows, width = resid.shape
    block = rows // 4
    chunks = sum_main.shape[0]
    cw = sum_main.shape[-1]
    count = len(JOB)
    sems = rest[3 * count :]
    ld, zs, a1s, a2s, pps, agr, xs, xr, rs_s, rs_r, ag_s, ag_r = sems

    def dev1(t):
        return (r, at.column(lax.rem(i1 + t, n1), i2, core))

    def dev2(t):
        return (r, at.column(i1, lax.rem(i2 + t, n2), core))

    def devz(k):
        return (lax.rem(r + k, nz), at.col)

    def any_device(k):
        d = lax.rem(me + k, n)
        return (d // neg, lax.rem(d, neg))

    barrier = pltpu.get_barrier_semaphore()

    def greet(device):
        pl.semaphore_signal(barrier, inc=1, device_id=device, device_id_type=MESH)

    each(nz, lambda k: greet(devz(k)))
    each(n1, lambda t: greet(dev1(t)))
    each(n2, lambda t: greet(dev2(t)))
    greet(partner)
    loads = [
        pltpu.make_async_copy(query, q_all.at[me], ld.at[0]),
        pltpu.make_async_copy(passage, pas_v, ld.at[1]),
        pltpu.make_async_copy(context, context_grad, ld.at[2]),
        pltpu.make_async_copy(out_proj, wo_v, ld.at[3]),
        pltpu.make_async_copy(resid, resid_grad, ld.at[4]),
        pltpu.make_async_copy(colbert, cp_v, ld.at[5]),
        pltpu.make_async_copy(gain_in, gain, ld.at[7]),
        pltpu.make_async_copy(positive_in, positive, ld.at[8]),
    ]
    for copy in loads:
        copy.start()
    loads[0].wait()
    pl.semaphore_wait(barrier, nz + n1 + n2 - 2)

    def z_copy(k):
        return remote(q_all.at[me], q_all.at[me], zs.at[k], agr.at[me], devz(k))

    def a1_copy(s, rr, t):
        return remote(q_all.at[s], q_all.at[s], a1s.at[rr, t], agr.at[s], dev1(t))

    def a2_copy(s, rr, j1, t):
        return remote(q_all.at[s], q_all.at[s], a2s.at[rr * n1 + j1, t], agr.at[s], dev2(t))

    def pp_copy(s, rr, j1, j2):
        return remote(q_all.at[s], q_all.at[s], pps.at[(j1 * n2 + j2) * nz + rr], agr.at[s], partner)

    def landed(s):
        remote(q_all.at[s], q_all.at[s], zs.at[0], agr.at[s], partner).wait_recv()

    def route(i, act):
        rr, j1, j2 = at.arrival(i, core)
        s = at.slot(rr, j1, j2, core)

        @pl.when(i < nz)
        def _():
            each(n1, lambda t: act(a1_copy(s, rr, t)))

        @pl.when(i < nz * n1)
        def _():
            each(n2, lambda t: act(a2_copy(s, rr, j1, t)))

        act(pp_copy(s, rr, j1, j2))

    def attend(v):
        u, side = v // 2, lax.rem(v, 2)
        whose = core * (1 - side) + other * side
        slots = [at.slot(*at.arrival(2 * u + w, whose), whose) for w in range(2)]

        @pl.when(side == 1)
        def _():
            for s in slots:
                landed(s)

        tokens = jnp.concatenate([q_all[s] for s in slots], axis=0)
        scores = lax.dot_general(pas_v[...], tokens, NT, preferred_element_type=F32) + bias[...]
        highest = jnp.max(scores, axis=0, keepdims=True)
        spread = jnp.exp(scores - highest)
        total = jnp.sum(spread, axis=0, keepdims=True)
        low = spread.astype(BF16)
        level = highest + jnp.log(total)
        for w, s in enumerate(slots):
            cut = slice(w * tok, (w + 1) * tok)
            e_all[s] = low[:, cut]
            sums[pl.ds(s, 1), :] = total[:, cut]
            inner[pl.ds(s, 1), :] = level[:, cut]

    each(nz, lambda k: z_copy(k).start())
    route(0, lambda copy: copy.start())
    loads[1].wait()
    length = lengths[0]
    position = lax.broadcasted_iota(jnp.int32, bias.shape, 0)
    bias[...] = jnp.where(position < length, 0.0, LOW)
    flipped[...] = pas_v[...].astype(F32).T.astype(BF16)

    def relay(i):
        landed(at.slot(*at.arrival(i, core), core))
        route(i, lambda copy: copy.start())

    def relay_step(i):
        relay(i)

        @pl.when(i >= LAG)
        def _():
            attend(i - LAG)

    loop(1, half, relay_step)
    loop(half - LAG, half, attend)

    loads[7].wait()
    token = lax.broadcasted_iota(jnp.int32, (tok, wide), 0)
    lane = lax.broadcasted_iota(jnp.int32, (tok, wide), 1)
    spots = jnp.where(token // per == lax.rem(lane, own), 1.0, 0.0)
    slot_of = lax.broadcasted_iota(jnp.int32, (n, wide), 0)
    lane_of = lax.broadcasted_iota(jnp.int32, (n, wide), 1)
    mine = slot_of == lane_of // own
    grouped = exact(inner[...], spots)
    similar = jnp.sum(jnp.where(mine, grouped, 0.0), axis=0, keepdims=True)
    shift = jnp.log(jnp.full((1, wide), length, jnp.int32).astype(F32)) * per
    row_lane = lax.broadcasted_iota(jnp.int32, (1, wide), 1)
    chosen = jnp.zeros((1, wide), jnp.int32)
    for i in range(own):
        chosen = chosen + jnp.where(row_lane == me * own + i, positive[i], 0)
    msg[me, :, :wide] = similar - shift
    msg[me, :, wide:] = chosen.astype(F32)

    def msg_copy(k, slot):
        return remote(msg.at[slot], msg.at[slot], xs.at[k], xr.at[k], any_device(k))

    each(n, lambda k: msg_copy(k, me).start())

    for copy in loads[2:7]:
        copy.wait()

    def norm_block(i):
        cut = pl.ds(pl.multiple_of(i * block, block), block)
        ctx = context_grad[cut, :]
        hidden = resid_grad[cut, :].astype(F32) + jnp.dot(ctx, wo_v[...], preferred_element_type=F32)
        centred = hidden - jnp.mean(hidden, axis=1, keepdims=True)
        variance = jnp.mean(centred * centred, axis=1, keepdims=True)
        inv = 1.0 / jnp.sqrt(variance + 1e-05)
        norm = centred * inv
        normed[cut, :] = norm
        inv_std[cut, :] = jnp.broadcast_to(inv, (block, inv_std.shape[1]))
        scaled = norm * gain[...]
        scaled_t[:, cut] = scaled.T.astype(BF16)
        blend[cut, :] = jnp.dot(scaled.astype(BF16), cp_v[...], preferred_element_type=F32) / width
        ctx_t[:, cut] = ctx.astype(F32).T.astype(BF16)

    loop(0, 4, norm_block)
    flat = exact(jnp.broadcast_to(gain[...], (8, width)), cp_v[...].astype(F32))[0:1, :] / width

    each(n, lambda k: msg_copy(k, lax.rem(me - k + n, n)).wait_recv())

    everyone = msg[:, :, :wide]
    picked = jnp.sum(msg[:, :, wide:], axis=0)
    highest = jnp.max(everyone, axis=0)
    log_total = highest + jnp.log(jnp.sum(jnp.exp(everyone - highest[None]), axis=0))
    which = lax.broadcasted_iota(jnp.int32, everyone.shape, 0).astype(F32)
    score = jnp.sum(jnp.where(which == picked[None], everyone, 0.0), axis=0)
    average = jnp.sum(log_total - score, axis=1, keepdims=True) / wide
    loss[...] = jnp.broadcast_to(average, loss.shape)
    hit = jnp.where(picked == me.astype(F32), 1.0, 0.0)
    coefficient = jnp.exp(similar - shift - log_total) - hit
    laid = jnp.where(mine, jnp.broadcast_to(coefficient, mine.shape), 0.0)
    scale[...] = exact(laid, spots, NT) / sums[...]

    jobs = []
    for which_job, out in ((0, None), (1, sum_col)):
        jobs.append(dict(zip(JOB, rest[which_job * count : (which_job + 1) * count]), out=out))
    for k in range(chunks):
        jobs.append(dict(zip(JOB, [ref.at[k] for ref in rest[2 * count : 3 * count]]), out=sum_main.at[k]))

    def pair_copy(j):
        return remote(jobs[j]["snd"], jobs[j]["pl"], rs_s.at[j, 0, 0], rs_r.at[j, 0, 0], partner)

    def rs1_copy(j, t):
        there = pl.ds(lax.rem(i1 + t, n1) * plane, plane)
        return remote(jobs[j]["b1"].at[there], jobs[j]["l1"].at[t], rs_s.at[j, 1, t], rs_r.at[j, 1, t], dev1(t))

    def rs2_copy(j, t):
        there = pl.ds(lax.rem(i2 + t, n2) * nz, nz)
        return remote(jobs[j]["b2"].at[there], jobs[j]["l2"].at[t], rs_s.at[j, 2, t], rs_r.at[j, 2, t], dev2(t))

    def rs3_copy(j, k):
        return remote(jobs[j]["b3"].at[lax.rem(r + k, nz)], jobs[j]["l3"].at[k], rs_s.at[j, 3, k], rs_r.at[j, 3, k], devz(k))

    def ag3_copy(j, k, here):
        piece = jobs[j]["out"].at[core, here]
        return remote(piece, piece, ag_s.at[j, 0, k], ag_r.at[j, 0, k], devz(k))

    def ag2_copy(j, t, j2):
        piece = jobs[j]["out"].at[core, pl.ds((i1 * n2 + j2) * nz, nz)]
        return remote(piece, piece, ag_s.at[j, 1, t], ag_r.at[j, 1, t], dev2(t))

    def ag1_copy(j, t, j1):
        piece = jobs[j]["out"].at[core, pl.ds(j1 * plane, plane)]
        return remote(piece, piece, ag_s.at[j, 2, t], ag_r.at[j, 2, t], dev1(t))

    def ag0_copy(j, c):
        piece = jobs[j]["out"].at[c]
        return remote(piece, piece, ag_s.at[j, 3, 0], ag_r.at[j, 3, 0], partner)

    def step1(j):
        job = jobs[j]
        pair_copy(j).wait_recv()
        if j > 0:
            job["b1"][...] = (job["own"][...] + job["pl"][...].astype(F32)).astype(BF16)
            kept = pl.ds(i1 * plane, plane)
            job["k1"][...] = job["own"][kept] + job["pl"][kept].astype(F32)
        else:

            def send_term(p):
                j1, j2, rr = p // plane, lax.rem(p // nz, n2), lax.rem(p, nz)
                s = at.slot(rr, j1, j2, core)
                total = u_all[s] * scale[pl.ds(s, 1), :] + job["pl"][p].astype(F32)
                job["b1"][p] = total.astype(BF16)

            def keep_term(q):
                p = i1 * plane + q
                j1, j2, rr = p // plane, lax.rem(p // nz, n2), lax.rem(p, nz)
                s = at.slot(rr, j1, j2, core)
                job["k1"][q] = u_all[s] * scale[pl.ds(s, 1), :] + job["pl"][p].astype(F32)

            loop(plane, half, lambda p: send_term(lax.rem(i1 * plane + p, half)))
            loop(0, plane, keep_term)
        for t in range(1, n1):
            rs1_copy(j, t).start()

    def step2(j):
        job = jobs[j]
        total = job["k1"][...]
        for t in range(1, n1):
            rs1_copy(j, t).wait_recv()
            total = total + job["l1"][t].astype(F32)
        job["b2"][...] = total.astype(BF16)
        job["k1"][...] = total
        for t in range(1, n2):
            rs2_copy(j, t).start()

    def step3(j):
        job = jobs[j]
        total = job["k1"][pl.ds(i2 * nz, nz)]
        for t in range(1, n2):
            rs2_copy(j, t).wait_recv()
            total = total + job["l2"][t].astype(F32)
        job["b3"][...] = total.astype(BF16)
        job["k2"][...] = total
        for k in range(1, nz):
            rs3_copy(j, k).start()

    def step4(j):
        job = jobs[j]
        total = job["k2"][r]
        for k in range(1, nz):
            rs3_copy(j, k).wait_recv()
            total = total + job["l3"][k].astype(F32)
        if job["out"] is None:
            query_grad[...] = total.T
        else:
            job["out"][core, place] = total.astype(BF16)
            for k in range(1, nz):
                ag3_copy(j, k, place).start()

    def step5(j):
        for k in range(1, nz):
            ag3_copy(j, k, (i1 * n2 + i2) * nz + lax.rem(r - k + nz, nz)).wait_recv()
        for t in range(1, n2):
            ag2_copy(j, t, i2).start()

    def step6(j):
        for t in range(1, n2):
            ag2_copy(j, t, lax.rem(i2 - t + n2, n2)).wait_recv()
        for t in range(1, n1):
            ag1_copy(j, t, i1).start()

    def step7(j):
        for t in range(1, n1):
            ag1_copy(j, t, lax.rem(i1 - t + n1, n1)).wait_recv()
        ag0_copy(j, core).start()

    def step8(j):
        ag0_copy(j, other).wait_recv()

    def drain_sum(j):
        pair_copy(j).wait_send()
        for t in range(1, n1):
            rs1_copy(j, t).wait_send()
        for t in range(1, n2):
            rs2_copy(j, t).wait_send()
        for k in range(1, nz):
            rs3_copy(j, k).wait_send()

    def drain_out(j):
        for k in range(1, nz):
            ag3_copy(j, k, place).wait_send()
        for t in range(1, n2):
            ag2_copy(j, t, i2).wait_send()
        for t in range(1, n1):
            ag1_copy(j, t, i1).wait_send()
        ag0_copy(j, core).wait_send()

    emb_acc[...] = jnp.zeros_like(emb_acc)

    def emb_term(u):
        parts = []
        for v in range(16):
            s = u * 16 + v
            row = jnp.broadcast_to(scale[pl.ds(s, 1), :], (16, tok)).astype(BF16)
            spread = e_all[s]
            parts.append((spread.reshape(-1, 16, tok) * row[None]).reshape(spread.shape))
        weight = jnp.concatenate(parts, axis=1)
        tokens = q_all[pl.ds(u * 16, 16)].reshape(16 * tok, q_all.shape[2])
        emb_acc[...] += jnp.dot(weight, tokens, preferred_element_type=F32)

    loop(0, n // 16, emb_term)
    emb = emb_acc[...].astype(BF16)
    emb_acc[...] = emb.astype(F32)

    def grad_block(i):
        cut = pl.ds(pl.multiple_of(i * block, block), block)
        grad = emb_acc[cut, :]
        first = jnp.sum(grad * flat, axis=1, keepdims=True)
        second = jnp.sum(grad * blend[cut, :], axis=1, keepdims=True)
        scaled_grad = lax.dot_general(grad.astype(BF16), cp_v[...], NT, preferred_element_type=F32)
        hidden_grad = inv_std[cut, 0:1] * (scaled_grad * gain[...] - first - normed[cut, :] * second)
        resid_grad[cut, :] = hidden_grad.astype(BF16)

    loop(0, 4, grad_block)

    mid = width // 2

    def half_rows(ref, c):
        return ref[pl.ds(pl.multiple_of(c * mid, mid), mid), :]

    def proj_terms(c, name, group):
        span = chunks // 2 * cw
        term = jnp.dot(
            half_rows(ctx_t, c), resid_grad[:, group * span : (group + 1) * span], preferred_element_type=F32
        )
        for k in range(chunks // 2):
            ref = jobs[2 + group * (chunks // 2) + k][name]
            ref[...] = term[:, k * cw : (k + 1) * cw].reshape(ref.shape).astype(ref.dtype)

    def col_term(c, name):
        ref = jobs[1][name]
        term = jnp.dot(half_rows(scaled_t, c), emb_acc[...].astype(BF16), preferred_element_type=F32)
        ref[...] = term.reshape(ref.shape).astype(ref.dtype)

    for group in range(2):
        proj_terms(other, "snd", group)
        for k in range(chunks // 2):
            pair_copy(2 + group * (chunks // 2) + k).start()
    col_term(other, "snd")
    pair_copy(1).start()
    for group in range(2):
        proj_terms(core, "own", group)
    col_term(core, "own")

    def query_terms():
        def term(p):
            j1, j2, rr = p // plane, lax.rem(p // nz, n2), lax.rem(p, nz)
            s = at.slot(rr, j1, j2, other)
            jobs[0]["snd"][p] = (u_all[s] * scale[pl.ds(s, 1), :]).astype(BF16)

        loop(0, half, term)
        pair_copy(0).start()

    def below_terms(i):
        def below(u):
            for w in range(2):
                s = u * 4 + w * 2
                spread = jnp.concatenate([e_all[s], e_all[s + 1]], axis=1)
                term = jnp.dot(flipped[...], spread, preferred_element_type=F32)
                u_all[s] = term[:, :tok]
                u_all[s + 1] = term[:, tok:]

        loop(i * (n // 16), (i + 1) * (n // 16), below)

    def context_terms(i):
        cut = slice(i * (width // 4), (i + 1) * (width // 4))
        context_grad[:, cut] = lax.dot_general(
            resid_grad[...], wo_v[cut, :], NT, preferred_element_type=F32
        ).astype(BF16)

    def drain_gather():
        each(nz, lambda k: z_copy(k).wait_send())
        loop(0, half, lambda i: route(i, lambda copy: copy.wait_send()))
        each(n, lambda k: msg_copy(k, me).wait_send())

    fillers = [functools.partial(context_terms, i) for i in range(4)]
    fillers += [functools.partial(below_terms, i) for i in range(4)] + [query_terms]
    steps = [None, step1, step2, step3, step4, step5, step6, step7, step8]
    for code in ORDER:
        if code < 0:
            if fillers:
                fillers.pop(0)()
            continue
        if code == 1:
            while fillers:
                fillers.pop(0)()
            drain_gather()
        steps[code % 10](code // 10)
    for j in range(chunks + 2):
        drain_sum(j)
    for j in range(1, chunks + 2):
        drain_out(j)


JOB = ("own", "snd", "pl", "b1", "k1", "l1", "b2", "l2", "b3", "k2", "l3")


def finish_kernel(main, col, gain, colbert, loss_in, query_in, resid_in, context_in,
                  proj_grad, colbert_grad, gain_grad, loss, query_grad, resid_grad, context_grad, proj_v, sem):
    copies = [
        pltpu.make_async_copy(resid_in, resid_grad, sem.at[0]),
        pltpu.make_async_copy(context_in, context_grad, sem.at[1]),
        pltpu.make_async_copy(query_in, query_grad, sem.at[2]),
    ]
    for copy in copies:
        copy.start()
    chunks, rows, cw = main.shape
    band = rows // 4
    for b in range(4):
        cut = slice(b * band, (b + 1) * band)
        for k in range(chunks):
            proj_v[cut, k * cw : (k + 1) * cw] = main[k, cut, :].astype(F32)
        copy = pltpu.make_async_copy(proj_v.at[cut], proj_grad.at[cut], sem.at[3 + b])
        copy.start()
        copies.append(copy)
    wide = col[...].astype(F32)
    colbert_grad[...] = wide
    ones = jnp.ones((8, wide.shape[1]), F32)
    summed = exact(ones, wide * colbert[...].astype(F32), NT)
    gain_grad[...] = summed[0:1, :] / gain[...]
    loss[...] = loss_in[:, 0:1]
    for copy in copies:
        copy.wait()


def stay(array):
    return pltpu.with_memory_space_constraint(array, pltpu.HBM)


def job_buffers(at, piece, cols, lead=(), own=True):
    shapes = [
        ((at.half if own else 1, piece, cols), F32),
        ((at.half, piece, cols), BF16),
        ((at.half, piece, cols), BF16),
        ((at.half, piece, cols), BF16),
        ((at.plane, piece, cols), F32),
        ((at.n1, at.plane, piece, cols), BF16),
        ((at.plane, piece, cols), BF16),
        ((at.n2, at.nz, piece, cols), BF16),
        ((at.nz, piece, cols), BF16),
        ((at.nz, piece, cols), F32),
        ((at.nz, piece, cols), BF16),
    ]
    return [pltpu.VMEM(lead + shape, kind) for shape, kind in shapes]


def body(sizes, query_emb, positive, passage_emb, lengths, residual, context, out_proj, norm_gain, colbert_proj):
    dp, neg = sizes["dp"], sizes["neg"]
    at = Grid(dp, neg)
    own, per, dim = query_emb.shape
    plen = passage_emb.shape[1]
    rows, width = residual.shape
    tok = own * per
    n = at.n
    chunks = 8
    cw = width // chunks
    piece = width // (2 * at.half)
    dma = pltpu.SemaphoreType.DMA
    vm = pltpu.VMEM
    most = max(at.n1, at.n2, at.nz)
    scratch = [
        vm((n, tok, dim), BF16),
        vm((n, 1, 2 * n * own), F32),
        vm((n, plen, tok), BF16),
        vm((n, dim, tok), F32),
        vm((n, tok), F32),
        vm((n, tok), F32),
        vm((n, tok), F32),
        vm((plen, 2 * tok), F32),
        vm((plen, dim), BF16),
        vm((dim, plen), BF16),
        vm((plen, dim), F32),
        pltpu.SMEM((own,), jnp.int32),
        vm((1, width), F32),
        vm((width, width), BF16),
        vm((width, dim), BF16),
        vm((width, rows), BF16),
        vm((width, rows), BF16),
        vm((rows, width), F32),
        vm((rows, 128), F32),
        vm((rows, dim), F32),
    ]
    scratch += job_buffers(at, dim, tok, own=False)
    scratch += job_buffers(at, piece, dim)
    scratch += job_buffers(at, piece, cw, (chunks,))
    scratch += [
        dma((9,)),
        dma((at.nz,)),
        dma((at.nz, at.n1)),
        dma((at.nz * at.n1, at.n2)),
        dma((at.half,)),
        dma((n,)),
        dma((n,)),
        dma((n,)),
        dma((chunks + 2, 4, most)),
        dma((chunks + 2, 4, most)),
        dma((chunks + 2, 4, most)),
        dma((chunks + 2, 4, most)),
    ]
    held = sum(math.prod(ref.shape) * jnp.dtype(ref.dtype).itemsize for ref in scratch[:-12])
    limit = min(held + held // 8 + 8 * 1024 * 1024, 67043328)
    loss, query_grad, resid_grad, context_grad, sum_main, sum_col = pl.pallas_call(
        functools.partial(main_kernel, dp, neg, own, per),
        out_shape=[
            jax.ShapeDtypeStruct((1, 128), F32),
            jax.ShapeDtypeStruct((tok, dim), F32),
            jax.ShapeDtypeStruct((rows, width), BF16),
            jax.ShapeDtypeStruct((rows, width), BF16),
            jax.ShapeDtypeStruct((chunks, 2, at.half, piece, cw), BF16),
            jax.ShapeDtypeStruct((2, at.half, piece, dim), BF16),
        ],
        in_specs=[HBM, HBM, HBM, SMEM, HBM, HBM, HBM, HBM, HBM],
        out_specs=[VMEM] * 6,
        scratch_shapes=scratch,
        compiler_params=pltpu.CompilerParams(
            collective_id=1, has_side_effects=True, vmem_limit_bytes=limit
        ),
        name="maxsim_main",
    )(
        stay(query_emb.reshape(tok, dim)),
        stay(positive),
        stay(passage_emb.reshape(plen, dim)),
        lengths,
        stay(residual),
        stay(context),
        stay(out_proj),
        stay(norm_gain[None, :]),
        stay(colbert_proj),
    )
    proj_grad, colbert_grad, gain_grad, loss, query_grad, resid_grad, context_grad = pl.pallas_call(
        finish_kernel,
        out_shape=[
            jax.ShapeDtypeStruct((width, width), F32),
            jax.ShapeDtypeStruct((width, dim), F32),
            jax.ShapeDtypeStruct((1, width), F32),
            jax.ShapeDtypeStruct((1, 1), F32),
            jax.ShapeDtypeStruct((tok, dim), F32),
            jax.ShapeDtypeStruct((rows, width), BF16),
            jax.ShapeDtypeStruct((rows, width), BF16),
        ],
        in_specs=[VMEM] * 8,
        out_specs=[ANY, VMEM, VMEM, VMEM, ANY, ANY, ANY],
        scratch_shapes=[vm((width, width), F32), dma((7,))],
        compiler_params=pltpu.CompilerParams(vmem_limit_bytes=20000000),
        name="maxsim_finish",
    )(
        sum_main.reshape(chunks, width, cw),
        sum_col.reshape(width, dim),
        norm_gain[None, :],
        colbert_proj,
        loss,
        query_grad,
        resid_grad,
        context_grad,
    )
    return (
        loss.reshape(()),
        query_grad.reshape(own, per, dim),
        resid_grad,
        context_grad,
        proj_grad,
        colbert_grad,
        gain_grad.reshape(width),
    )


def solution(mesh):
    sizes = {axis: mesh.shape[axis] for axis in ("dp", "neg")}
    split = ("dp", "neg")
    in_specs = (
        P(split, None, None),
        P(split),
        P(split, None, None),
        P(split),
        P(split, None),
        P(split, None),
        P(),
        P(),
        P(),
    )
    out_specs = (
        P(),
        P(split, None, None),
        P(split, None),
        P(split, None),
        P(),
        P(),
        P(),
    )
    return jax.shard_map(
        functools.partial(body, sizes), mesh=mesh, in_specs=in_specs, out_specs=out_specs, check_vma=False
    )
```

```python
import functools
import math

import jax
import jax.numpy as jnp
from jax import lax
from jax.experimental import pallas as pl
from jax.experimental.pallas import tpu as pltpu
from jax.sharding import PartitionSpec as P

MESH = pl.DeviceIdType.MESH
VMEM = pl.BlockSpec(memory_space=pltpu.VMEM)
SMEM = pl.BlockSpec(memory_space=pltpu.SMEM)
ANY = pl.BlockSpec(memory_space=pl.ANY)
HBM = pl.BlockSpec(memory_space=pltpu.HBM)
LOW = -1e30
F32 = jnp.float32
BF16 = jnp.bfloat16
NT = (((1,), (1,)), ((), ()))
LAG = 2
ORDER = (
    21, -1, 41, -1, 51, -1, -1, -1, 91, -1, 22, -1, 42, 61, -1, 52, 71, -1, 92, 23, 81, 62, 31, 11, 43, 53, 72, 93, 63,
    24, 82, 44, 32, 1, 73, 54, 94, 83, 33, 12, 25, 45, 74, 55, 2, 13, 46, 64, 84, 95, 34, 56, 14, 75, 26, 3, 65, 96, 85,
    76, 35, 15, 66, 57, 97, 86, 36, 47, 16, 48, 77, 27, 67, 87, 58, 37, 17, 78, 98, 88, 28, 4, 68, 38, 18,
)


def exact(a, b, dims=(((1,), (0,)), ((), ()))):
    return lax.dot_general(a, b, dims, precision=lax.Precision.HIGHEST, preferred_element_type=F32)


def each(size, act):
    def turn(k, carry):
        act(k)
        return carry

    lax.fori_loop(1, size, turn, 0)


def loop(low, high, act):
    def turn(k, carry):
        act(k)
        return carry

    lax.fori_loop(low, high, turn, 0)


def remote(src, dst, send, recv, device):
    return pltpu.make_async_remote_copy(
        src_ref=src, dst_ref=dst, send_sem=send, recv_sem=recv, device_id=device, device_id_type=MESH
    )


class Grid:
    def __init__(self, dp, neg):
        groups = neg // 2
        self.dp, self.neg = dp, neg
        self.a = 2 if groups % 2 == 0 else 1
        self.b = groups // self.a
        self.n1, self.n2, self.nz = self.b, self.a, dp
        self.turned = self.a == self.b
        self.n = dp * neg
        self.half = self.n // 2
        self.plane = self.n2 * self.nz

    def locate(self):
        self.r, self.col = lax.axis_index("dp"), lax.axis_index("neg")
        self.core = lax.rem(self.col, 2)
        g = self.col // 2
        self.y, self.x = g // self.b, lax.rem(g, self.b)
        self.me = self.r * self.neg + self.col

    def flip(self, core):
        return core if self.turned else 0 * core

    def own(self, core):
        f = self.flip(core)
        return (self.x * (1 - f) + self.y * f, self.y * (1 - f) + self.x * f)

    def column(self, j1, j2, core):
        f = self.flip(core)
        x, y = j1 * (1 - f) + j2 * f, j2 * (1 - f) + j1 * f
        return (y * self.b + x) * 2 + core

    def nearby(self, k):
        there, bit = self.r, 1
        while bit < self.nz:
            there = there + lax.rem(k // bit, 2) * bit * (1 - 2 * lax.rem(self.r // bit, 2))
            bit *= 2
        return there

    def arrival(self, i, core):
        i1, i2 = self.own(core)
        m2, m1, k = i // (self.n1 * self.nz), lax.rem(i // self.nz, self.n1), lax.rem(i, self.nz)
        return (self.nearby(k), lax.rem(i1 + m1, self.n1), lax.rem(i2 + m2, self.n2))

    def slot(self, rr, j1, j2, core):
        return rr * self.neg + self.column(j1, j2, core)


def main_kernel(dp, neg, own, per, query, positive_in, passage, lengths, resid, context, out_proj, gain_in, colbert,
                loss, query_grad, resid_grad, context_grad, summed,
                q_all, msg, e_all, u_all, sums, inner, scale, bias, pas_v, flipped, emb_acc,
                positive, gain, wo_v, cp_v, ctx_t, scaled_t, normed, inv_std, blend, *rest):
    at = Grid(dp, neg)
    at.locate()
    r, core, me = at.r, at.core, at.me
    other = 1 - core
    i1, i2 = at.own(core)
    n, n1, n2, nz, half, plane = at.n, at.n1, at.n2, at.nz, at.half, at.plane
    place = (i1 * n2 + i2) * nz + r
    partner = (r, at.col + 1 - 2 * core)
    tok = own * per
    wide = n * own
    rows, width = resid.shape
    block = rows // 4
    chunks = summed.shape[0] - 1
    cw = summed.shape[-1]
    count = len(JOB)
    sems = rest[2 * count :]
    ld, gs, agr, xs, xr, q_s, q_r, rs_s, rs_r, ag_s, ag_r = sems

    def dev1(t):
        return (r, at.column(lax.rem(i1 + t, n1), i2, core))

    def dev2(t):
        return (r, at.column(i1, lax.rem(i2 + t, n2), core))

    def devz(k):
        return (lax.rem(r + k, nz), at.col)

    def any_device(k):
        d = lax.rem(me + k, n)
        return (d // neg, lax.rem(d, neg))

    barrier = pltpu.get_barrier_semaphore()

    def greet(device):
        pl.semaphore_signal(barrier, inc=1, device_id=device, device_id_type=MESH)

    each(nz, lambda k: greet(devz(k)))
    each(n1, lambda t: greet(dev1(t)))
    each(n2, lambda t: greet(dev2(t)))
    greet(partner)
    loads = [
        pltpu.make_async_copy(query, q_all.at[me], ld.at[0]),
        pltpu.make_async_copy(passage, pas_v, ld.at[1]),
        pltpu.make_async_copy(context, context_grad, ld.at[2]),
        pltpu.make_async_copy(out_proj, wo_v, ld.at[3]),
        pltpu.make_async_copy(resid, resid_grad, ld.at[4]),
        pltpu.make_async_copy(colbert, cp_v, ld.at[5]),
        pltpu.make_async_copy(gain_in, gain, ld.at[6]),
        pltpu.make_async_copy(positive_in, positive, ld.at[7]),
    ]
    for copy in loads:
        copy.start()
    loads[0].wait()
    pl.semaphore_wait(barrier, nz + n1 + n2 - 2)

    def arrived(ref, sem):
        pltpu.make_async_copy(ref, ref, sem).wait()

    def spread(s, device):
        return remote(q_all.at[s], q_all.at[s], gs, agr.at[s], device)

    def landed(s):
        spread(s, partner).wait_recv()

    def pass_on(i):
        rr, j1, j2 = at.arrival(i, core)
        s = at.slot(rr, j1, j2, core)

        @pl.when(i < nz)
        def _():
            each(n1, lambda t: spread(s, dev1(t)).start())

        @pl.when(i < nz * n1)
        def _():
            each(n2, lambda t: spread(s, dev2(t)).start())

        spread(s, partner).start()

    def attend(v):
        u, side = v // 2, lax.rem(v, 2)
        whose = core * (1 - side) + other * side
        slots = [at.slot(*at.arrival(2 * u + w, whose), whose) for w in range(2)]

        @pl.when(side == 1)
        def _():
            for s in slots:
                landed(s)

        tokens = jnp.concatenate([q_all[s] for s in slots], axis=0)
        scores = lax.dot_general(pas_v[...], tokens, NT, preferred_element_type=F32) + bias[...]
        highest = jnp.max(scores, axis=0, keepdims=True)
        spread = jnp.exp(scores - highest)
        total = jnp.sum(spread, axis=0, keepdims=True)
        low = spread.astype(BF16)
        level = highest + jnp.log(total)
        for w, s in enumerate(slots):
            cut = slice(w * tok, (w + 1) * tok)
            e_all[s] = low[:, cut]
            sums[pl.ds(s, 1), :] = total[:, cut]
            inner[pl.ds(s, 1), :] = level[:, cut]

    each(nz, lambda k: spread(me, devz(k)).start())
    pass_on(0)
    loads[1].wait()
    length = lengths[0]
    position = lax.broadcasted_iota(jnp.int32, bias.shape, 0)
    bias[...] = jnp.where(position < length, 0.0, LOW)
    flipped[...] = pas_v[...].astype(F32).T.astype(BF16)

    def relay(i):
        landed(at.slot(*at.arrival(i, core), core))
        pass_on(i)

    def relay_step(i):
        relay(i)

        @pl.when(i >= LAG)
        def _():
            attend(i - LAG)

    loop(1, half, relay_step)
    loop(half - LAG, half, attend)

    loads[7].wait()
    token = lax.broadcasted_iota(jnp.int32, (tok, wide), 0)
    lane = lax.broadcasted_iota(jnp.int32, (tok, wide), 1)
    spots = jnp.where(token // per == lax.rem(lane, own), 1.0, 0.0)
    slot_of = lax.broadcasted_iota(jnp.int32, (n, wide), 0)
    lane_of = lax.broadcasted_iota(jnp.int32, (n, wide), 1)
    mine = slot_of == lane_of // own
    grouped = exact(inner[...], spots)
    similar = jnp.sum(jnp.where(mine, grouped, 0.0), axis=0, keepdims=True)
    shift = jnp.log(jnp.full((1, wide), length, jnp.int32).astype(F32)) * per
    row_lane = lax.broadcasted_iota(jnp.int32, (1, wide), 1)
    chosen = jnp.zeros((1, wide), jnp.int32)
    for i in range(own):
        chosen = chosen + jnp.where(row_lane == me * own + i, positive[i], 0)
    msg[me, :, :wide] = similar - shift
    msg[me, :, wide:] = chosen.astype(F32)

    each(n, lambda k: remote(msg.at[me], msg.at[me], xs, xr, any_device(k)).start())

    for copy in loads[2:7]:
        copy.wait()

    def norm_block(i):
        cut = pl.ds(pl.multiple_of(i * block, block), block)
        ctx = context_grad[cut, :]
        hidden = resid_grad[cut, :].astype(F32) + jnp.dot(ctx, wo_v[...], preferred_element_type=F32)
        centred = hidden - jnp.mean(hidden, axis=1, keepdims=True)
        variance = jnp.mean(centred * centred, axis=1, keepdims=True)
        inv = 1.0 / jnp.sqrt(variance + 1e-05)
        norm = centred * inv
        normed[cut, :] = norm
        inv_std[cut, :] = jnp.broadcast_to(inv, (block, inv_std.shape[1]))
        scaled = norm * gain[...]
        scaled_t[:, cut] = scaled.T.astype(BF16)
        blend[cut, :] = jnp.dot(scaled.astype(BF16), cp_v[...], preferred_element_type=F32) / width
        ctx_t[:, cut] = ctx.astype(F32).T.astype(BF16)

    loop(0, 4, norm_block)
    flat = exact(jnp.broadcast_to(gain[...], (8, width)), cp_v[...].astype(F32))[0:1, :] / width

    arrived(msg.at[pl.ds(1, n - 1)], xr)

    everyone = msg[:, :, :wide]
    picked = jnp.sum(msg[:, :, wide:], axis=0)
    highest = jnp.max(everyone, axis=0)
    log_total = highest + jnp.log(jnp.sum(jnp.exp(everyone - highest[None]), axis=0))
    which = lax.broadcasted_iota(jnp.int32, everyone.shape, 0).astype(F32)
    score = jnp.sum(jnp.where(which == picked[None], everyone, 0.0), axis=0)
    average = jnp.sum(log_total - score, axis=1, keepdims=True) / wide
    loss[...] = jnp.broadcast_to(average, loss.shape)
    hit = jnp.where(picked == me.astype(F32), 1.0, 0.0)
    coefficient = jnp.exp(similar - shift - log_total) - hit
    laid = jnp.where(mine, jnp.broadcast_to(coefficient, mine.shape), 0.0)
    scale[...] = exact(laid, spots, NT) / sums[...]

    jobs = [dict(zip(JOB, rest[:count]), out=None, sums=[(q_s.at[k], q_r.at[k]) for k in range(4)])]
    stacked = dict(zip(JOB, rest[count : 2 * count]))
    for j in range(1, chunks + 2):
        k = chunks if j == 1 else j - 2
        job = {name: ref.at[k] for name, ref in stacked.items()}
        job["out"] = summed.at[k]
        job["sums"] = [(rs_s.at[m], rs_r.at[k, m]) for m in range(4)]
        job["outs"] = [(ag_s.at[m], ag_r.at[k, m]) for m in range(4)]
        jobs.append(job)

    def pair_copy(j):
        return remote(jobs[j]["snd"], jobs[j]["pl"], *jobs[j]["sums"][0], partner)

    def rs1_copy(j, t):
        there = pl.ds(lax.rem(i1 + t, n1) * plane, plane)
        return remote(jobs[j]["b1"].at[there], jobs[j]["l1"].at[t], *jobs[j]["sums"][1], dev1(t))

    def rs2_copy(j, t):
        there = pl.ds(lax.rem(i2 + t, n2) * nz, nz)
        return remote(jobs[j]["b2"].at[there], jobs[j]["l2"].at[t], *jobs[j]["sums"][2], dev2(t))

    def rs3_copy(j, k):
        return remote(jobs[j]["b3"].at[lax.rem(r + k, nz)], jobs[j]["l3"].at[k], *jobs[j]["sums"][3], devz(k))

    def out_copy(j, level, piece, device):
        return remote(piece, piece, *jobs[j]["outs"][level], device)

    def others(j, name, size):
        return jobs[j][name].at[pl.ds(1, size - 1)]

    def step1(j):
        job = jobs[j]
        pair_copy(j).wait_recv()
        if j > 0:
            job["b1"][...] = (job["own"][...] + job["pl"][...].astype(F32)).astype(BF16)
            kept = pl.ds(i1 * plane, plane)
            job["k1"][...] = job["own"][kept] + job["pl"][kept].astype(F32)
        else:

            def send_term(p):
                j1, j2, rr = p // plane, lax.rem(p // nz, n2), lax.rem(p, nz)
                s = at.slot(rr, j1, j2, core)
                total = u_all[s] * scale[pl.ds(s, 1), :] + job["pl"][p].astype(F32)
                job["b1"][p] = total.astype(BF16)

            def keep_term(q):
                p = i1 * plane + q
                j1, j2, rr = p // plane, lax.rem(p // nz, n2), lax.rem(p, nz)
                s = at.slot(rr, j1, j2, core)
                job["k1"][q] = u_all[s] * scale[pl.ds(s, 1), :] + job["pl"][p].astype(F32)

            loop(plane, half, lambda p: send_term(lax.rem(i1 * plane + p, half)))
            loop(0, plane, keep_term)
        for t in range(1, n1):
            rs1_copy(j, t).start()

    def step2(j):
        job = jobs[j]
        arrived(others(j, "l1", n1), job["sums"][1][1])
        total = job["k1"][...]
        for t in range(1, n1):
            total = total + job["l1"][t].astype(F32)
        job["b2"][...] = total.astype(BF16)
        job["k1"][...] = total
        for t in range(1, n2):
            rs2_copy(j, t).start()

    def step3(j):
        job = jobs[j]
        arrived(others(j, "l2", n2), job["sums"][2][1])
        total = job["k1"][pl.ds(i2 * nz, nz)]
        for t in range(1, n2):
            total = total + job["l2"][t].astype(F32)
        job["b3"][...] = total.astype(BF16)
        job["k2"][...] = total
        for k in range(1, nz):
            rs3_copy(j, k).start()

    def step4(j):
        job = jobs[j]
        arrived(others(j, "l3", nz), job["sums"][3][1])
        total = job["k2"][r]
        for k in range(1, nz):
            total = total + job["l3"][k].astype(F32)
        if job["out"] is None:
            query_grad[...] = total.T
        else:
            job["out"][core, place] = total.astype(BF16)
            for k in range(1, nz):
                out_copy(j, 0, job["out"].at[core, place], devz(k)).start()

    def step5(j):
        arrived(others(j, "l3", nz), jobs[j]["outs"][0][1])
        piece = jobs[j]["out"].at[core, pl.ds((i1 * n2 + i2) * nz, nz)]
        for t in range(1, n2):
            out_copy(j, 1, piece, dev2(t)).start()

    def step6(j):
        arrived(others(j, "l2", n2), jobs[j]["outs"][1][1])
        piece = jobs[j]["out"].at[core, pl.ds(i1 * plane, plane)]
        for t in range(1, n1):
            out_copy(j, 2, piece, dev1(t)).start()

    def step7(j):
        arrived(others(j, "l1", n1), jobs[j]["outs"][2][1])
        out_copy(j, 3, jobs[j]["out"].at[core], partner).start()

    def step8(j):
        arrived(jobs[j]["pl"], jobs[j]["outs"][3][1])

    emb_acc[...] = jnp.zeros_like(emb_acc)

    def emb_term(u):
        parts = []
        for v in range(16):
            s = u * 16 + v
            row = jnp.broadcast_to(scale[pl.ds(s, 1), :], (16, tok)).astype(BF16)
            spread = e_all[s]
            parts.append((spread.reshape(-1, 16, tok) * row[None]).reshape(spread.shape))
        weight = jnp.concatenate(parts, axis=1)
        tokens = q_all[pl.ds(u * 16, 16)].reshape(16 * tok, q_all.shape[2])
        emb_acc[...] += jnp.dot(weight, tokens, preferred_element_type=F32)

    loop(0, n // 16, emb_term)
    emb = emb_acc[...].astype(BF16)
    emb_acc[...] = emb.astype(F32)

    def grad_block(i):
        cut = pl.ds(pl.multiple_of(i * block, block), block)
        grad = emb_acc[cut, :]
        first = jnp.sum(grad * flat, axis=1, keepdims=True)
        second = jnp.sum(grad * blend[cut, :], axis=1, keepdims=True)
        scaled_grad = lax.dot_general(grad.astype(BF16), cp_v[...], NT, preferred_element_type=F32)
        hidden_grad = inv_std[cut, 0:1] * (scaled_grad * gain[...] - first - normed[cut, :] * second)
        resid_grad[cut, :] = hidden_grad.astype(BF16)

    loop(0, 4, grad_block)

    mid = width // 2

    def half_rows(ref, c):
        return ref[pl.ds(pl.multiple_of(c * mid, mid), mid), :]

    def proj_terms(c, name, group):
        span = chunks // 2 * cw
        term = jnp.dot(
            half_rows(ctx_t, c), resid_grad[:, group * span : (group + 1) * span], preferred_element_type=F32
        )
        for k in range(chunks // 2):
            ref = jobs[2 + group * (chunks // 2) + k][name]
            ref[...] = term[:, k * cw : (k + 1) * cw].reshape(ref.shape).astype(ref.dtype)

    def col_term(c, name):
        ref = jobs[1][name]
        term = jnp.dot(half_rows(scaled_t, c), emb_acc[...].astype(BF16), preferred_element_type=F32)
        ref[...] = term.reshape(ref.shape).astype(ref.dtype)

    for group in range(2):
        proj_terms(other, "snd", group)
        for k in range(chunks // 2):
            pair_copy(2 + group * (chunks // 2) + k).start()
    col_term(other, "snd")
    pair_copy(1).start()
    for group in range(2):
        proj_terms(core, "own", group)
    col_term(core, "own")

    def query_terms():
        def term(p):
            j1, j2, rr = p // plane, lax.rem(p // nz, n2), lax.rem(p, nz)
            s = at.slot(rr, j1, j2, other)
            jobs[0]["snd"][p] = (u_all[s] * scale[pl.ds(s, 1), :]).astype(BF16)

        loop(0, half, term)
        pair_copy(0).start()

    def below_terms(i):
        def below(u):
            for w in range(2):
                s = u * 4 + w * 2
                spread = jnp.concatenate([e_all[s], e_all[s + 1]], axis=1)
                term = jnp.dot(flipped[...], spread, preferred_element_type=F32)
                u_all[s] = term[:, :tok]
                u_all[s + 1] = term[:, tok:]

        loop(i * (n // 16), (i + 1) * (n // 16), below)

    def context_terms(i):
        cut = slice(i * (width // 4), (i + 1) * (width // 4))
        context_grad[:, cut] = lax.dot_general(
            resid_grad[...], wo_v[cut, :], NT, preferred_element_type=F32
        ).astype(BF16)

    fillers = [functools.partial(context_terms, i) for i in range(4)]
    fillers += [functools.partial(below_terms, i) for i in range(4)] + [query_terms]
    steps = [None, step1, step2, step3, step4, step5, step6, step7, step8]
    for code in ORDER:
        if code < 0:
            if fillers:
                fillers.pop(0)()
            continue
        if code == 1:
            while fillers:
                fillers.pop(0)()
        steps[code % 10](code // 10)

    arrived(q_all.at[pl.ds(1, n - 1)], gs)
    arrived(msg.at[pl.ds(1, n - 1)], xs)
    whole, first, second, third = stacked["pl"], stacked["l1"], stacked["l2"], stacked["l3"]
    first = first.at[:, pl.ds(1, n1 - 1)]
    second = second.at[:, pl.ds(1, n2 - 1)]
    third = third.at[:, pl.ds(1, nz - 1)]
    for sem, refs in ((rs_s, (whole, first, second, third)), (ag_s, (third, second, first, whole))):
        for m, ref in enumerate(refs):
            arrived(ref, sem.at[m])
    for m, ref in enumerate((jobs[0]["pl"], others(0, "l1", n1), others(0, "l2", n2), others(0, "l3", nz))):
        arrived(ref, q_s.at[m])


JOB = ("own", "snd", "pl", "b1", "k1", "l1", "b2", "l2", "b3", "k2", "l3")


def finish_kernel(main, gain, colbert, loss_in, query_in, resid_in, context_in,
                  proj_grad, colbert_grad, gain_grad, loss, query_grad, resid_grad, context_grad, proj_v, sem):
    copies = [
        pltpu.make_async_copy(resid_in, resid_grad, sem.at[0]),
        pltpu.make_async_copy(context_in, context_grad, sem.at[1]),
        pltpu.make_async_copy(query_in, query_grad, sem.at[2]),
    ]
    for copy in copies:
        copy.start()
    chunks, rows, cw = main.shape
    chunks = chunks - 1
    band = rows // 4
    for b in range(4):
        cut = slice(b * band, (b + 1) * band)
        for k in range(chunks):
            proj_v[cut, k * cw : (k + 1) * cw] = main[k, cut, :].astype(F32)
        copy = pltpu.make_async_copy(proj_v.at[cut], proj_grad.at[cut], sem.at[3 + b])
        copy.start()
        copies.append(copy)
    wide = main[chunks].astype(F32)
    colbert_grad[...] = wide
    ones = jnp.ones((8, wide.shape[1]), F32)
    summed = exact(ones, wide * colbert[...].astype(F32), NT)
    gain_grad[...] = summed[0:1, :] / gain[...]
    loss[...] = loss_in[:, 0:1]
    for copy in copies:
        copy.wait()


def stay(array):
    return pltpu.with_memory_space_constraint(array, pltpu.HBM)


def job_buffers(at, piece, cols, lead=(), own=True):
    shapes = [
        ((at.half if own else 1, piece, cols), F32),
        ((at.half, piece, cols), BF16),
        ((at.half, piece, cols), BF16),
        ((at.half, piece, cols), BF16),
        ((at.plane, piece, cols), F32),
        ((at.n1, at.plane, piece, cols), BF16),
        ((at.plane, piece, cols), BF16),
        ((at.n2, at.nz, piece, cols), BF16),
        ((at.nz, piece, cols), BF16),
        ((at.nz, piece, cols), F32),
        ((at.nz, piece, cols), BF16),
    ]
    return [pltpu.VMEM(lead + shape, kind) for shape, kind in shapes]


def body(sizes, query_emb, positive, passage_emb, lengths, residual, context, out_proj, norm_gain, colbert_proj):
    dp, neg = sizes["dp"], sizes["neg"]
    at = Grid(dp, neg)
    own, per, dim = query_emb.shape
    plen = passage_emb.shape[1]
    rows, width = residual.shape
    tok = own * per
    n = at.n
    chunks = width // dim
    cw = dim
    piece = width // (2 * at.half)
    dma = pltpu.SemaphoreType.DMA
    vm = pltpu.VMEM
    scratch = [
        vm((n, tok, dim), BF16),
        vm((n, 1, 2 * n * own), F32),
        vm((n, plen, tok), BF16),
        vm((n, dim, tok), F32),
        vm((n, tok), F32),
        vm((n, tok), F32),
        vm((n, tok), F32),
        vm((plen, 2 * tok), F32),
        vm((plen, dim), BF16),
        vm((dim, plen), BF16),
        vm((plen, dim), F32),
        pltpu.SMEM((own,), jnp.int32),
        vm((1, width), F32),
        vm((width, width), BF16),
        vm((width, dim), BF16),
        vm((width, rows), BF16),
        vm((width, rows), BF16),
        vm((rows, width), F32),
        vm((rows, 128), F32),
        vm((rows, dim), F32),
    ]
    scratch += job_buffers(at, dim, tok, own=False)
    scratch += job_buffers(at, piece, cw, (chunks + 1,))
    scratch += [
        dma((8,)),
        dma,
        dma((n,)),
        dma,
        dma,
        dma((4,)),
        dma((4,)),
        dma((4,)),
        dma((chunks + 1, 4)),
        dma((4,)),
        dma((chunks + 1, 4)),
    ]
    held = sum(math.prod(ref.shape) * jnp.dtype(ref.dtype).itemsize for ref in scratch[:-11])
    limit = min(held + held // 8 + 8 * 1024 * 1024, 67043328)
    loss, query_grad, resid_grad, context_grad, summed = pl.pallas_call(
        functools.partial(main_kernel, dp, neg, own, per),
        out_shape=[
            jax.ShapeDtypeStruct((1, 128), F32),
            jax.ShapeDtypeStruct((tok, dim), F32),
            jax.ShapeDtypeStruct((rows, width), BF16),
            jax.ShapeDtypeStruct((rows, width), BF16),
            jax.ShapeDtypeStruct((chunks + 1, 2, at.half, piece, cw), BF16),
        ],
        in_specs=[HBM, HBM, HBM, SMEM, HBM, HBM, HBM, HBM, HBM],
        out_specs=[VMEM] * 5,
        scratch_shapes=scratch,
        compiler_params=pltpu.CompilerParams(
            collective_id=1, has_side_effects=True, vmem_limit_bytes=limit
        ),
        name="maxsim_main",
    )(
        stay(query_emb.reshape(tok, dim)),
        stay(positive),
        stay(passage_emb.reshape(plen, dim)),
        lengths,
        stay(residual),
        stay(context),
        stay(out_proj),
        stay(norm_gain[None, :]),
        stay(colbert_proj),
    )
    proj_grad, colbert_grad, gain_grad, loss, query_grad, resid_grad, context_grad = pl.pallas_call(
        finish_kernel,
        out_shape=[
            jax.ShapeDtypeStruct((width, width), F32),
            jax.ShapeDtypeStruct((width, dim), F32),
            jax.ShapeDtypeStruct((1, width), F32),
            jax.ShapeDtypeStruct((1, 1), F32),
            jax.ShapeDtypeStruct((tok, dim), F32),
            jax.ShapeDtypeStruct((rows, width), BF16),
            jax.ShapeDtypeStruct((rows, width), BF16),
        ],
        in_specs=[VMEM] * 7,
        out_specs=[ANY, VMEM, VMEM, VMEM, ANY, ANY, ANY],
        scratch_shapes=[vm((width, width), F32), dma((7,))],
        compiler_params=pltpu.CompilerParams(vmem_limit_bytes=20000000),
        name="maxsim_finish",
    )(
        summed.reshape(chunks + 1, width, cw),
        norm_gain[None, :],
        colbert_proj,
        loss,
        query_grad,
        resid_grad,
        context_grad,
    )
    return (
        loss.reshape(()),
        query_grad.reshape(own, per, dim),
        resid_grad,
        context_grad,
        proj_grad,
        colbert_grad,
        gain_grad.reshape(width),
    )


def solution(mesh):
    sizes = {axis: mesh.shape[axis] for axis in ("dp", "neg")}
    split = ("dp", "neg")
    in_specs = (
        P(split, None, None),
        P(split),
        P(split, None, None),
        P(split),
        P(split, None),
        P(split, None),
        P(),
        P(),
        P(),
    )
    out_specs = (
        P(),
        P(split, None, None),
        P(split, None),
        P(split, None),
        P(),
        P(),
        P(),
    )
    return jax.shard_map(
        functools.partial(body, sizes), mesh=mesh, in_specs=in_specs, out_specs=out_specs, check_vma=False
    )
```

```python
import functools
import math

import jax
import jax.numpy as jnp
from jax import lax
from jax.experimental import pallas as pl
from jax.experimental.pallas import tpu as pltpu
from jax.sharding import PartitionSpec as P

MESH = pl.DeviceIdType.MESH
VMEM = pl.BlockSpec(memory_space=pltpu.VMEM)
SMEM = pl.BlockSpec(memory_space=pltpu.SMEM)
ANY = pl.BlockSpec(memory_space=pl.ANY)
HBM = pl.BlockSpec(memory_space=pltpu.HBM)
LOW = -1e30
F32 = jnp.float32
BF16 = jnp.bfloat16
NT = (((1,), (1,)), ((), ()))
LAG = 2
EARLY = 2
TURNED = (2, 4, 7, 8)
ORDER = (
    31, 21, -1, 51, 71, -1, -1, 32, 61, 41, -1, 22, -1, -1, 72, 91, -1, -1, 33, 52, 81, 11, -1, 23, 42, 62, 73, 53,
    34, 92, 24, 12, 82, 43, 1, 63, 93, 13, 83, 44, 25, 64, 35, 74, 2, 26, 94, 54, 14, 45, 84, 36, 65, 75, 46, 3,
    95, 55, 66, 15, 76, 85, 96, 56, 67, 16, 37, 4, 47, 27, 86, 97, 77, 38, 57, 68, 48, 17, 28, 78, 87, 58, 18, 98,
    88,
)


def exact(a, b, dims=(((1,), (0,)), ((), ()))):
    return lax.dot_general(a, b, dims, precision=lax.Precision.HIGHEST, preferred_element_type=F32)


def each(size, act):
    def turn(k, carry):
        act(k)
        return carry

    lax.fori_loop(1, size, turn, 0)


def loop(low, high, act):
    def turn(k, carry):
        act(k)
        return carry

    lax.fori_loop(low, high, turn, 0)


def remote(src, dst, send, recv, device):
    return pltpu.make_async_remote_copy(
        src_ref=src, dst_ref=dst, send_sem=send, recv_sem=recv, device_id=device, device_id_type=MESH
    )


class Grid:
    def __init__(self, dp, neg):
        groups = neg // 2
        self.dp, self.neg = dp, neg
        self.a = 2 if groups % 2 == 0 else 1
        self.b = groups // self.a
        self.n1, self.n2, self.nz = self.b, self.a, dp
        self.turned = self.a == self.b
        self.n = dp * neg
        self.half = self.n // 2
        self.plane = self.n2 * self.nz

    def locate(self):
        self.r, self.col = lax.axis_index("dp"), lax.axis_index("neg")
        self.core = lax.rem(self.col, 2)
        g = self.col // 2
        self.y, self.x = g // self.b, lax.rem(g, self.b)
        self.me = self.r * self.neg + self.col

    def flip(self, core, turn=0):
        return core * (1 - turn) + (1 - core) * turn if self.turned else 0 * core

    def own(self, core, turn=0):
        f = self.flip(core, turn)
        return (self.x * (1 - f) + self.y * f, self.y * (1 - f) + self.x * f)

    def column(self, j1, j2, core, turn=0):
        f = self.flip(core, turn)
        x, y = j1 * (1 - f) + j2 * f, j2 * (1 - f) + j1 * f
        return (y * self.b + x) * 2 + core

    def nearby(self, k):
        there, bit = self.r, 1
        while bit < self.nz:
            there = there + lax.rem(k // bit, 2) * bit * (1 - 2 * lax.rem(self.r // bit, 2))
            bit *= 2
        return there

    def arrival(self, i, core):
        i1, i2 = self.own(core)
        m2, m1, k = i // (self.n1 * self.nz), lax.rem(i // self.nz, self.n1), lax.rem(i, self.nz)
        return (self.nearby(k), lax.rem(i1 + m1, self.n1), lax.rem(i2 + m2, self.n2))

    def slot(self, rr, j1, j2, core):
        return rr * self.neg + self.column(j1, j2, core)


def main_kernel(dp, neg, own, per, query, positive_in, passage, lengths, resid, context, out_proj, gain_in, colbert,
                loss, query_grad, resid_grad, context_grad, summed, summed_map,
                q_all, msg, e_all, u_all, sums, inner, scale, bias, pas_v, flipped, emb_acc,
                positive, gain, wo_v, cp_v, ctx_t, scaled_t, normed, inv_std, blend, *rest):
    at = Grid(dp, neg)
    at.locate()
    r, core, me = at.r, at.core, at.me
    other = 1 - core
    i1, i2 = at.own(core)
    n, n1, n2, nz, half, plane = at.n, at.n1, at.n2, at.nz, at.half, at.plane
    partner = (r, at.col + 1 - 2 * core)
    away = 2 * (2 * r // nz) - 1
    tok = own * per
    wide = n * own
    rows, width = resid.shape
    block = rows // 4
    chunks = summed.shape[0]
    cw = summed.shape[-1]
    count = len(JOB)
    sems = rest[3 * count :]
    ld, gs, agr, xs, xr, q_s, q_r, c_s, c_r, rs_s, rs_r, ag_s, ag_r, ap_r = sems

    def dev1(t):
        return (r, at.column(lax.rem(i1 + t, n1), i2, core))

    def dev2(t):
        return (r, at.column(i1, lax.rem(i2 + t, n2), core))

    def devz(k):
        return (lax.rem(r + k, nz), at.col)

    def any_device(k):
        d = lax.rem(me + k * away + n, n)
        return (d // neg, lax.rem(d, neg))

    barrier = pltpu.get_barrier_semaphore()

    def greet(device):
        pl.semaphore_signal(barrier, inc=1, device_id=device, device_id_type=MESH)

    each(nz, lambda k: greet(devz(k)))
    each(n1, lambda t: greet(dev1(t)))
    each(n2, lambda t: greet(dev2(t)))
    greet(partner)
    loads = [
        pltpu.make_async_copy(query, q_all.at[me], ld.at[0]),
        pltpu.make_async_copy(passage, pas_v, ld.at[1]),
        pltpu.make_async_copy(context, context_grad, ld.at[2]),
        pltpu.make_async_copy(out_proj, wo_v, ld.at[3]),
        pltpu.make_async_copy(resid, resid_grad, ld.at[4]),
        pltpu.make_async_copy(colbert, cp_v, ld.at[5]),
        pltpu.make_async_copy(gain_in, gain, ld.at[6]),
        pltpu.make_async_copy(positive_in, positive, ld.at[7]),
    ]
    for copy in loads:
        copy.start()
    loads[0].wait()
    pl.semaphore_wait(barrier, nz + n1 + n2 - 2)

    def arrived(ref, sem):
        pltpu.make_async_copy(ref, ref, sem).wait()

    def spread(s, device):
        return remote(q_all.at[s], q_all.at[s], gs, agr.at[s], device)

    def landed(s):
        spread(s, partner).wait_recv()

    def pass_on(i):
        rr, j1, j2 = at.arrival(i, core)
        s = at.slot(rr, j1, j2, core)

        @pl.when(i < nz)
        def _():
            each(n1, lambda t: spread(s, dev1(t)).start())

        @pl.when(i < nz * n1)
        def _():
            each(n2, lambda t: spread(s, dev2(t)).start())

        spread(s, partner).start()

    def attend(v):
        u, side = v // 2, lax.rem(v, 2)
        whose = core * (1 - side) + other * side
        slots = [at.slot(*at.arrival(2 * u + w, whose), whose) for w in range(2)]

        @pl.when(side == 1)
        def _():
            for s in slots:
                landed(s)

        tokens = jnp.concatenate([q_all[s] for s in slots], axis=0)
        scores = lax.dot_general(pas_v[...], tokens, NT, preferred_element_type=F32) + bias[...]
        highest = jnp.max(scores, axis=0, keepdims=True)
        spread = jnp.exp(scores - highest)
        total = jnp.sum(spread, axis=0, keepdims=True)
        low = spread.astype(BF16)
        level = highest + jnp.log(total)
        for w, s in enumerate(slots):
            cut = slice(w * tok, (w + 1) * tok)
            e_all[s] = low[:, cut]
            sums[pl.ds(s, 1), :] = total[:, cut]
            inner[pl.ds(s, 1), :] = level[:, cut]

    each(nz, lambda k: spread(me, devz(k)).start())
    pass_on(0)
    loads[1].wait()
    length = lengths[0]
    position = lax.broadcasted_iota(jnp.int32, bias.shape, 0)
    bias[...] = jnp.where(position < length, 0.0, LOW)
    flipped[...] = pas_v[...].astype(F32).T.astype(BF16)

    def norm_block(i):
        cut = pl.ds(pl.multiple_of(i * block, block), block)
        ctx = context_grad[cut, :]
        hidden = resid_grad[cut, :].astype(F32) + jnp.dot(ctx, wo_v[...], preferred_element_type=F32)
        centred = hidden - jnp.mean(hidden, axis=1, keepdims=True)
        variance = jnp.mean(centred * centred, axis=1, keepdims=True)
        inv = 1.0 / jnp.sqrt(variance + 1e-05)
        norm = centred * inv
        normed[cut, :] = norm
        inv_std[cut, :] = jnp.broadcast_to(inv, (block, inv_std.shape[1]))
        scaled = norm * gain[...]
        scaled_t[:, cut] = scaled.T.astype(BF16)
        blend[cut, :] = jnp.dot(scaled.astype(BF16), cp_v[...], preferred_element_type=F32) / width
        ctx_t[:, cut] = ctx.astype(F32).T.astype(BF16)

    for copy in loads[2:7]:
        copy.wait()
    loop(0, EARLY, norm_block)

    def relay(i):
        landed(at.slot(*at.arrival(i, core), core))
        pass_on(i)

    def relay_step(i):
        relay(i)

        @pl.when(i >= LAG)
        def _():
            attend(i - LAG)

    loop(1, half, relay_step)
    loop(half - LAG, half, attend)

    loads[7].wait()
    token = lax.broadcasted_iota(jnp.int32, (tok, wide), 0)
    lane = lax.broadcasted_iota(jnp.int32, (tok, wide), 1)
    spots = jnp.where(token // per == lax.rem(lane, own), 1.0, 0.0)
    slot_of = lax.broadcasted_iota(jnp.int32, (n, wide), 0)
    lane_of = lax.broadcasted_iota(jnp.int32, (n, wide), 1)
    mine = slot_of == lane_of // own
    grouped = exact(inner[...], spots)
    similar = jnp.sum(jnp.where(mine, grouped, 0.0), axis=0, keepdims=True)
    shift = jnp.log(jnp.full((1, wide), length, jnp.int32).astype(F32)) * per
    row_lane = lax.broadcasted_iota(jnp.int32, (1, wide), 1)
    chosen = jnp.zeros((1, wide), jnp.int32)
    for i in range(own):
        chosen = chosen + jnp.where(row_lane == me * own + i, positive[i], 0)
    msg[me, :, :wide] = similar - shift
    msg[me, :, wide:] = chosen.astype(F32)

    each(n, lambda k: remote(msg.at[me], msg.at[me], xs, xr, any_device(k)).start())

    loop(EARLY, 4, norm_block)
    flat = exact(jnp.broadcast_to(gain[...], (8, width)), cp_v[...].astype(F32))[0:1, :] / width

    arrived(msg.at[pl.ds(1, n - 1)], xr)

    everyone = msg[:, :, :wide]
    picked = jnp.sum(msg[:, :, wide:], axis=0)
    highest = jnp.max(everyone, axis=0)
    log_total = highest + jnp.log(jnp.sum(jnp.exp(everyone - highest[None]), axis=0))
    which = lax.broadcasted_iota(jnp.int32, everyone.shape, 0).astype(F32)
    score = jnp.sum(jnp.where(which == picked[None], everyone, 0.0), axis=0)
    average = jnp.sum(log_total - score, axis=1, keepdims=True) / wide
    loss[...] = jnp.broadcast_to(average, loss.shape)
    hit = jnp.where(picked == me.astype(F32), 1.0, 0.0)
    coefficient = jnp.exp(similar - shift - log_total) - hit
    laid = jnp.where(mine, jnp.broadcast_to(coefficient, mine.shape), 0.0)
    scale[...] = exact(laid, spots, NT) / sums[...]

    jobs = [dict(zip(JOB, rest[:count]), out=None, sums=[(q_s.at[k], q_r.at[k]) for k in range(4)])]
    jobs.append(dict(zip(JOB, rest[count : 2 * count]), out=summed_map))
    jobs[1]["sums"] = [(c_s.at[m], c_r.at[m]) for m in range(4)]
    jobs[1]["outs"] = [(c_s.at[4 + m], c_r.at[4 + m]) for m in range(4)]
    stacked = dict(zip(JOB, rest[2 * count : 3 * count]))
    for k in range(chunks):
        job = {name: ref.at[k] for name, ref in stacked.items()}
        job["out"] = summed.at[k, core]
        job["sums"] = [(rs_s.at[m], rs_r.at[k, m]) for m in range(4)]
        job["outs"] = [(ag_s.at[m], ag_r.at[k, m]) for m in range(3)] + [(ag_s.at[3], ap_r)]
        jobs.append(job)
    for j, job in enumerate(jobs):
        turn = 1 if j in TURNED else 0
        job["at"] = h1, h2 = at.own(core, turn)
        job["place"] = (h1 * n2 + h2) * nz + r
        job["turn"] = turn

    def job1(j, t):
        h1, h2 = jobs[j]["at"]
        return (r, at.column(lax.rem(h1 + t, n1), h2, core, jobs[j]["turn"]))

    def job2(j, t):
        h1, h2 = jobs[j]["at"]
        return (r, at.column(h1, lax.rem(h2 + t, n2), core, jobs[j]["turn"]))

    def pair_copy(j):
        return remote(jobs[j]["snd"], jobs[j]["pl"], *jobs[j]["sums"][0], partner)

    def rs1_copy(j, t):
        there = pl.ds(lax.rem(jobs[j]["at"][0] + t, n1) * plane, plane)
        return remote(jobs[j]["b1"].at[there], jobs[j]["l1"].at[t], *jobs[j]["sums"][1], job1(j, t))

    def rs2_copy(j, t):
        there = pl.ds(lax.rem(jobs[j]["at"][1] + t, n2) * nz, nz)
        return remote(jobs[j]["b2"].at[there], jobs[j]["l2"].at[t], *jobs[j]["sums"][2], job2(j, t))

    def rs3_copy(j, k):
        return remote(jobs[j]["b3"].at[lax.rem(r + k, nz)], jobs[j]["l3"].at[k], *jobs[j]["sums"][3], devz(k))

    def out_copy(j, level, piece, device):
        return remote(piece, piece, *jobs[j]["outs"][level], device)

    def others(j, name, size):
        return jobs[j][name].at[pl.ds(1, size - 1)]

    def step1(j):
        job = jobs[j]
        pair_copy(j).wait_recv()
        if j > 0:
            job["b1"][...] = (job["own"][...] + job["pl"][...].astype(F32)).astype(BF16)
            kept = pl.ds(job["at"][0] * plane, plane)
            job["k1"][...] = job["own"][kept] + job["pl"][kept].astype(F32)
        else:

            def send_term(p):
                j1, j2, rr = p // plane, lax.rem(p // nz, n2), lax.rem(p, nz)
                s = at.slot(rr, j1, j2, core)
                total = u_all[s] * scale[pl.ds(s, 1), :] + job["pl"][p].astype(F32)
                job["b1"][p] = total.astype(BF16)

            def keep_term(q):
                p = i1 * plane + q
                j1, j2, rr = p // plane, lax.rem(p // nz, n2), lax.rem(p, nz)
                s = at.slot(rr, j1, j2, core)
                job["k1"][q] = u_all[s] * scale[pl.ds(s, 1), :] + job["pl"][p].astype(F32)

            loop(plane, half, lambda p: send_term(lax.rem(i1 * plane + p, half)))
            loop(0, plane, keep_term)
        for t in range(1, n1):
            rs1_copy(j, t).start()

    def step2(j):
        job = jobs[j]
        arrived(others(j, "l1", n1), job["sums"][1][1])
        total = job["k1"][...]
        for t in range(1, n1):
            total = total + job["l1"][t].astype(F32)
        job["b2"][...] = total.astype(BF16)
        job["k1"][...] = total
        for t in range(1, n2):
            rs2_copy(j, t).start()

    def step3(j):
        job = jobs[j]
        arrived(others(j, "l2", n2), job["sums"][2][1])
        total = job["k1"][pl.ds(job["at"][1] * nz, nz)]
        for t in range(1, n2):
            total = total + job["l2"][t].astype(F32)
        job["b3"][...] = total.astype(BF16)
        job["k2"][...] = total
        for k in range(1, nz):
            rs3_copy(j, k).start()

    def step4(j):
        job = jobs[j]
        arrived(others(j, "l3", nz), job["sums"][3][1])
        total = job["k2"][r]
        for k in range(1, nz):
            total = total + job["l3"][k].astype(F32)
        if job["out"] is None:
            query_grad[...] = total.T
        else:
            job["out"][job["place"]] = total.astype(BF16)
            for k in range(1, nz):
                out_copy(j, 0, job["out"].at[job["place"]], devz(k)).start()

    def step5(j):
        arrived(others(j, "l3", nz), jobs[j]["outs"][0][1])
        h1, h2 = jobs[j]["at"]
        piece = jobs[j]["out"].at[pl.ds((h1 * n2 + h2) * nz, nz)]
        for t in range(1, n2):
            out_copy(j, 1, piece, job2(j, t)).start()

    def step6(j):
        arrived(others(j, "l2", n2), jobs[j]["outs"][1][1])
        piece = jobs[j]["out"].at[pl.ds(jobs[j]["at"][0] * plane, plane)]
        for t in range(1, n1):
            out_copy(j, 2, piece, job1(j, t)).start()

    def step7(j):
        arrived(others(j, "l1", n1), jobs[j]["outs"][2][1])
        out_copy(j, 3, jobs[j]["out"], partner).start()

    emb_acc[...] = jnp.zeros_like(emb_acc)

    def emb_term(u):
        parts = []
        for v in range(16):
            s = u * 16 + v
            row = jnp.broadcast_to(scale[pl.ds(s, 1), :], (16, tok)).astype(BF16)
            spread = e_all[s]
            parts.append((spread.reshape(-1, 16, tok) * row[None]).reshape(spread.shape))
        weight = jnp.concatenate(parts, axis=1)
        tokens = q_all[pl.ds(u * 16, 16)].reshape(16 * tok, q_all.shape[2])
        emb_acc[...] += jnp.dot(weight, tokens, preferred_element_type=F32)

    loop(0, n // 16, emb_term)
    emb = emb_acc[...].astype(BF16)
    emb_acc[...] = emb.astype(F32)

    def grad_block(i):
        cut = pl.ds(pl.multiple_of(i * block, block), block)
        grad = emb_acc[cut, :]
        first = jnp.sum(grad * flat, axis=1, keepdims=True)
        second = jnp.sum(grad * blend[cut, :], axis=1, keepdims=True)
        scaled_grad = lax.dot_general(grad.astype(BF16), cp_v[...], NT, preferred_element_type=F32)
        hidden_grad = inv_std[cut, 0:1] * (scaled_grad * gain[...] - first - normed[cut, :] * second)
        resid_grad[cut, :] = hidden_grad.astype(BF16)

    loop(0, 4, grad_block)

    mid = width // 2

    def half_rows(ref, c):
        return ref[pl.ds(pl.multiple_of(c * mid, mid), mid), :]

    def proj_terms(c, name, group):
        span = chunks // 2 * cw
        term = jnp.dot(
            half_rows(ctx_t, c), resid_grad[:, group * span : (group + 1) * span], preferred_element_type=F32
        )
        for k in range(chunks // 2):
            ref = jobs[2 + group * (chunks // 2) + k][name]
            ref[...] = term[:, k * cw : (k + 1) * cw].reshape(ref.shape).astype(ref.dtype)

    def col_term(name):
        ref = jobs[1][name]
        term = jnp.dot(scaled_t[...], emb_acc[...].astype(BF16), preferred_element_type=F32)
        ref[...] = term.reshape(ref.shape).astype(ref.dtype)

    for group in range(2):
        proj_terms(other, "snd", group)
        for k in range(chunks // 2):
            pair_copy(2 + group * (chunks // 2) + k).start()

    @pl.when(core == 0)
    def _():
        col_term("snd")
        pair_copy(1).start()

    for group in range(2):
        proj_terms(core, "own", group)

    @pl.when(core == 1)
    def _():
        col_term("own")


    def query_terms():
        def term(p):
            j1, j2, rr = p // plane, lax.rem(p // nz, n2), lax.rem(p, nz)
            s = at.slot(rr, j1, j2, other)
            jobs[0]["snd"][p] = (u_all[s] * scale[pl.ds(s, 1), :]).astype(BF16)

        loop(0, half, term)
        pair_copy(0).start()

    def below_terms(i):
        def below(u):
            for w in range(2):
                s = u * 4 + w * 2
                spread = jnp.concatenate([e_all[s], e_all[s + 1]], axis=1)
                term = jnp.dot(flipped[...], spread, preferred_element_type=F32)
                u_all[s] = term[:, :tok]
                u_all[s + 1] = term[:, tok:]

        loop(i * (n // 16), (i + 1) * (n // 16), below)

    def context_terms(i):
        cut = slice(i * (width // 4), (i + 1) * (width // 4))
        context_grad[:, cut] = lax.dot_general(
            resid_grad[...], wo_v[cut, :], NT, preferred_element_type=F32
        ).astype(BF16)

    fillers = [functools.partial(context_terms, i) for i in range(4)]
    fillers += [functools.partial(below_terms, i) for i in range(4)] + [query_terms]
    steps = [None, step1, step2, step3, step4, step5, step6, step7]
    for code in ORDER:
        if code < 0:
            if fillers:
                fillers.pop(0)()
            continue
        if code == 1:
            while fillers:
                fillers.pop(0)()
        if code % 10 == len(steps):
            continue
        if code // 10 == 1:
            pl.when(core == 1)(functools.partial(steps[code % 10], 1))
        else:
            steps[code % 10](code // 10)

    arrived(stacked["pl"], ap_r)
    arrived(q_all.at[pl.ds(1, n - 1)], gs)
    arrived(msg.at[pl.ds(1, n - 1)], xs)

    @pl.when(core == 0)
    def _():
        arrived(jobs[1]["pl"], c_s.at[0])
        arrived(jobs[1]["pl"], c_r.at[7])

    @pl.when(core == 1)
    def _():
        parts = [others(1, "l1", n1), others(1, "l2", n2), others(1, "l3", nz)]
        for m, ref in enumerate(parts + parts[::-1] + [jobs[1]["pl"]]):
            arrived(ref, c_s.at[1 + m])

    whole, first, second, third = stacked["pl"], stacked["l1"], stacked["l2"], stacked["l3"]
    first = first.at[:, pl.ds(1, n1 - 1)]
    second = second.at[:, pl.ds(1, n2 - 1)]
    third = third.at[:, pl.ds(1, nz - 1)]
    for sem, refs in ((rs_s, (whole, first, second, third)), (ag_s, (third, second, first, whole))):
        for m, ref in enumerate(refs):
            arrived(ref, sem.at[m])
    for m, ref in enumerate((jobs[0]["pl"], others(0, "l1", n1), others(0, "l2", n2), others(0, "l3", nz))):
        arrived(ref, q_s.at[m])


JOB = ("own", "snd", "pl", "b1", "k1", "l1", "b2", "l2", "b3", "k2", "l3")


def finish_kernel(main, col, gain, colbert, loss_in, query_in, resid_in, context_in,
                  proj_grad, colbert_grad, gain_grad, loss, query_grad, resid_grad, context_grad,
                  proj_v, colbert_v, gain_v, sem):
    copies = []

    def send(src, dst):
        copy = pltpu.make_async_copy(src, dst, sem.at[len(copies)])
        copy.start()
        copies.append(copy)

    send(resid_in, resid_grad)
    send(context_in, context_grad)
    send(query_in, query_grad)
    loss[...] = loss_in[:, 0:1]
    chunks, rows, cw = main.shape
    wide = col[...].astype(F32)
    colbert_v[...] = wide
    send(colbert_v, colbert_grad)
    band = rows // 4
    for b in range(4):
        cut = slice(b * band, (b + 1) * band)
        for k in range(chunks):
            proj_v[cut, k * cw : (k + 1) * cw] = main[k, cut, :].astype(F32)
        send(proj_v.at[cut], proj_grad.at[cut])
    ones = jnp.ones((8, wide.shape[1]), F32)
    gain_v[...] = exact(ones, wide * colbert[...].astype(F32), NT)[0:1, :] / gain[...]
    send(gain_v, gain_grad)
    for copy in copies:
        copy.wait()


def stay(array):
    return pltpu.with_memory_space_constraint(array, pltpu.HBM)


def job_buffers(at, piece, cols, lead=(), own=True):
    shapes = [
        ((at.half if own else 1, piece, cols), F32),
        ((at.half, piece, cols), BF16),
        ((at.half, piece, cols), BF16),
        ((at.half, piece, cols), BF16),
        ((at.plane, piece, cols), F32),
        ((at.n1, at.plane, piece, cols), BF16),
        ((at.plane, piece, cols), BF16),
        ((at.n2, at.nz, piece, cols), BF16),
        ((at.nz, piece, cols), BF16),
        ((at.nz, piece, cols), F32),
        ((at.nz, piece, cols), BF16),
    ]
    return [pltpu.VMEM(lead + shape, kind) for shape, kind in shapes]


def body(sizes, query_emb, positive, passage_emb, lengths, residual, context, out_proj, norm_gain, colbert_proj):
    dp, neg = sizes["dp"], sizes["neg"]
    at = Grid(dp, neg)
    own, per, dim = query_emb.shape
    plen = passage_emb.shape[1]
    rows, width = residual.shape
    tok = own * per
    n = at.n
    chunks = width // dim
    cw = dim
    piece = width // (2 * at.half)
    dma = pltpu.SemaphoreType.DMA
    vm = pltpu.VMEM
    scratch = [
        vm((n, tok, dim), BF16),
        vm((n, 1, 2 * n * own), F32),
        vm((n, plen, tok), BF16),
        vm((n, dim, tok), F32),
        vm((n, tok), F32),
        vm((n, tok), F32),
        vm((n, tok), F32),
        vm((plen, 2 * tok), F32),
        vm((plen, dim), BF16),
        vm((dim, plen), BF16),
        vm((plen, dim), F32),
        pltpu.SMEM((own,), jnp.int32),
        vm((1, width), F32),
        vm((width, width), BF16),
        vm((width, dim), BF16),
        vm((width, rows), BF16),
        vm((width, rows), BF16),
        vm((rows, width), F32),
        vm((rows, 128), F32),
        vm((rows, dim), F32),
    ]
    scratch += job_buffers(at, dim, tok, own=False)
    scratch += job_buffers(at, 2 * piece, cw)
    scratch += job_buffers(at, piece, cw, (chunks,))
    scratch += [
        dma((8,)),
        dma,
        dma((n,)),
        dma,
        dma,
        dma((4,)),
        dma((4,)),
        dma((8,)),
        dma((8,)),
        dma((4,)),
        dma((chunks, 4)),
        dma((4,)),
        dma((chunks, 3)),
        dma,
    ]
    held = sum(math.prod(ref.shape) * jnp.dtype(ref.dtype).itemsize for ref in scratch[:-14])
    limit = min(held + held // 8 + 8 * 1024 * 1024, 67043328)
    loss, query_grad, resid_grad, context_grad, summed, summed_map = pl.pallas_call(
        functools.partial(main_kernel, dp, neg, own, per),
        out_shape=[
            jax.ShapeDtypeStruct((1, 128), F32),
            jax.ShapeDtypeStruct((tok, dim), F32),
            jax.ShapeDtypeStruct((rows, width), BF16),
            jax.ShapeDtypeStruct((rows, width), BF16),
            jax.ShapeDtypeStruct((chunks, 2, at.half, piece, cw), BF16),
            jax.ShapeDtypeStruct((at.half, 2 * piece, cw), BF16),
        ],
        in_specs=[HBM, HBM, HBM, SMEM, HBM, HBM, HBM, HBM, HBM],
        out_specs=[VMEM] * 6,
        scratch_shapes=scratch,
        compiler_params=pltpu.CompilerParams(
            collective_id=1, has_side_effects=True, vmem_limit_bytes=limit
        ),
        name="maxsim_main",
    )(
        stay(query_emb.reshape(tok, dim)),
        stay(positive),
        stay(passage_emb.reshape(plen, dim)),
        lengths,
        stay(residual),
        stay(context),
        stay(out_proj),
        stay(norm_gain[None, :]),
        stay(colbert_proj),
    )
    proj_grad, colbert_grad, gain_grad, loss, query_grad, resid_grad, context_grad = pl.pallas_call(
        finish_kernel,
        out_shape=[
            jax.ShapeDtypeStruct((width, width), F32),
            jax.ShapeDtypeStruct((width, dim), F32),
            jax.ShapeDtypeStruct((1, width), F32),
            jax.ShapeDtypeStruct((1, 1), F32),
            jax.ShapeDtypeStruct((tok, dim), F32),
            jax.ShapeDtypeStruct((rows, width), BF16),
            jax.ShapeDtypeStruct((rows, width), BF16),
        ],
        in_specs=[VMEM] * 8,
        out_specs=[ANY, ANY, ANY, VMEM, ANY, ANY, ANY],
        scratch_shapes=[vm((width, width), F32), vm((width, dim), F32), vm((1, width), F32), dma((10,))],
        compiler_params=pltpu.CompilerParams(vmem_limit_bytes=20000000),
        name="maxsim_finish",
    )(
        summed.reshape(chunks, width, cw),
        summed_map.reshape(width, dim),
        norm_gain[None, :],
        colbert_proj,
        loss,
        query_grad,
        resid_grad,
        context_grad,
    )
    return (
        loss.reshape(()),
        query_grad.reshape(own, per, dim),
        resid_grad,
        context_grad,
        proj_grad,
        colbert_grad,
        gain_grad.reshape(width),
    )


def solution(mesh):
    sizes = {axis: mesh.shape[axis] for axis in ("dp", "neg")}
    split = ("dp", "neg")
    in_specs = (
        P(split, None, None),
        P(split),
        P(split, None, None),
        P(split),
        P(split, None),
        P(split, None),
        P(),
        P(),
        P(),
    )
    out_specs = (
        P(),
        P(split, None, None),
        P(split, None),
        P(split, None),
        P(),
        P(),
        P(),
    )
    return jax.shard_map(
        functools.partial(body, sizes), mesh=mesh, in_specs=in_specs, out_specs=out_specs, check_vma=False
    )
```

```python
import functools
import math

import jax
import jax.numpy as jnp
from jax import lax
from jax.experimental import pallas as pl
from jax.experimental.pallas import tpu as pltpu
from jax.sharding import PartitionSpec as P

MESH = pl.DeviceIdType.MESH
VMEM = pl.BlockSpec(memory_space=pltpu.VMEM)
SMEM = pl.BlockSpec(memory_space=pltpu.SMEM)
ANY = pl.BlockSpec(memory_space=pl.ANY)
HBM = pl.BlockSpec(memory_space=pltpu.HBM)
LOW = -1e30
F32 = jnp.float32
BF16 = jnp.bfloat16
NT = (((1,), (1,)), ((), ()))
LAG = 2
EARLY = 2
TURNED = ()
ORDER = (
    21, 31, 41, 51, 61, -1, -1, -1, 22, 32, 71, -1, -1, 42, 81, -1, 62, 52, 91, 23, -1, -1, 33, -1, 43, 72, 11, 63,
    82, 53, 24, 92, 73, 34, 12, 1, 83, 93, 64, 44, 25, 13, 54, 35, 2, 84, 94, 45, 65, 74, 36, 26, 14, 55, 85, 66,
    46, 75, 95, 3, 56, 15, 86, 27, 76, 96, 47, 37, 57, 16, 67, 87, 28, 77, 4, 68, 38, 97, 88, 58, 78, 48, 17, 98,
    18,
)


def exact(a, b, dims=(((1,), (0,)), ((), ()))):
    return lax.dot_general(a, b, dims, precision=lax.Precision.HIGHEST, preferred_element_type=F32)


def each(size, act):
    def turn(k, carry):
        act(k)
        return carry

    lax.fori_loop(1, size, turn, 0)


def loop(low, high, act):
    def turn(k, carry):
        act(k)
        return carry

    lax.fori_loop(low, high, turn, 0)


def remote(src, dst, send, recv, device):
    return pltpu.make_async_remote_copy(
        src_ref=src, dst_ref=dst, send_sem=send, recv_sem=recv, device_id=device, device_id_type=MESH
    )


class Grid:
    def __init__(self, dp, neg):
        groups = neg // 2
        self.dp, self.neg = dp, neg
        self.a = 2 if groups % 2 == 0 else 1
        self.b = groups // self.a
        self.n1, self.n2, self.nz = self.b, self.a, dp
        self.turned = self.a == self.b
        self.n = dp * neg
        self.half = self.n // 2
        self.plane = self.n2 * self.nz

    def locate(self):
        self.r, self.col = lax.axis_index("dp"), lax.axis_index("neg")
        self.core = lax.rem(self.col, 2)
        g = self.col // 2
        self.y, self.x = g // self.b, lax.rem(g, self.b)
        self.me = self.r * self.neg + self.col

    def flip(self, core, turn=0):
        return core * (1 - turn) + (1 - core) * turn if self.turned else 0 * core

    def own(self, core, turn=0):
        f = self.flip(core, turn)
        return (self.x * (1 - f) + self.y * f, self.y * (1 - f) + self.x * f)

    def column(self, j1, j2, core, turn=0):
        f = self.flip(core, turn)
        x, y = j1 * (1 - f) + j2 * f, j2 * (1 - f) + j1 * f
        return (y * self.b + x) * 2 + core

    def nearby(self, k):
        there, bit = self.r, 1
        while bit < self.nz:
            there = there + lax.rem(k // bit, 2) * bit * (1 - 2 * lax.rem(self.r // bit, 2))
            bit *= 2
        return there

    def arrival(self, i, core):
        i1, i2 = self.own(core)
        m2, m1, k = i // (self.n1 * self.nz), lax.rem(i // self.nz, self.n1), lax.rem(i, self.nz)
        return (self.nearby(k), lax.rem(i1 + m1, self.n1), lax.rem(i2 + m2, self.n2))

    def slot(self, rr, j1, j2, core):
        return rr * self.neg + self.column(j1, j2, core)


def main_kernel(dp, neg, own, per, query, positive_in, passage, lengths, resid, context, out_proj, gain_in, colbert,
                loss, query_grad, resid_grad, context_grad, summed, summed_map,
                q_all, msg, e_all, u_all, sums, inner, scale, bias, pas_v, flipped, emb_acc,
                positive, gain, wo_v, cp_v, ctx_t, scaled_t, normed, inv_std, blend, *rest):
    at = Grid(dp, neg)
    at.locate()
    r, core, me = at.r, at.core, at.me
    other = 1 - core
    i1, i2 = at.own(core)
    n, n1, n2, nz, half, plane = at.n, at.n1, at.n2, at.nz, at.half, at.plane
    partner = (r, at.col + 1 - 2 * core)
    away = 2 * (2 * r // nz) - 1
    tok = own * per
    wide = n * own
    rows, width = resid.shape
    block = rows // 4
    chunks = summed.shape[0]
    cw = summed.shape[-1]
    count = len(JOB)
    sems = rest[3 * count :]
    ld, gs, agr, xs, xr, q_s, q_r, c_s, c_r, rs_s, rs_r, ag_s, ag_r, ap_r = sems

    def dev1(t):
        return (r, at.column(lax.rem(i1 + t, n1), i2, core))

    def dev2(t):
        return (r, at.column(i1, lax.rem(i2 + t, n2), core))

    def devz(k):
        return (lax.rem(r + k, nz), at.col)

    def any_device(k):
        d = lax.rem(me + k * away + n, n)
        return (d // neg, lax.rem(d, neg))

    barrier = pltpu.get_barrier_semaphore()

    def greet(device):
        pl.semaphore_signal(barrier, inc=1, device_id=device, device_id_type=MESH)

    each(nz, lambda k: greet(devz(k)))
    each(n1, lambda t: greet(dev1(t)))
    each(n2, lambda t: greet(dev2(t)))
    greet(partner)
    loads = [
        pltpu.make_async_copy(query, q_all.at[me], ld.at[0]),
        pltpu.make_async_copy(passage, pas_v, ld.at[1]),
        pltpu.make_async_copy(context, context_grad, ld.at[2]),
        pltpu.make_async_copy(out_proj, wo_v, ld.at[3]),
        pltpu.make_async_copy(resid, resid_grad, ld.at[4]),
        pltpu.make_async_copy(colbert, cp_v, ld.at[5]),
        pltpu.make_async_copy(gain_in, gain, ld.at[6]),
        pltpu.make_async_copy(positive_in, positive, ld.at[7]),
    ]
    for copy in loads:
        copy.start()
    loads[0].wait()
    pl.semaphore_wait(barrier, nz + n1 + n2 - 2)

    def arrived(ref, sem):
        pltpu.make_async_copy(ref, ref, sem).wait()

    def spread(s, device):
        return remote(q_all.at[s], q_all.at[s], gs, agr.at[s], device)

    def landed(s):
        spread(s, partner).wait_recv()

    def pass_on(i):
        rr, j1, j2 = at.arrival(i, core)
        s = at.slot(rr, j1, j2, core)

        @pl.when(i < nz)
        def _():
            each(n1, lambda t: spread(s, dev1(t)).start())

        @pl.when(i < nz * n1)
        def _():
            each(n2, lambda t: spread(s, dev2(t)).start())

        spread(s, partner).start()

    def attend(v):
        u, side = v // 2, lax.rem(v, 2)
        whose = core * (1 - side) + other * side
        slots = [at.slot(*at.arrival(2 * u + w, whose), whose) for w in range(2)]

        @pl.when(side == 1)
        def _():
            for s in slots:
                landed(s)

        tokens = jnp.concatenate([q_all[s] for s in slots], axis=0)
        scores = lax.dot_general(pas_v[...], tokens, NT, preferred_element_type=F32) + bias[...]
        highest = jnp.max(scores, axis=0, keepdims=True)
        spread = jnp.exp(scores - highest)
        total = jnp.sum(spread, axis=0, keepdims=True)
        low = spread.astype(BF16)
        level = highest + jnp.log(total)
        for w, s in enumerate(slots):
            cut = slice(w * tok, (w + 1) * tok)
            e_all[s] = low[:, cut]
            sums[pl.ds(s, 1), :] = total[:, cut]
            inner[pl.ds(s, 1), :] = level[:, cut]

    each(nz, lambda k: spread(me, devz(k)).start())
    pass_on(0)
    loads[1].wait()
    length = lengths[0]
    position = lax.broadcasted_iota(jnp.int32, bias.shape, 0)
    bias[...] = jnp.where(position < length, 0.0, LOW)
    flipped[...] = pas_v[...].astype(F32).T.astype(BF16)

    def norm_block(i):
        cut = pl.ds(pl.multiple_of(i * block, block), block)
        ctx = context_grad[cut, :]
        hidden = resid_grad[cut, :].astype(F32) + jnp.dot(ctx, wo_v[...], preferred_element_type=F32)
        centred = hidden - jnp.mean(hidden, axis=1, keepdims=True)
        variance = jnp.mean(centred * centred, axis=1, keepdims=True)
        inv = 1.0 / jnp.sqrt(variance + 1e-05)
        norm = centred * inv
        normed[cut, :] = norm
        inv_std[cut, :] = jnp.broadcast_to(inv, (block, inv_std.shape[1]))
        scaled = norm * gain[...]
        scaled_t[:, cut] = scaled.T.astype(BF16)
        blend[cut, :] = jnp.dot(scaled.astype(BF16), cp_v[...], preferred_element_type=F32) / width
        ctx_t[:, cut] = ctx.astype(F32).T.astype(BF16)

    for copy in loads[2:7]:
        copy.wait()
    loop(0, EARLY, norm_block)

    def relay(i):
        landed(at.slot(*at.arrival(i, core), core))
        pass_on(i)

    def relay_step(i):
        relay(i)

        @pl.when(i >= LAG)
        def _():
            attend(i - LAG)

    loop(1, half, relay_step)
    loop(half - LAG, half, attend)

    loads[7].wait()
    token = lax.broadcasted_iota(jnp.int32, (tok, wide), 0)
    lane = lax.broadcasted_iota(jnp.int32, (tok, wide), 1)
    spots = jnp.where(token // per == lax.rem(lane, own), 1.0, 0.0)
    slot_of = lax.broadcasted_iota(jnp.int32, (n, wide), 0)
    lane_of = lax.broadcasted_iota(jnp.int32, (n, wide), 1)
    mine = slot_of == lane_of // own
    grouped = exact(inner[...], spots)
    similar = jnp.sum(jnp.where(mine, grouped, 0.0), axis=0, keepdims=True)
    shift = jnp.log(jnp.full((1, wide), length, jnp.int32).astype(F32)) * per
    row_lane = lax.broadcasted_iota(jnp.int32, (1, wide), 1)
    chosen = jnp.zeros((1, wide), jnp.int32)
    for i in range(own):
        chosen = chosen + jnp.where(row_lane == me * own + i, positive[i], 0)
    msg[me, :, :wide] = similar - shift
    msg[me, :, wide:] = chosen.astype(F32)

    each(n, lambda k: remote(msg.at[me], msg.at[me], xs, xr, any_device(k)).start())

    loop(EARLY, 4, norm_block)
    flat = exact(jnp.broadcast_to(gain[...], (8, width)), cp_v[...].astype(F32))[0:1, :] / width

    arrived(msg.at[pl.ds(1, n - 1)], xr)

    everyone = msg[:, :, :wide]
    picked = jnp.sum(msg[:, :, wide:], axis=0)
    highest = jnp.max(everyone, axis=0)
    log_total = highest + jnp.log(jnp.sum(jnp.exp(everyone - highest[None]), axis=0))
    which = lax.broadcasted_iota(jnp.int32, everyone.shape, 0).astype(F32)
    score = jnp.sum(jnp.where(which == picked[None], everyone, 0.0), axis=0)
    average = jnp.sum(log_total - score, axis=1, keepdims=True) / wide
    loss[...] = jnp.broadcast_to(average, loss.shape)
    hit = jnp.where(picked == me.astype(F32), 1.0, 0.0)
    coefficient = jnp.exp(similar - shift - log_total) - hit
    laid = jnp.where(mine, jnp.broadcast_to(coefficient, mine.shape), 0.0)
    scale[...] = exact(laid, spots, NT) / sums[...]

    jobs = [dict(zip(JOB, rest[:count]), out=None, sums=[(q_s.at[k], q_r.at[k]) for k in range(4)])]
    jobs.append(dict(zip(JOB, rest[count : 2 * count]), out=summed_map))
    jobs[1]["sums"] = [(c_s.at[m], c_r.at[m]) for m in range(4)]
    jobs[1]["outs"] = [(c_s.at[4 + m], c_r.at[4 + m]) for m in range(4)]
    stacked = dict(zip(JOB, rest[2 * count : 3 * count]))
    for k in range(chunks):
        job = {name: ref.at[k] for name, ref in stacked.items()}
        job["out"] = summed.at[k, core]
        job["sums"] = [(rs_s.at[m], rs_r.at[k, m]) for m in range(4)]
        job["outs"] = [(ag_s.at[m], ag_r.at[k, m]) for m in range(3)] + [(ag_s.at[3], ap_r)]
        jobs.append(job)
    for j, job in enumerate(jobs):
        turn = 1 if j in TURNED else 0
        job["at"] = h1, h2 = at.own(core, turn)
        job["place"] = (h1 * n2 + h2) * nz + r
        job["turn"] = turn

    def job1(j, t):
        h1, h2 = jobs[j]["at"]
        return (r, at.column(lax.rem(h1 + t, n1), h2, core, jobs[j]["turn"]))

    def job2(j, t):
        h1, h2 = jobs[j]["at"]
        return (r, at.column(h1, lax.rem(h2 + t, n2), core, jobs[j]["turn"]))

    def pair_copy(j):
        return remote(jobs[j]["snd"], jobs[j]["pl"], *jobs[j]["sums"][0], partner)

    def rs1_copy(j, t):
        there = pl.ds(lax.rem(jobs[j]["at"][0] + t, n1) * plane, plane)
        return remote(jobs[j]["b1"].at[there], jobs[j]["l1"].at[t], *jobs[j]["sums"][1], job1(j, t))

    def rs2_copy(j, t):
        there = pl.ds(lax.rem(jobs[j]["at"][1] + t, n2) * nz, nz)
        return remote(jobs[j]["b2"].at[there], jobs[j]["l2"].at[t], *jobs[j]["sums"][2], job2(j, t))

    def rs3_copy(j, k):
        return remote(jobs[j]["b3"].at[lax.rem(r + k, nz)], jobs[j]["l3"].at[k], *jobs[j]["sums"][3], devz(k))

    def out_copy(j, level, piece, device):
        return remote(piece, piece, *jobs[j]["outs"][level], device)

    def others(j, name, size):
        return jobs[j][name].at[pl.ds(1, size - 1)]

    def step1(j):
        job = jobs[j]
        pair_copy(j).wait_recv()
        if j > 0:
            job["b1"][...] = (job["own"][...] + job["pl"][...].astype(F32)).astype(BF16)
            kept = pl.ds(job["at"][0] * plane, plane)
            job["k1"][...] = job["own"][kept] + job["pl"][kept].astype(F32)
        else:

            def send_term(p):
                j1, j2, rr = p // plane, lax.rem(p // nz, n2), lax.rem(p, nz)
                s = at.slot(rr, j1, j2, core)
                total = u_all[s] * scale[pl.ds(s, 1), :] + job["pl"][p].astype(F32)
                job["b1"][p] = total.astype(BF16)

            def keep_term(q):
                p = i1 * plane + q
                j1, j2, rr = p // plane, lax.rem(p // nz, n2), lax.rem(p, nz)
                s = at.slot(rr, j1, j2, core)
                job["k1"][q] = u_all[s] * scale[pl.ds(s, 1), :] + job["pl"][p].astype(F32)

            loop(plane, half, lambda p: send_term(lax.rem(i1 * plane + p, half)))
            loop(0, plane, keep_term)
        for t in range(1, n1):
            rs1_copy(j, t).start()

    def step2(j):
        job = jobs[j]
        arrived(others(j, "l1", n1), job["sums"][1][1])
        total = job["k1"][...]
        for t in range(1, n1):
            total = total + job["l1"][t].astype(F32)
        job["b2"][...] = total.astype(BF16)
        job["k1"][...] = total
        for t in range(1, n2):
            rs2_copy(j, t).start()

    def step3(j):
        job = jobs[j]
        arrived(others(j, "l2", n2), job["sums"][2][1])
        total = job["k1"][pl.ds(job["at"][1] * nz, nz)]
        for t in range(1, n2):
            total = total + job["l2"][t].astype(F32)
        job["b3"][...] = total.astype(BF16)
        job["k2"][...] = total
        for k in range(1, nz):
            rs3_copy(j, k).start()

    def step4(j):
        job = jobs[j]
        arrived(others(j, "l3", nz), job["sums"][3][1])
        total = job["k2"][r]
        for k in range(1, nz):
            total = total + job["l3"][k].astype(F32)
        if job["out"] is None:
            query_grad[...] = total.T
        else:
            job["out"][job["place"]] = total.astype(BF16)
            for k in range(1, nz):
                out_copy(j, 0, job["out"].at[job["place"]], devz(k)).start()

    def step5(j):
        arrived(others(j, "l3", nz), jobs[j]["outs"][0][1])
        h1, h2 = jobs[j]["at"]
        piece = jobs[j]["out"].at[pl.ds((h1 * n2 + h2) * nz, nz)]
        for t in range(1, n2):
            out_copy(j, 1, piece, job2(j, t)).start()

    def step6(j):
        arrived(others(j, "l2", n2), jobs[j]["outs"][1][1])
        piece = jobs[j]["out"].at[pl.ds(jobs[j]["at"][0] * plane, plane)]
        for t in range(1, n1):
            out_copy(j, 2, piece, job1(j, t)).start()

    def step7(j):
        arrived(others(j, "l1", n1), jobs[j]["outs"][2][1])
        out_copy(j, 3, jobs[j]["out"], partner).start()

    emb_acc[...] = jnp.zeros_like(emb_acc)

    def emb_term(u):
        parts = []
        for v in range(16):
            s = u * 16 + v
            row = jnp.broadcast_to(scale[pl.ds(s, 1), :], (16, tok)).astype(BF16)
            spread = e_all[s]
            parts.append((spread.reshape(-1, 16, tok) * row[None]).reshape(spread.shape))
        weight = jnp.concatenate(parts, axis=1)
        tokens = q_all[pl.ds(u * 16, 16)].reshape(16 * tok, q_all.shape[2])
        emb_acc[...] += jnp.dot(weight, tokens, preferred_element_type=F32)

    loop(0, n // 16, emb_term)
    emb = emb_acc[...].astype(BF16)
    emb_acc[...] = emb.astype(F32)

    def grad_block(i):
        cut = pl.ds(pl.multiple_of(i * block, block), block)
        grad = emb_acc[cut, :]
        first = jnp.sum(grad * flat, axis=1, keepdims=True)
        second = jnp.sum(grad * blend[cut, :], axis=1, keepdims=True)
        scaled_grad = lax.dot_general(grad.astype(BF16), cp_v[...], NT, preferred_element_type=F32)
        hidden_grad = inv_std[cut, 0:1] * (scaled_grad * gain[...] - first - normed[cut, :] * second)
        resid_grad[cut, :] = hidden_grad.astype(BF16)

    loop(0, 4, grad_block)

    mid = width // 2

    def half_rows(ref, c):
        return ref[pl.ds(pl.multiple_of(c * mid, mid), mid), :]

    def proj_terms(c, name, group):
        span = chunks // 2 * cw
        term = jnp.dot(
            half_rows(ctx_t, c), resid_grad[:, group * span : (group + 1) * span], preferred_element_type=F32
        )
        for k in range(chunks // 2):
            ref = jobs[2 + group * (chunks // 2) + k][name]
            ref[...] = term[:, k * cw : (k + 1) * cw].reshape(ref.shape).astype(ref.dtype)

    def col_term(name):
        ref = jobs[1][name]
        term = jnp.dot(scaled_t[...], emb_acc[...].astype(BF16), preferred_element_type=F32)
        ref[...] = term.reshape(ref.shape).astype(ref.dtype)

    for group in range(2):
        proj_terms(other, "snd", group)
        for k in range(chunks // 2):
            pair_copy(2 + group * (chunks // 2) + k).start()

    @pl.when(core == 0)
    def _():
        col_term("snd")
        pair_copy(1).start()

    for group in range(2):
        proj_terms(core, "own", group)

    @pl.when(core == 1)
    def _():
        col_term("own")


    def query_terms():
        def term(p):
            j1, j2, rr = p // plane, lax.rem(p // nz, n2), lax.rem(p, nz)
            s = at.slot(rr, j1, j2, other)
            jobs[0]["snd"][p] = (u_all[s] * scale[pl.ds(s, 1), :]).astype(BF16)

        loop(0, half, term)
        pair_copy(0).start()

    def below_terms(i):
        def below(u):
            for w in range(2):
                s = u * 4 + w * 2
                spread = jnp.concatenate([e_all[s], e_all[s + 1]], axis=1)
                term = jnp.dot(flipped[...], spread, preferred_element_type=F32)
                u_all[s] = term[:, :tok]
                u_all[s + 1] = term[:, tok:]

        loop(i * (n // 16), (i + 1) * (n // 16), below)

    def context_terms(i):
        cut = slice(i * (width // 4), (i + 1) * (width // 4))
        context_grad[:, cut] = lax.dot_general(
            resid_grad[...], wo_v[cut, :], NT, preferred_element_type=F32
        ).astype(BF16)

    fillers = [functools.partial(context_terms, i) for i in range(4)]
    fillers += [functools.partial(below_terms, i) for i in range(4)] + [query_terms]
    steps = [None, step1, step2, step3, step4, step5, step6, step7]
    for code in ORDER:
        if code < 0:
            if fillers:
                fillers.pop(0)()
            continue
        if code == 1:
            while fillers:
                fillers.pop(0)()
        if code % 10 == len(steps):
            continue
        if code // 10 == 1:
            pl.when(core == 1)(functools.partial(steps[code % 10], 1))
        else:
            steps[code % 10](code // 10)

    arrived(stacked["pl"], ap_r)
    arrived(q_all.at[pl.ds(1, n - 1)], gs)
    arrived(msg.at[pl.ds(1, n - 1)], xs)

    @pl.when(core == 0)
    def _():
        arrived(jobs[1]["pl"], c_s.at[0])
        arrived(jobs[1]["pl"], c_r.at[7])

    @pl.when(core == 1)
    def _():
        parts = [others(1, "l1", n1), others(1, "l2", n2), others(1, "l3", nz)]
        for m, ref in enumerate(parts + parts[::-1] + [jobs[1]["pl"]]):
            arrived(ref, c_s.at[1 + m])

    whole, first, second, third = stacked["pl"], stacked["l1"], stacked["l2"], stacked["l3"]
    first = first.at[:, pl.ds(1, n1 - 1)]
    second = second.at[:, pl.ds(1, n2 - 1)]
    third = third.at[:, pl.ds(1, nz - 1)]
    for sem, refs in ((rs_s, (whole, first, second, third)), (ag_s, (third, second, first, whole))):
        for m, ref in enumerate(refs):
            arrived(ref, sem.at[m])
    for m, ref in enumerate((jobs[0]["pl"], others(0, "l1", n1), others(0, "l2", n2), others(0, "l3", nz))):
        arrived(ref, q_s.at[m])


JOB = ("own", "snd", "pl", "b1", "k1", "l1", "b2", "l2", "b3", "k2", "l3")


def finish_kernel(main, col, gain, colbert, loss_in, query_in, resid_in, context_in,
                  proj_grad, colbert_grad, gain_grad, loss, query_grad, resid_grad, context_grad,
                  proj_v, colbert_v, gain_v, sem):
    copies = []

    def send(src, dst):
        copy = pltpu.make_async_copy(src, dst, sem.at[len(copies)])
        copy.start()
        copies.append(copy)

    send(resid_in, resid_grad)
    send(context_in, context_grad)
    send(query_in, query_grad)
    loss[...] = loss_in[:, 0:1]
    chunks, rows, cw = main.shape
    wide = col[...].astype(F32)
    colbert_v[...] = wide
    send(colbert_v, colbert_grad)
    band = rows // 4
    for b in range(4):
        cut = slice(b * band, (b + 1) * band)
        for k in range(chunks):
            proj_v[cut, k * cw : (k + 1) * cw] = main[k, cut, :].astype(F32)
        send(proj_v.at[cut], proj_grad.at[cut])
    ones = jnp.ones((8, wide.shape[1]), F32)
    gain_v[...] = exact(ones, wide * colbert[...].astype(F32), NT)[0:1, :] / gain[...]
    send(gain_v, gain_grad)
    for copy in copies:
        copy.wait()


def stay(array):
    return pltpu.with_memory_space_constraint(array, pltpu.HBM)


def job_buffers(at, piece, cols, lead=(), own=True):
    shapes = [
        ((at.half if own else 1, piece, cols), F32),
        ((at.half, piece, cols), BF16),
        ((at.half, piece, cols), BF16),
        ((at.half, piece, cols), BF16),
        ((at.plane, piece, cols), F32),
        ((at.n1, at.plane, piece, cols), BF16),
        ((at.plane, piece, cols), BF16),
        ((at.n2, at.nz, piece, cols), BF16),
        ((at.nz, piece, cols), BF16),
        ((at.nz, piece, cols), F32),
        ((at.nz, piece, cols), BF16),
    ]
    return [pltpu.VMEM(lead + shape, kind) for shape, kind in shapes]


def body(sizes, query_emb, positive, passage_emb, lengths, residual, context, out_proj, norm_gain, colbert_proj):
    dp, neg = sizes["dp"], sizes["neg"]
    at = Grid(dp, neg)
    own, per, dim = query_emb.shape
    plen = passage_emb.shape[1]
    rows, width = residual.shape
    tok = own * per
    n = at.n
    chunks = width // dim
    cw = dim
    piece = width // (2 * at.half)
    dma = pltpu.SemaphoreType.DMA
    vm = pltpu.VMEM
    scratch = [
        vm((n, tok, dim), BF16),
        vm((n, 1, 2 * n * own), F32),
        vm((n, plen, tok), BF16),
        vm((n, dim, tok), F32),
        vm((n, tok), F32),
        vm((n, tok), F32),
        vm((n, tok), F32),
        vm((plen, 2 * tok), F32),
        vm((plen, dim), BF16),
        vm((dim, plen), BF16),
        vm((plen, dim), F32),
        pltpu.SMEM((own,), jnp.int32),
        vm((1, width), F32),
        vm((width, width), BF16),
        vm((width, dim), BF16),
        vm((width, rows), BF16),
        vm((width, rows), BF16),
        vm((rows, width), F32),
        vm((rows, 128), F32),
        vm((rows, dim), F32),
    ]
    scratch += job_buffers(at, dim, tok, own=False)
    scratch += job_buffers(at, 2 * piece, cw)
    scratch += job_buffers(at, piece, cw, (chunks,))
    scratch += [
        dma((8,)),
        dma,
        dma((n,)),
        dma,
        dma,
        dma((4,)),
        dma((4,)),
        dma((8,)),
        dma((8,)),
        dma((4,)),
        dma((chunks, 4)),
        dma((4,)),
        dma((chunks, 3)),
        dma,
    ]
    held = sum(math.prod(ref.shape) * jnp.dtype(ref.dtype).itemsize for ref in scratch[:-14])
    limit = min(held + held // 8 + 8 * 1024 * 1024, 67043328)
    loss, query_grad, resid_grad, context_grad, summed, summed_map = pl.pallas_call(
        functools.partial(main_kernel, dp, neg, own, per),
        out_shape=[
            jax.ShapeDtypeStruct((1, 128), F32),
            jax.ShapeDtypeStruct((tok, dim), F32),
            jax.ShapeDtypeStruct((rows, width), BF16),
            jax.ShapeDtypeStruct((rows, width), BF16),
            jax.ShapeDtypeStruct((chunks, 2, at.half, piece, cw), BF16),
            jax.ShapeDtypeStruct((at.half, 2 * piece, cw), BF16),
        ],
        in_specs=[HBM, HBM, HBM, SMEM, HBM, HBM, HBM, HBM, HBM],
        out_specs=[VMEM] * 6,
        scratch_shapes=scratch,
        compiler_params=pltpu.CompilerParams(
            collective_id=1, has_side_effects=True, vmem_limit_bytes=limit
        ),
        name="maxsim_main",
    )(
        stay(query_emb.reshape(tok, dim)),
        stay(positive),
        stay(passage_emb.reshape(plen, dim)),
        lengths,
        stay(residual),
        stay(context),
        stay(out_proj),
        stay(norm_gain[None, :]),
        stay(colbert_proj),
    )
    proj_grad, colbert_grad, gain_grad, loss, query_grad, resid_grad, context_grad = pl.pallas_call(
        finish_kernel,
        out_shape=[
            jax.ShapeDtypeStruct((width, width), F32),
            jax.ShapeDtypeStruct((width, dim), F32),
            jax.ShapeDtypeStruct((1, width), F32),
            jax.ShapeDtypeStruct((1, 1), F32),
            jax.ShapeDtypeStruct((tok, dim), F32),
            jax.ShapeDtypeStruct((rows, width), BF16),
            jax.ShapeDtypeStruct((rows, width), BF16),
        ],
        in_specs=[VMEM] * 8,
        out_specs=[ANY, ANY, ANY, VMEM, ANY, ANY, ANY],
        scratch_shapes=[vm((width, width), F32), vm((width, dim), F32), vm((1, width), F32), dma((10,))],
        compiler_params=pltpu.CompilerParams(vmem_limit_bytes=20000000),
        name="maxsim_finish",
    )(
        summed.reshape(chunks, width, cw),
        summed_map.reshape(width, dim),
        norm_gain[None, :],
        colbert_proj,
        loss,
        query_grad,
        resid_grad,
        context_grad,
    )
    return (
        loss.reshape(()),
        query_grad.reshape(own, per, dim),
        resid_grad,
        context_grad,
        proj_grad,
        colbert_grad,
        gain_grad.reshape(width),
    )


def solution(mesh):
    sizes = {axis: mesh.shape[axis] for axis in ("dp", "neg")}
    split = ("dp", "neg")
    in_specs = (
        P(split, None, None),
        P(split),
        P(split, None, None),
        P(split),
        P(split, None),
        P(split, None),
        P(),
        P(),
        P(),
    )
    out_specs = (
        P(),
        P(split, None, None),
        P(split, None),
        P(split, None),
        P(),
        P(),
        P(),
    )
    return jax.shard_map(
        functools.partial(body, sizes), mesh=mesh, in_specs=in_specs, out_specs=out_specs, check_vma=False
    )
```

```python
import functools
import math

import jax
import jax.numpy as jnp
from jax import lax
from jax.experimental import pallas as pl
from jax.experimental.pallas import tpu as pltpu
from jax.sharding import PartitionSpec as P

MESH = pl.DeviceIdType.MESH
VMEM = pl.BlockSpec(memory_space=pltpu.VMEM)
SMEM = pl.BlockSpec(memory_space=pltpu.SMEM)
ANY = pl.BlockSpec(memory_space=pl.ANY)
HBM = pl.BlockSpec(memory_space=pltpu.HBM)
LOW = -1e30
F32 = jnp.float32
BF16 = jnp.bfloat16
NT = (((1,), (1,)), ((), ()))
LAG = 2
EARLY = 2
TURNED = ()
ORDER = (
    21, 31, 41, 51, 61, -1, -1, -1, 22, 32, 71, -1, -1, 42, 81, -1, 62, 52, 91, 23, -1, -1, 33, -1, 43, 72, 11, 63,
    82, 53, 24, 92, 73, 34, 12, 1, 83, 93, 64, 44, 25, 13, 54, 35, 2, 84, 94, 45, 65, 74, 36, 26, 14, 55, 85, 66,
    46, 75, 95, 3, 56, 15, 86, 27, 76, 96, 47, 37, 57, 16, 67, 87, 28, 77, 4, 68, 38, 97, 88, 58, 78, 48, 17, 98,
    18,
)


def exact(a, b, dims=(((1,), (0,)), ((), ()))):
    return lax.dot_general(a, b, dims, precision=lax.Precision.HIGHEST, preferred_element_type=F32)


def each(size, act):
    def turn(k, carry):
        act(k)
        return carry

    lax.fori_loop(1, size, turn, 0)


def loop(low, high, act):
    def turn(k, carry):
        act(k)
        return carry

    lax.fori_loop(low, high, turn, 0)


def remote(src, dst, send, recv, device):
    return pltpu.make_async_remote_copy(
        src_ref=src, dst_ref=dst, send_sem=send, recv_sem=recv, device_id=device, device_id_type=MESH
    )


class Grid:
    def __init__(self, dp, neg):
        groups = neg // 2
        self.dp, self.neg = dp, neg
        self.a = 2 if groups % 2 == 0 else 1
        self.b = groups // self.a
        self.n1, self.n2, self.nz = self.b, self.a, dp
        self.turned = self.a == self.b
        self.n = dp * neg
        self.half = self.n // 2
        self.plane = self.n2 * self.nz

    def locate(self):
        self.r, self.col = lax.axis_index("dp"), lax.axis_index("neg")
        self.core = lax.rem(self.col, 2)
        g = self.col // 2
        self.y, self.x = g // self.b, lax.rem(g, self.b)
        self.me = self.r * self.neg + self.col

    def flip(self, core, turn=0):
        return core * (1 - turn) + (1 - core) * turn if self.turned else 0 * core

    def own(self, core, turn=0):
        f = self.flip(core, turn)
        return (self.x * (1 - f) + self.y * f, self.y * (1 - f) + self.x * f)

    def column(self, j1, j2, core, turn=0):
        f = self.flip(core, turn)
        x, y = j1 * (1 - f) + j2 * f, j2 * (1 - f) + j1 * f
        return (y * self.b + x) * 2 + core

    def nearby(self, k):
        there, bit = self.r, 1
        while bit < self.nz:
            there = there + lax.rem(k // bit, 2) * bit * (1 - 2 * lax.rem(self.r // bit, 2))
            bit *= 2
        return there

    def arrival(self, i, core):
        i1, i2 = self.own(core)
        m2, m1, k = i // (self.n1 * self.nz), lax.rem(i // self.nz, self.n1), lax.rem(i, self.nz)
        return (self.nearby(k), lax.rem(i1 + m1, self.n1), lax.rem(i2 + m2, self.n2))

    def slot(self, rr, j1, j2, core):
        return rr * self.neg + self.column(j1, j2, core)


def main_kernel(dp, neg, own, per, query, positive_in, passage, lengths, resid, context, out_proj, gain_in, colbert,
                loss, query_grad, resid_grad, context_grad, summed, summed_map,
                q_all, msg, e_all, u_all, sums, inner, scale, bias, pas_v, flipped, emb_acc,
                positive, gain, wo_v, cp_v, ctx_t, scaled_t, normed, inv_std, blend, *rest):
    at = Grid(dp, neg)
    at.locate()
    r, core, me = at.r, at.core, at.me
    other = 1 - core
    i1, i2 = at.own(core)
    n, n1, n2, nz, half, plane = at.n, at.n1, at.n2, at.nz, at.half, at.plane
    partner = (r, at.col + 1 - 2 * core)
    away = 2 * (2 * r // nz) - 1
    tok = own * per
    wide = n * own
    rows, width = resid.shape
    block = rows // 4
    chunks = summed.shape[0]
    cw = summed.shape[-1]
    count = len(JOB)
    sems = rest[3 * count :]
    ld, gs, agr, xs, xr, q_s, q_r, c_s, c_r, rs_s, rs_r, ag_s, ag_r, ap_r = sems

    def dev1(t):
        return (r, at.column(lax.rem(i1 + t, n1), i2, core))

    def dev2(t):
        return (r, at.column(i1, lax.rem(i2 + t, n2), core))

    def devz(k):
        return (lax.rem(r + k, nz), at.col)

    def any_device(k):
        d = lax.rem(me + k * away + n, n)
        return (d // neg, lax.rem(d, neg))

    barrier = pltpu.get_barrier_semaphore()

    def greet(device):
        pl.semaphore_signal(barrier, inc=1, device_id=device, device_id_type=MESH)

    each(nz, lambda k: greet(devz(k)))
    each(n1, lambda t: greet(dev1(t)))
    each(n2, lambda t: greet(dev2(t)))
    greet(partner)
    loads = [
        pltpu.make_async_copy(query, q_all.at[me], ld.at[0]),
        pltpu.make_async_copy(passage, pas_v, ld.at[1]),
        pltpu.make_async_copy(context, context_grad, ld.at[2]),
        pltpu.make_async_copy(out_proj, wo_v, ld.at[3]),
        pltpu.make_async_copy(resid, resid_grad, ld.at[4]),
        pltpu.make_async_copy(colbert, cp_v, ld.at[5]),
        pltpu.make_async_copy(gain_in, gain, ld.at[6]),
        pltpu.make_async_copy(positive_in, positive, ld.at[7]),
    ]
    for copy in loads:
        copy.start()
    loads[0].wait()
    pl.semaphore_wait(barrier, nz + n1 + n2 - 2)

    def arrived(ref, sem):
        pltpu.make_async_copy(ref, ref, sem).wait()

    def spread(s, device):
        return remote(q_all.at[s], q_all.at[s], gs, agr.at[s], device)

    def landed(s):
        spread(s, partner).wait_recv()

    def pass_on(i):
        rr, j1, j2 = at.arrival(i, core)
        s = at.slot(rr, j1, j2, core)

        @pl.when(i < nz)
        def _():
            each(n1, lambda t: spread(s, dev1(t)).start())

        @pl.when(i < nz * n1)
        def _():
            each(n2, lambda t: spread(s, dev2(t)).start())

        spread(s, partner).start()

    def attend(v):
        u, side = v // 2, lax.rem(v, 2)
        whose = core * (1 - side) + other * side
        slots = [at.slot(*at.arrival(2 * u + w, whose), whose) for w in range(2)]

        @pl.when(side == 1)
        def _():
            for s in slots:
                landed(s)

        tokens = jnp.concatenate([q_all[s] for s in slots], axis=0)
        scores = lax.dot_general(pas_v[...], tokens, NT, preferred_element_type=F32) + bias[...]
        highest = jnp.max(scores, axis=0, keepdims=True)
        spread = jnp.exp(scores - highest)
        total = jnp.sum(spread, axis=0, keepdims=True)
        low = spread.astype(BF16)
        level = highest + jnp.log(total)
        for w, s in enumerate(slots):
            cut = slice(w * tok, (w + 1) * tok)
            e_all[s] = low[:, cut]
            sums[pl.ds(s, 1), :] = total[:, cut]
            inner[pl.ds(s, 1), :] = level[:, cut]

    each(nz, lambda k: spread(me, devz(k)).start())
    pass_on(0)
    loads[1].wait()
    length = lengths[0]
    position = lax.broadcasted_iota(jnp.int32, bias.shape, 0)
    bias[...] = jnp.where(position < length, 0.0, LOW)
    flipped[...] = pas_v[...].astype(F32).T.astype(BF16)

    def norm_block(i):
        cut = pl.ds(pl.multiple_of(i * block, block), block)
        ctx = context_grad[cut, :]
        hidden = resid_grad[cut, :].astype(F32) + jnp.dot(ctx, wo_v[...], preferred_element_type=F32)
        centred = hidden - jnp.mean(hidden, axis=1, keepdims=True)
        variance = jnp.mean(centred * centred, axis=1, keepdims=True)
        inv = 1.0 / jnp.sqrt(variance + 1e-05)
        norm = centred * inv
        normed[cut, :] = norm
        inv_std[cut, :] = jnp.broadcast_to(inv, (block, inv_std.shape[1]))
        scaled = norm * gain[...]
        scaled_t[:, cut] = scaled.T.astype(BF16)
        blend[cut, :] = jnp.dot(scaled.astype(BF16), cp_v[...], preferred_element_type=F32) / width
        ctx_t[:, cut] = ctx.astype(F32).T.astype(BF16)

    for copy in loads[2:7]:
        copy.wait()
    loop(0, EARLY, norm_block)

    def relay(i):
        landed(at.slot(*at.arrival(i, core), core))
        pass_on(i)

    def relay_step(i):
        relay(i)

        @pl.when(i >= LAG)
        def _():
            attend(i - LAG)

    loop(1, half, relay_step)
    loop(half - LAG, half, attend)

    loads[7].wait()
    token = lax.broadcasted_iota(jnp.int32, (tok, wide), 0)
    lane = lax.broadcasted_iota(jnp.int32, (tok, wide), 1)
    spots = jnp.where(token // per == lax.rem(lane, own), 1.0, 0.0)
    slot_of = lax.broadcasted_iota(jnp.int32, (n, wide), 0)
    lane_of = lax.broadcasted_iota(jnp.int32, (n, wide), 1)
    mine = slot_of == lane_of // own
    grouped = exact(inner[...], spots)
    similar = jnp.sum(jnp.where(mine, grouped, 0.0), axis=0, keepdims=True)
    shift = jnp.log(jnp.full((1, wide), length, jnp.int32).astype(F32)) * per
    row_lane = lax.broadcasted_iota(jnp.int32, (1, wide), 1)
    chosen = jnp.zeros((1, wide), jnp.int32)
    for i in range(own):
        chosen = chosen + jnp.where(row_lane == me * own + i, positive[i], 0)
    msg[me, :, :wide] = similar - shift
    msg[me, :, wide:] = chosen.astype(F32)

    each(n, lambda k: remote(msg.at[me], msg.at[me], xs, xr, any_device(k)).start())

    loop(EARLY, 4, norm_block)
    flat = exact(jnp.broadcast_to(gain[...], (8, width)), cp_v[...].astype(F32))[0:1, :] / width

    arrived(msg.at[pl.ds(1, n - 1)], xr)

    everyone = msg[:, :, :wide]
    picked = jnp.sum(msg[:, :, wide:], axis=0)
    highest = jnp.max(everyone, axis=0)
    log_total = highest + jnp.log(jnp.sum(jnp.exp(everyone - highest[None]), axis=0))
    which = lax.broadcasted_iota(jnp.int32, everyone.shape, 0).astype(F32)
    score = jnp.sum(jnp.where(which == picked[None], everyone, 0.0), axis=0)
    average = jnp.sum(log_total - score, axis=1, keepdims=True) / wide
    loss[...] = jnp.broadcast_to(average, loss.shape)
    hit = jnp.where(picked == me.astype(F32), 1.0, 0.0)
    coefficient = jnp.exp(similar - shift - log_total) - hit
    laid = jnp.where(mine, jnp.broadcast_to(coefficient, mine.shape), 0.0)
    scale[...] = exact(laid, spots, NT) / sums[...]

    jobs = [dict(zip(JOB, rest[:count]), out=None, sums=[(q_s.at[k], q_r.at[k]) for k in range(4)])]
    jobs.append(dict(zip(JOB, rest[count : 2 * count]), out=summed_map))
    jobs[1]["sums"] = [(c_s.at[m], c_r.at[m]) for m in range(4)]
    jobs[1]["outs"] = [(c_s.at[4 + m], c_r.at[4 + m]) for m in range(4)]
    stacked = dict(zip(JOB, rest[2 * count : 3 * count]))
    for k in range(chunks):
        job = {name: ref.at[k] for name, ref in stacked.items()}
        job["out"] = summed.at[k, core]
        job["sums"] = [(rs_s.at[m], rs_r.at[k, m]) for m in range(4)]
        job["outs"] = [(ag_s.at[m], ag_r.at[k, m]) for m in range(3)] + [(ag_s.at[3], ap_r)]
        jobs.append(job)
    for j, job in enumerate(jobs):
        turn = 1 if j in TURNED else 0
        job["at"] = h1, h2 = at.own(core, turn)
        job["place"] = (h1 * n2 + h2) * nz + r
        job["turn"] = turn

    def job1(j, t):
        h1, h2 = jobs[j]["at"]
        return (r, at.column(lax.rem(h1 + t, n1), h2, core, jobs[j]["turn"]))

    def job2(j, t):
        h1, h2 = jobs[j]["at"]
        return (r, at.column(h1, lax.rem(h2 + t, n2), core, jobs[j]["turn"]))

    def pair_copy(j):
        return remote(jobs[j]["snd"], jobs[j]["pl"], *jobs[j]["sums"][0], partner)

    def rs1_copy(j, t):
        there = pl.ds(lax.rem(jobs[j]["at"][0] + t, n1) * plane, plane)
        return remote(jobs[j]["b1"].at[there], jobs[j]["l1"].at[t], *jobs[j]["sums"][1], job1(j, t))

    def rs2_copy(j, t):
        there = pl.ds(lax.rem(jobs[j]["at"][1] + t, n2) * nz, nz)
        return remote(jobs[j]["b2"].at[there], jobs[j]["l2"].at[t], *jobs[j]["sums"][2], job2(j, t))

    def rs3_copy(j, k):
        return remote(jobs[j]["b3"].at[lax.rem(r + k, nz)], jobs[j]["l3"].at[k], *jobs[j]["sums"][3], devz(k))

    def out_copy(j, level, piece, device):
        return remote(piece, piece, *jobs[j]["outs"][level], device)

    def others(j, name, size):
        return jobs[j][name].at[pl.ds(1, size - 1)]

    def step1(j):
        job = jobs[j]
        pair_copy(j).wait_recv()
        if j > 0:
            job["b1"][...] = (job["own"][...] + job["pl"][...].astype(F32)).astype(BF16)
            kept = pl.ds(job["at"][0] * plane, plane)
            job["k1"][...] = job["own"][kept] + job["pl"][kept].astype(F32)
        else:

            def send_term(p):
                j1, j2, rr = p // plane, lax.rem(p // nz, n2), lax.rem(p, nz)
                s = at.slot(rr, j1, j2, core)
                total = u_all[s] * scale[pl.ds(s, 1), :] + job["pl"][p].astype(F32)
                job["b1"][p] = total.astype(BF16)

            def keep_term(q):
                p = i1 * plane + q
                j1, j2, rr = p // plane, lax.rem(p // nz, n2), lax.rem(p, nz)
                s = at.slot(rr, j1, j2, core)
                job["k1"][q] = u_all[s] * scale[pl.ds(s, 1), :] + job["pl"][p].astype(F32)

            loop(plane, half, lambda p: send_term(lax.rem(i1 * plane + p, half)))
            loop(0, plane, keep_term)
        for t in range(1, n1):
            rs1_copy(j, t).start()

    def step2(j):
        job = jobs[j]
        arrived(others(j, "l1", n1), job["sums"][1][1])
        total = job["k1"][...]
        for t in range(1, n1):
            total = total + job["l1"][t].astype(F32)
        job["b2"][...] = total.astype(BF16)
        job["k1"][...] = total
        for t in range(1, n2):
            rs2_copy(j, t).start()

    def step3(j):
        job = jobs[j]
        arrived(others(j, "l2", n2), job["sums"][2][1])
        total = job["k1"][pl.ds(job["at"][1] * nz, nz)]
        for t in range(1, n2):
            total = total + job["l2"][t].astype(F32)
        job["b3"][...] = total.astype(BF16)
        job["k2"][...] = total
        for k in range(1, nz):
            rs3_copy(j, k).start()

    def step4(j):
        job = jobs[j]
        arrived(others(j, "l3", nz), job["sums"][3][1])
        total = job["k2"][r]
        for k in range(1, nz):
            total = total + job["l3"][k].astype(F32)
        if job["out"] is None:
            query_grad[...] = total.T
        else:
            job["out"][job["place"]] = total.astype(BF16)
            for k in range(1, nz):
                out_copy(j, 0, job["out"].at[job["place"]], devz(k)).start()

    def step5(j):
        arrived(others(j, "l3", nz), jobs[j]["outs"][0][1])
        h1, h2 = jobs[j]["at"]
        piece = jobs[j]["out"].at[pl.ds((h1 * n2 + h2) * nz, nz)]
        for t in range(1, n2):
            out_copy(j, 1, piece, job2(j, t)).start()

    def step6(j):
        arrived(others(j, "l2", n2), jobs[j]["outs"][1][1])
        piece = jobs[j]["out"].at[pl.ds(jobs[j]["at"][0] * plane, plane)]
        for t in range(1, n1):
            out_copy(j, 2, piece, job1(j, t)).start()

    def step7(j):
        arrived(others(j, "l1", n1), jobs[j]["outs"][2][1])
        out_copy(j, 3, jobs[j]["out"], partner).start()

    emb_acc[...] = jnp.zeros_like(emb_acc)

    def emb_term(u):
        parts = []
        for v in range(16):
            s = u * 16 + v
            row = jnp.broadcast_to(scale[pl.ds(s, 1), :], (16, tok)).astype(BF16)
            spread = e_all[s]
            parts.append((spread.reshape(-1, 16, tok) * row[None]).reshape(spread.shape))
        weight = jnp.concatenate(parts, axis=1)
        tokens = q_all[pl.ds(u * 16, 16)].reshape(16 * tok, q_all.shape[2])
        emb_acc[...] += jnp.dot(weight, tokens, preferred_element_type=F32)

    loop(0, n // 16, emb_term)
    emb = emb_acc[...].astype(BF16)
    emb_acc[...] = emb.astype(F32)

    def grad_block(i):
        cut = pl.ds(pl.multiple_of(i * block, block), block)
        grad = emb_acc[cut, :]
        first = jnp.sum(grad * flat, axis=1, keepdims=True)
        second = jnp.sum(grad * blend[cut, :], axis=1, keepdims=True)
        scaled_grad = lax.dot_general(grad.astype(BF16), cp_v[...], NT, preferred_element_type=F32)
        hidden_grad = inv_std[cut, 0:1] * (scaled_grad * gain[...] - first - normed[cut, :] * second)
        resid_grad[cut, :] = hidden_grad.astype(BF16)

    loop(0, 4, grad_block)

    mid = width // 2

    def half_rows(ref, c):
        return ref[pl.ds(pl.multiple_of(c * mid, mid), mid), :]

    def proj_terms(c, name, group):
        span = chunks // 2 * cw
        term = jnp.dot(
            half_rows(ctx_t, c), resid_grad[:, group * span : (group + 1) * span], preferred_element_type=F32
        )
        for k in range(chunks // 2):
            ref = jobs[2 + group * (chunks // 2) + k][name]
            ref[...] = term[:, k * cw : (k + 1) * cw].reshape(ref.shape).astype(ref.dtype)

    def col_term(name):
        ref = jobs[1][name]
        term = jnp.dot(scaled_t[...], emb_acc[...].astype(BF16), preferred_element_type=F32)
        ref[...] = term.reshape(ref.shape).astype(ref.dtype)

    for group in range(2):
        proj_terms(other, "snd", group)
        for k in range(chunks // 2):
            pair_copy(2 + group * (chunks // 2) + k).start()

    @pl.when(core == 0)
    def _():
        col_term("snd")
        pair_copy(1).start()

    for group in range(2):
        proj_terms(core, "own", group)

    @pl.when(core == 1)
    def _():
        col_term("own")


    def query_terms():
        def term(p):
            j1, j2, rr = p // plane, lax.rem(p // nz, n2), lax.rem(p, nz)
            s = at.slot(rr, j1, j2, other)
            jobs[0]["snd"][p] = (u_all[s] * scale[pl.ds(s, 1), :]).astype(BF16)

        loop(0, half, term)
        pair_copy(0).start()

    def below_terms(i):
        def below(u):
            for w in range(2):
                s = u * 4 + w * 2
                spread = jnp.concatenate([e_all[s], e_all[s + 1]], axis=1)
                term = jnp.dot(flipped[...], spread, preferred_element_type=F32)
                u_all[s] = term[:, :tok]
                u_all[s + 1] = term[:, tok:]

        loop(i * (n // 16), (i + 1) * (n // 16), below)

    def context_terms(i):
        cut = slice(i * (width // 4), (i + 1) * (width // 4))
        context_grad[:, cut] = lax.dot_general(
            resid_grad[...], wo_v[cut, :], NT, preferred_element_type=F32
        ).astype(BF16)

    fillers = [functools.partial(context_terms, i) for i in range(4)]
    fillers += [functools.partial(below_terms, i) for i in range(4)] + [query_terms]
    steps = [None, step1, step2, step3, step4, step5, step6, step7]
    for code in ORDER:
        if code < 0:
            if fillers:
                fillers.pop(0)()
            continue
        if code == 1:
            while fillers:
                fillers.pop(0)()
        if code % 10 == len(steps):
            continue
        if code // 10 == 1:
            pl.when(core == 1)(functools.partial(steps[code % 10], 1))
        else:
            steps[code % 10](code // 10)

    arrived(stacked["pl"], ap_r)
    arrived(q_all.at[pl.ds(1, n - 1)], gs)
    arrived(msg.at[pl.ds(1, n - 1)], xs)

    @pl.when(core == 0)
    def _():
        arrived(jobs[1]["pl"], c_s.at[0])
        arrived(jobs[1]["pl"], c_r.at[7])

    @pl.when(core == 1)
    def _():
        parts = [others(1, "l1", n1), others(1, "l2", n2), others(1, "l3", nz)]
        for m, ref in enumerate(parts + parts[::-1] + [jobs[1]["pl"]]):
            arrived(ref, c_s.at[1 + m])

    whole, first, second, third = stacked["pl"], stacked["l1"], stacked["l2"], stacked["l3"]
    first = first.at[:, pl.ds(1, n1 - 1)]
    second = second.at[:, pl.ds(1, n2 - 1)]
    third = third.at[:, pl.ds(1, nz - 1)]
    for sem, refs in ((rs_s, (whole, first, second, third)), (ag_s, (third, second, first, whole))):
        for m, ref in enumerate(refs):
            arrived(ref, sem.at[m])
    for m, ref in enumerate((jobs[0]["pl"], others(0, "l1", n1), others(0, "l2", n2), others(0, "l3", nz))):
        arrived(ref, q_s.at[m])


JOB = ("own", "snd", "pl", "b1", "k1", "l1", "b2", "l2", "b3", "k2", "l3")


def finish_kernel(main, col, gain, colbert, loss_in, query_in, resid_in, context_in,
                  proj_grad, colbert_grad, gain_grad, loss, query_grad, resid_grad, context_grad,
                  proj_v, colbert_v, gain_v, sem):
    copies = []

    def send(src, dst):
        copy = pltpu.make_async_copy(src, dst, sem.at[len(copies)])
        copy.start()
        copies.append(copy)

    send(resid_in, resid_grad)
    send(context_in, context_grad)
    send(query_in, query_grad)
    loss[...] = loss_in[:, 0:1]
    chunks, rows, cw = main.shape
    wide = col[...].astype(F32)
    colbert_v[...] = wide
    send(colbert_v, colbert_grad)
    band = rows // 4
    for b in range(4):
        if b == 3:
            ones = jnp.ones((8, wide.shape[1]), F32)
            gain_v[...] = exact(ones, wide * colbert[...].astype(F32), NT)[0:1, :] / gain[...]
            send(gain_v, gain_grad)
        cut = slice(b * band, (b + 1) * band)
        for k in range(chunks):
            proj_v[cut, k * cw : (k + 1) * cw] = main[k, cut, :].astype(F32)
        send(proj_v.at[cut], proj_grad.at[cut])
    for copy in copies:
        copy.wait()


def stay(array):
    return pltpu.with_memory_space_constraint(array, pltpu.HBM)


def job_buffers(at, piece, cols, lead=(), own=True):
    shapes = [
        ((at.half if own else 1, piece, cols), F32),
        ((at.half, piece, cols), BF16),
        ((at.half, piece, cols), BF16),
        ((at.half, piece, cols), BF16),
        ((at.plane, piece, cols), F32),
        ((at.n1, at.plane, piece, cols), BF16),
        ((at.plane, piece, cols), BF16),
        ((at.n2, at.nz, piece, cols), BF16),
        ((at.nz, piece, cols), BF16),
        ((at.nz, piece, cols), F32),
        ((at.nz, piece, cols), BF16),
    ]
    return [pltpu.VMEM(lead + shape, kind) for shape, kind in shapes]


def body(sizes, query_emb, positive, passage_emb, lengths, residual, context, out_proj, norm_gain, colbert_proj):
    dp, neg = sizes["dp"], sizes["neg"]
    at = Grid(dp, neg)
    own, per, dim = query_emb.shape
    plen = passage_emb.shape[1]
    rows, width = residual.shape
    tok = own * per
    n = at.n
    chunks = width // dim
    cw = dim
    piece = width // (2 * at.half)
    dma = pltpu.SemaphoreType.DMA
    vm = pltpu.VMEM
    scratch = [
        vm((n, tok, dim), BF16),
        vm((n, 1, 2 * n * own), F32),
        vm((n, plen, tok), BF16),
        vm((n, dim, tok), F32),
        vm((n, tok), F32),
        vm((n, tok), F32),
        vm((n, tok), F32),
        vm((plen, 2 * tok), F32),
        vm((plen, dim), BF16),
        vm((dim, plen), BF16),
        vm((plen, dim), F32),
        pltpu.SMEM((own,), jnp.int32),
        vm((1, width), F32),
        vm((width, width), BF16),
        vm((width, dim), BF16),
        vm((width, rows), BF16),
        vm((width, rows), BF16),
        vm((rows, width), F32),
        vm((rows, 128), F32),
        vm((rows, dim), F32),
    ]
    scratch += job_buffers(at, dim, tok, own=False)
    scratch += job_buffers(at, 2 * piece, cw)
    scratch += job_buffers(at, piece, cw, (chunks,))
    scratch += [
        dma((8,)),
        dma,
        dma((n,)),
        dma,
        dma,
        dma((4,)),
        dma((4,)),
        dma((8,)),
        dma((8,)),
        dma((4,)),
        dma((chunks, 4)),
        dma((4,)),
        dma((chunks, 3)),
        dma,
    ]
    held = sum(math.prod(ref.shape) * jnp.dtype(ref.dtype).itemsize for ref in scratch[:-14])
    limit = min(held + held // 8 + 8 * 1024 * 1024, 67043328)
    loss, query_grad, resid_grad, context_grad, summed, summed_map = pl.pallas_call(
        functools.partial(main_kernel, dp, neg, own, per),
        out_shape=[
            jax.ShapeDtypeStruct((1, 128), F32),
            jax.ShapeDtypeStruct((tok, dim), F32),
            jax.ShapeDtypeStruct((rows, width), BF16),
            jax.ShapeDtypeStruct((rows, width), BF16),
            jax.ShapeDtypeStruct((chunks, 2, at.half, piece, cw), BF16),
            jax.ShapeDtypeStruct((at.half, 2 * piece, cw), BF16),
        ],
        in_specs=[HBM, HBM, HBM, SMEM, HBM, HBM, HBM, HBM, HBM],
        out_specs=[VMEM] * 6,
        scratch_shapes=scratch,
        compiler_params=pltpu.CompilerParams(
            collective_id=1, has_side_effects=True, vmem_limit_bytes=limit
        ),
        name="maxsim_main",
    )(
        stay(query_emb.reshape(tok, dim)),
        stay(positive),
        stay(passage_emb.reshape(plen, dim)),
        lengths,
        stay(residual),
        stay(context),
        stay(out_proj),
        stay(norm_gain[None, :]),
        stay(colbert_proj),
    )
    proj_grad, colbert_grad, gain_grad, loss, query_grad, resid_grad, context_grad = pl.pallas_call(
        finish_kernel,
        out_shape=[
            jax.ShapeDtypeStruct((width, width), F32),
            jax.ShapeDtypeStruct((width, dim), F32),
            jax.ShapeDtypeStruct((1, width), F32),
            jax.ShapeDtypeStruct((1, 1), F32),
            jax.ShapeDtypeStruct((tok, dim), F32),
            jax.ShapeDtypeStruct((rows, width), BF16),
            jax.ShapeDtypeStruct((rows, width), BF16),
        ],
        in_specs=[VMEM] * 8,
        out_specs=[ANY, ANY, ANY, VMEM, ANY, ANY, ANY],
        scratch_shapes=[vm((width, width), F32), vm((width, dim), F32), vm((1, width), F32), dma((10,))],
        compiler_params=pltpu.CompilerParams(vmem_limit_bytes=20000000),
        name="maxsim_finish",
    )(
        summed.reshape(chunks, width, cw),
        summed_map.reshape(width, dim),
        norm_gain[None, :],
        colbert_proj,
        loss,
        query_grad,
        resid_grad,
        context_grad,
    )
    return (
        loss.reshape(()),
        query_grad.reshape(own, per, dim),
        resid_grad,
        context_grad,
        proj_grad,
        colbert_grad,
        gain_grad.reshape(width),
    )


def solution(mesh):
    sizes = {axis: mesh.shape[axis] for axis in ("dp", "neg")}
    split = ("dp", "neg")
    in_specs = (
        P(split, None, None),
        P(split),
        P(split, None, None),
        P(split),
        P(split, None),
        P(split, None),
        P(),
        P(),
        P(),
    )
    out_specs = (
        P(),
        P(split, None, None),
        P(split, None),
        P(split, None),
        P(),
        P(),
        P(),
    )
    return jax.shard_map(
        functools.partial(body, sizes), mesh=mesh, in_specs=in_specs, out_specs=out_specs, check_vma=False
    )
```
